128 devices in a mesh: dp: 1, ep: 128 (over z, y, x, core).
Axes of the slice: x: 4, y: 4, z: 4, core: 2. Of those that a mesh axis runs over, the one named last changes fastest.
Arguments:
- x_in: bfloat16 [12288, 512], P(('dp', 'ep'))
- idx_a: int32 [12288, 8], P(('dp', 'ep'))
- idx_b: int32 [12288, 8], P(('dp', 'ep'))
- gate_a: float32 [12288, 8], P(('dp', 'ep'))
- gate_b: float32 [12288, 8], P(('dp', 'ep'))
- dy_out: bfloat16 [12288, 512], P(('dp', 'ep'))
- w1_a: bfloat16 [384, 512, 128], P('ep')
- w3_a: bfloat16 [384, 512, 128], P('ep')
- w2_a: bfloat16 [384, 128, 512], P('ep')
- w1_b: bfloat16 [384, 512, 128], P('ep')
- w3_b: bfloat16 [384, 512, 128], P('ep')
- w2_b: bfloat16 [384, 128, 512], P('ep')
Outputs:
- output 1: bfloat16 [12288, 512], P(('dp', 'ep'))
- output 2: bfloat16 [12288, 512], P(('dp', 'ep'))
- output 3: float32 [384, 512, 128], P(('dp', 'ep'))
- output 4: float32 [384, 512, 128], P(('dp', 'ep'))
- output 5: float32 [384, 128, 512], P(('dp', 'ep'))
- output 6: float32 [384, 512, 128], P(('dp', 'ep'))
- output 7: float32 [384, 512, 128], P(('dp', 'ep'))
- output 8: float32 [384, 128, 512], P(('dp', 'ep'))
- output 9: float32 [12288, 8], P(('dp', 'ep'))
- output 10: float32 [12288, 8], P(('dp', 'ep'))
All inputs are finite; a program needn't handle non-finite values.
Results may differ from the reference program's by a relative error of at most 0.00686.
Values are sent between devices in bfloat16 or wider.
A program may use at most 1 GiB of HBM per device.

```python
import jax
import jax.numpy as jnp
from jax import lax

TOKENS = 96
D = 512
FF = 128
EXPERTS = 384
TOP = 8
GROUP = 128
CAP = 8
HOT = 24


def draw_routing(root_key):
    key_hot, key_dev = jax.random.split(root_key)
    ranking = jax.random.permutation(key_hot, EXPERTS)
    cold_total = EXPERTS - HOT
    spare_pairs = TOKENS * TOP - HOT * CAP
    base_count = spare_pairs // cold_total
    extra_count = spare_pairs - base_count * cold_total

    def one_device(dev_key):
        key_count, key_rows, key_shift = jax.random.split(dev_key, 3)
        cold_rank = jax.random.permutation(key_count, cold_total)
        cold_count = base_count + (cold_rank < extra_count).astype(jnp.int32)
        by_rank = jnp.concatenate([jnp.full((HOT,), CAP, jnp.int32), cold_count])
        expert_count = jnp.zeros((EXPERTS,), jnp.int32).at[ranking].set(by_rank)
        run_ends = jnp.cumsum(expert_count)
        positions = jnp.arange(TOKENS * TOP, dtype=jnp.int32)
        sorted_ids = jnp.searchsorted(run_ends, positions, side="right").astype(jnp.int32)
        id_table = sorted_ids.reshape(TOP, TOKENS).T
        id_table = id_table[jax.random.permutation(key_rows, TOKENS)]
        row_shift = jax.random.randint(key_shift, (TOKENS, 1), 0, TOP)
        col_order = (jnp.arange(TOP)[None, :] + row_shift) % TOP
        return jnp.take_along_axis(id_table, col_order, axis=1)

    return jax.vmap(one_device)(jax.random.split(key_dev, GROUP)).reshape(GROUP * TOKENS, TOP)


def setup_inputs(seed: int = 0, part: int = 0) -> dict:
    root_key = jax.random.key(seed)
    shared_keys = jax.random.split(root_key, 6)
    part_keys = jax.random.split(jax.random.fold_in(root_key, part), 6)
    row_total = GROUP * TOKENS
    gate_scale = 1.5 / TOP ** 0.5
    in_scale = D ** -0.5
    mid_scale = FF ** -0.5
    x_in = jax.random.normal(part_keys[0], (row_total, D), jnp.float32).astype(jnp.bfloat16)
    idx_a = draw_routing(part_keys[1])
    idx_b = draw_routing(part_keys[2])
    gate_a = (0.5 + jax.random.uniform(part_keys[3], (row_total, TOP), jnp.float32)) * gate_scale
    gate_b = (0.5 + jax.random.uniform(part_keys[4], (row_total, TOP), jnp.float32)) * gate_scale
    dy_out = jax.random.normal(part_keys[5], (row_total, D), jnp.float32).astype(jnp.bfloat16)
    w1_a = (jax.random.normal(shared_keys[0], (EXPERTS, D, FF), jnp.float32) * in_scale).astype(jnp.bfloat16)
    w3_a = (jax.random.normal(shared_keys[1], (EXPERTS, D, FF), jnp.float32) * in_scale).astype(jnp.bfloat16)
    w2_a = (jax.random.normal(shared_keys[2], (EXPERTS, FF, D), jnp.float32) * mid_scale).astype(jnp.bfloat16)
    w1_b = (jax.random.normal(shared_keys[3], (EXPERTS, D, FF), jnp.float32) * in_scale).astype(jnp.bfloat16)
    w3_b = (jax.random.normal(shared_keys[4], (EXPERTS, D, FF), jnp.float32) * in_scale).astype(jnp.bfloat16)
    w2_b = (jax.random.normal(shared_keys[5], (EXPERTS, FF, D), jnp.float32) * mid_scale).astype(jnp.bfloat16)
    return {"x_in": x_in, "idx_a": idx_a, "idx_b": idx_b, "gate_a": gate_a, "gate_b": gate_b, "dy_out": dy_out, "w1_a": w1_a, "w3_a": w3_a, "w2_a": w2_a, "w1_b": w1_b, "w3_b": w3_b, "w2_b": w2_b}


def expert_forward(u_rows, w_gate, w_up, w_down):
    pre_gate = jnp.dot(u_rows, w_gate, preferred_element_type=jnp.float32)
    pre_up = jnp.dot(u_rows, w_up, preferred_element_type=jnp.float32)
    hidden = (jax.nn.silu(pre_gate) * pre_up).astype(jnp.bfloat16)
    out_rows = jnp.dot(hidden, w_down, preferred_element_type=jnp.float32).astype(jnp.bfloat16)
    return pre_gate, pre_up, hidden, out_rows


def device_slots(flat_ids):
    onehot = (flat_ids[:, None] == jnp.arange(EXPERTS, dtype=jnp.int32)[None, :]).astype(jnp.int32)
    return jnp.sum(jnp.cumsum(onehot, axis=0) * onehot, axis=1) - 1


def expert_table(ids):
    per_device = ids.reshape(GROUP, TOKENS * TOP)
    pair_slot = lax.map(device_slots, per_device)
    expert_row = jnp.arange(GROUP, dtype=jnp.int32)[:, None] * CAP + pair_slot
    pair_ids = jnp.arange(GROUP * TOKENS * TOP, dtype=jnp.int32).reshape(GROUP, TOKENS * TOP)
    empty_pair = GROUP * TOKENS * TOP
    return jnp.full((EXPERTS, GROUP * CAP), empty_pair, jnp.int32).at[per_device, expert_row].set(pair_ids)


def layer_forward(x_rows, gates, table, w_gate, w_up, w_down):
    x_pad = jnp.concatenate([x_rows, jnp.zeros((1, D), x_rows.dtype)])
    gate_pad = jnp.concatenate([gates.reshape(-1), jnp.zeros((1,), gates.dtype)])

    def expert_step(out_acc, step_in):
        pair_ids, gate_w, up_w, down_w = step_in
        tok_index = pair_ids // TOP
        out_rows = expert_forward(x_pad[tok_index], gate_w, up_w, down_w)[3]
        weighted = gate_pad[pair_ids][:, None] * out_rows.astype(jnp.float32)
        return out_acc.at[tok_index].add(weighted), None

    out_acc = jnp.zeros((GROUP * TOKENS + 1, D), jnp.float32)
    out_acc = lax.scan(expert_step, out_acc, (table, w_gate, w_up, w_down))[0]
    return (x_rows.astype(jnp.float32) + out_acc[:-1]).astype(jnp.bfloat16)


def layer_backward(dy_rows, x_rows, gates, table, w_gate, w_up, w_down):
    x_pad = jnp.concatenate([x_rows, jnp.zeros((1, D), x_rows.dtype)])
    dy_pad = jnp.concatenate([dy_rows, jnp.zeros((1, D), dy_rows.dtype)])
    gate_pad = jnp.concatenate([gates.reshape(-1), jnp.zeros((1,), gates.dtype)])

    def expert_step(carry_in, step_in):
        dx_acc, dgate_acc = carry_in
        pair_ids, gate_w, up_w, down_w = step_in
        tok_index = pair_ids // TOP
        u_rows = x_pad[tok_index]
        dy_exp = dy_pad[tok_index].astype(jnp.float32)
        pre_gate, pre_up, hidden, out_rows = expert_forward(u_rows, gate_w, up_w, down_w)
        dgate_rows = jnp.sum(dy_exp * out_rows.astype(jnp.float32), axis=1)
        d_out = (gate_pad[pair_ids][:, None] * dy_exp).astype(jnp.bfloat16)
        dw_down = jnp.dot(hidden.T, d_out, preferred_element_type=jnp.float32)
        d_hidden = jnp.dot(d_out, down_w.T, preferred_element_type=jnp.float32)
        gate_sig = jax.nn.sigmoid(pre_gate)
        d_pre_gate = (d_hidden * pre_up * gate_sig * (1.0 + pre_gate * (1.0 - gate_sig))).astype(jnp.bfloat16)
        d_pre_up = (d_hidden * jax.nn.silu(pre_gate)).astype(jnp.bfloat16)
        dw_gate = jnp.dot(u_rows.T, d_pre_gate, preferred_element_type=jnp.float32)
        dw_up = jnp.dot(u_rows.T, d_pre_up, preferred_element_type=jnp.float32)
        du_rows = (jnp.dot(d_pre_gate, gate_w.T, preferred_element_type=jnp.float32) + jnp.dot(d_pre_up, up_w.T, preferred_element_type=jnp.float32)).astype(jnp.bfloat16)
        dx_acc = dx_acc.at[tok_index].add(du_rows.astype(jnp.float32))
        dgate_acc = dgate_acc.at[pair_ids].set(dgate_rows)
        return (dx_acc, dgate_acc), (dw_gate, dw_up, dw_down)

    dx_acc = jnp.zeros((GROUP * TOKENS + 1, D), jnp.float32)
    dgate_acc = jnp.zeros((GROUP * TOKENS * TOP + 1,), jnp.float32)
    (dx_acc, dgate_acc), grads = lax.scan(expert_step, (dx_acc, dgate_acc), (table, w_gate, w_up, w_down))
    dx_rows = (dy_rows.astype(jnp.float32) + dx_acc[:-1]).astype(jnp.bfloat16)
    return dx_rows, dgate_acc[:-1].reshape(GROUP * TOKENS, TOP), grads


def reference(x_in, idx_a, idx_b, gate_a, gate_b, dy_out, w1_a, w3_a, w2_a, w1_b, w3_b, w2_b):
    table_a = expert_table(idx_a)
    table_b = expert_table(idx_b)
    x_mid = layer_forward(x_in, gate_a, table_a, w1_a, w3_a, w2_a)
    x_out = layer_forward(x_mid, gate_b, table_b, w1_b, w3_b, w2_b)
    dx_mid, dgate_b, grads_b = layer_backward(dy_out, x_mid, gate_b, table_b, w1_b, w3_b, w2_b)
    dx_in, dgate_a, grads_a = layer_backward(dx_mid, x_in, gate_a, table_a, w1_a, w3_a, w2_a)
    return (x_out, dx_in, grads_a[0], grads_a[1], grads_a[2], grads_b[0], grads_b[1], grads_b[2], dgate_a, dgate_b)
```

```python
import jax
import jax.numpy as jnp
from jax import lax
from jax.sharding import PartitionSpec as P

CAP_FACTOR = 4
F32 = jnp.float32
BF16 = jnp.bfloat16


def pair_rows(ids, capacity):
    flat = ids.reshape(-1)
    pair = jnp.arange(flat.shape[0], dtype=jnp.int32)
    earlier = (flat[None, :] == flat[:, None]) & (pair[None, :] < pair[:, None])
    slot = jnp.sum(earlier.astype(jnp.int32), axis=1)
    return (flat * capacity + slot).reshape(ids.shape)


def slot_tables(rows, gates, total):
    tok_dev = rows.shape[0]
    hit = rows[:, :, None] == jnp.arange(total, dtype=jnp.int32)[None, None, :]
    token = jnp.sum(jnp.where(hit, jnp.arange(tok_dev, dtype=F32)[:, None, None] - tok_dev, 0.0), axis=(0, 1)) + tok_dev
    gate = jnp.sum(jnp.where(hit, gates[:, :, None], 0.0), axis=(0, 1))
    return token, gate


def pair_weight(rows, gates, total):
    hit = rows[:, :, None] == jnp.arange(total, dtype=jnp.int32)[None, None, :]
    return jnp.sum(jnp.where(hit, gates[:, :, None], 0.0), axis=1)


def split3(w):
    hi = lax.reduce_precision(w, 8, 7)
    mid = lax.reduce_precision(w - hi, 8, 7)
    low = w - hi - mid
    return jnp.concatenate([hi.astype(BF16), mid.astype(BF16), low.astype(BF16)], axis=0)


def pick_rows(all_rows, token, own):
    n_group, tok_dev, width = all_rows.shape
    pick = (token[:, :, None] == jnp.arange(tok_dev, dtype=F32)[None, None, :]).astype(BF16)
    rows = jnp.einsum("srt,std->srd", pick, all_rows, preferred_element_type=F32).astype(BF16)
    rows = rows.reshape(n_group, own, -1, width).transpose(1, 0, 2, 3)
    return rows.reshape(own, -1, width)


def home_order(rows, n_group):
    own, count, width = rows.shape
    rows = rows.reshape(own, n_group, count // n_group, width).transpose(1, 0, 2, 3)
    return rows.reshape(n_group, -1, width)


def expert_forward(u_rows, w_gate, w_up, w_down):
    pre_gate = jnp.einsum("erd,edf->erf", u_rows, w_gate, preferred_element_type=F32)
    pre_up = jnp.einsum("erd,edf->erf", u_rows, w_up, preferred_element_type=F32)
    hidden = (jax.nn.silu(pre_gate) * pre_up).astype(BF16)
    out_rows = jnp.einsum("erf,efd->erd", hidden, w_down, preferred_element_type=F32).astype(BF16)
    return pre_gate, pre_up, hidden, out_rows


def expert_backward(u_rows, dy_rows, gate_rows, w_gate, w_up, w_down):
    pre_gate, pre_up, hidden, out_rows = expert_forward(u_rows, w_gate, w_up, w_down)
    dgate_rows = jnp.einsum("erd,erd->er", dy_rows, out_rows, preferred_element_type=F32)
    d_out = (gate_rows[:, :, None] * dy_rows).astype(BF16)
    dw_down = jnp.einsum("erf,erd->efd", hidden, d_out, preferred_element_type=F32)
    d_hidden = jnp.einsum("erd,efd->erf", d_out, w_down, preferred_element_type=F32)
    gate_sig = jax.nn.sigmoid(pre_gate)
    d_pre_gate = (d_hidden * pre_up * gate_sig * (1.0 + pre_gate * (1.0 - gate_sig))).astype(BF16)
    d_pre_up = (d_hidden * jax.nn.silu(pre_gate)).astype(BF16)
    dw_gate = jnp.einsum("erd,erf->edf", u_rows, d_pre_gate, preferred_element_type=F32)
    dw_up = jnp.einsum("erd,erf->edf", u_rows, d_pre_up, preferred_element_type=F32)
    du_rows = (jnp.einsum("erf,edf->erd", d_pre_gate, w_gate, preferred_element_type=F32) + jnp.einsum("erf,edf->erd", d_pre_up, w_up, preferred_element_type=F32)).astype(BF16)
    return du_rows, dgate_rows, dw_gate, dw_up, dw_down


def solution(mesh):
    n_group = mesh.shape["ep"]
    tok_spec = P(("dp", "ep"))
    w_spec = P("ep")

    def device_program(x_in, idx_a, idx_b, gate_a, gate_b, dy_out, w1_a, w3_a, w2_a, w1_b, w3_b, w2_b):
        tok_dev, top_k = idx_a.shape
        width = x_in.shape[1]
        own = w1_a.shape[0]
        capacity = CAP_FACTOR * tok_dev * top_k // (own * n_group)
        total = own * n_group * capacity
        block = own * capacity

        rows_a = pair_rows(idx_a, capacity)
        rows_b = pair_rows(idx_b, capacity)
        tables = slot_tables(rows_a, gate_a, total) + slot_tables(rows_b, gate_b, total)
        table = jnp.concatenate([t.reshape(n_group, block) for t in tables], axis=1)
        table = lax.all_to_all(table, "ep", 0, 0, tiled=True)
        token_a, far_gate_a, token_b, far_gate_b = jnp.split(table, 4, axis=1)
        weight_a = split3(pair_weight(rows_a, gate_a, total))
        weight_b = split3(pair_weight(rows_b, gate_b, total))
        ones = jnp.ones_like(gate_a)
        pick_a = pair_weight(rows_a, ones, total).astype(BF16)
        pick_b = pair_weight(rows_b, ones, total).astype(BF16)

        def gather(rows):
            return lax.all_gather(rows, "ep", axis=0, tiled=False)

        def send_back(rows):
            back = lax.all_to_all(home_order(rows, n_group), "ep", 0, 0, tiled=True)
            return back.reshape(total, width)

        def combine(x_rows, back, weight):
            branch = jnp.dot(weight, back, preferred_element_type=F32).reshape(3, tok_dev, width)
            branch = branch[0] + (branch[1] + branch[2])
            return (x_rows.astype(F32) + branch).astype(BF16)

        def layer_backward(dy_rows, dy_all, x_all, token, far_gate, pick, w_gate, w_up, w_down):
            gates = far_gate.reshape(n_group, own, capacity).transpose(1, 0, 2).reshape(own, -1)
            u_rows = pick_rows(x_all, token, own)
            dy_sent = pick_rows(dy_all, token, own)
            du_rows, dgate_rows, dw_gate, dw_up, dw_down = expert_backward(u_rows, dy_sent, gates, w_gate, w_up, w_down)
            branch = jnp.dot(pick, send_back(du_rows), preferred_element_type=F32)
            dx_rows = (dy_rows.astype(F32) + branch).astype(BF16)
            return dx_rows, dgate_rows, (dw_gate, dw_up, dw_down)

        def dgate_home(dgate_rows, rows):
            back = lax.all_to_all(home_order(dgate_rows[:, :, None], n_group).reshape(n_group, block), "ep", 0, 0, tiled=True)
            hit = rows[:, :, None] == jnp.arange(total, dtype=jnp.int32)[None, None, :]
            return jnp.sum(jnp.where(hit, back.reshape(1, 1, total), 0.0), axis=2)

        x_all = gather(x_in)
        dy_all_b = gather(dy_out)
        out_a = expert_forward(pick_rows(x_all, token_a, own), w1_a, w3_a, w2_a)[3]
        x_mid = combine(x_in, send_back(out_a), weight_a)
        mid_all = gather(x_mid)
        out_b = expert_forward(pick_rows(mid_all, token_b, own), w1_b, w3_b, w2_b)[3]
        x_out = combine(x_mid, send_back(out_b), weight_b)
        mid_keep, dy_all_b, out_b = lax.optimization_barrier((mid_all, dy_all_b, out_b))
        dx_mid, dgate_rows_b, grads_b = layer_backward(dy_out, dy_all_b, mid_keep, token_b, far_gate_b, pick_b, w1_b, w3_b, w2_b)
        x_again, _ = lax.optimization_barrier((x_in, out_b))
        again_all = gather(x_again)
        dy_all_a = gather(dx_mid)
        dx_in, dgate_rows_a, grads_a = layer_backward(dx_mid, dy_all_a, again_all, token_a, far_gate_a, pick_a, w1_a, w3_a, w2_a)
        dgate_b = dgate_home(dgate_rows_b, rows_b)
        dgate_a = dgate_home(dgate_rows_a, rows_a)
        return (x_out, dx_in) + grads_a + grads_b + (dgate_a, dgate_b)

    return jax.shard_map(device_program, mesh=mesh, in_specs=(tok_spec,) * 6 + (w_spec,) * 6, out_specs=(tok_spec,) * 10, check_vma=False)
```

```python
import functools

import jax
import jax.numpy as jnp
from jax import lax
from jax.experimental import pallas as pl
from jax.experimental.pallas import tpu as pltpu
from jax.sharding import PartitionSpec as P

CAP_FACTOR = 4
F32 = jnp.float32
BF16 = jnp.bfloat16


def pair_rows(ids, capacity):
    flat = ids.reshape(-1)
    pair = jnp.arange(flat.shape[0], dtype=jnp.int32)
    earlier = (flat[None, :] == flat[:, None]) & (pair[None, :] < pair[:, None])
    slot = jnp.sum(earlier.astype(jnp.int32), axis=1)
    return (flat * capacity + slot).reshape(ids.shape)


def pair_weight(rows, gates, total):
    hit = rows[:, :, None] == jnp.arange(total, dtype=jnp.int32)[None, None, :]
    return jnp.sum(jnp.where(hit, gates[:, :, None], 0.0), axis=1)


def split3(w):
    hi = lax.reduce_precision(w, 8, 7)
    mid = lax.reduce_precision(w - hi, 8, 7)
    low = w - hi - mid
    return jnp.concatenate([hi.astype(BF16), mid.astype(BF16), low.astype(BF16)], axis=0)


SIDE = 4


def send_kernel(own, capacity, x_ref, code_ref, u_ref, held, local_sem, send_sem, recv_sem):
    me = lax.axis_index("ep")
    core = lax.rem(me, 2)
    chip = lax.div(me, 2)
    at = (lax.rem(chip, SIDE), lax.rem(lax.div(chip, SIDE), SIDE), lax.div(chip, SIDE * SIDE))
    third = x_ref.shape[0] // 3
    half = third // 2

    def device(dim, step):
        c = list(at)
        c[dim] = lax.rem(c[dim] + step + SIDE, SIDE)
        return ((c[2] * SIDE + c[1]) * SIDE + c[0]) * 2 + core

    partner = chip * 2 + (1 - core)

    def region(part, pos, first, count):
        idx = [pos[d] if d in pos else at[d] for d in range(3)]
        idx = [pl.ds(0, SIDE) if i is None else i for i in idx]
        return held.at[core, idx[2], idx[1], idx[0], pl.ds(part * third + first, count), :]

    copies = {}

    def start(key, ref, to):
        n = len(copies)
        copies[key] = pltpu.make_async_remote_copy(src_ref=ref, dst_ref=ref, send_sem=send_sem.at[n], recv_sem=recv_sem.at[n], device_id={"ep": to}, device_id_type=pl.DeviceIdType.MESH)
        copies[key].start()

    mine = pltpu.make_async_copy(x_ref, held.at[core, at[2], at[1], at[0]], local_sem)
    mine.start()
    barrier = pltpu.get_barrier_semaphore()
    for dim in range(3):
        for step in (1, -1):
            pl.semaphore_signal(barrier, inc=1, device_id={"ep": device(dim, step)}, device_id_type=pl.DeviceIdType.MESH)
    pl.semaphore_signal(barrier, inc=1, device_id={"ep": partner}, device_id_type=pl.DeviceIdType.MESH)
    mine.wait()
    pl.semaphore_wait(barrier, 7)

    def dims(part):
        return part, (part + 1) % 3, (part + 2) % 3

    def shift(dim, step):
        return lax.rem(at[dim] + step + SIDE, SIDE)

    def row_of(part, b, c, first=0, count=third):
        d1, d2, d3 = dims(part)
        return region(part, {d1: None, d2: shift(d2, b), d3: shift(d3, c)}, first, count)

    def across(part, b, c):
        start(("d2d", part, b, c), row_of(part, b, c), partner)

    def whole_row(part, b):
        d3 = dims(part)[2]
        for way in (1, -1):
            start(("m3", part, b, way), row_of(part, b, 0), device(d3, way))
        across(part, b, 0)

    def pass_on(part, b, way):
        d3 = dims(part)[2]
        copies["m3", part, b, way].wait_recv()
        start(("f3", part, b, way), row_of(part, b, -way, 0 if way == 1 else half, half), device(d3, way))
        across(part, b, -way)

    def last_row(part, b):
        for way in (1, -1):
            copies["f3", part, b, way].wait_recv()
        across(part, b, 2)

    for part in range(3):
        d1 = dims(part)[0]
        for way in (1, -1):
            start(("m1", part, way), region(part, {}, 0, third), device(d1, way))
    for part in range(3):
        d1 = dims(part)[0]
        for way in (1, -1):
            copies["m1", part, way].wait_recv()
            start(("f1", part, way), region(part, {d1: shift(d1, -way)}, 0 if way == 1 else half, half), device(d1, way))
    for part in range(3):
        d2 = dims(part)[1]
        for way in (1, -1):
            copies["f1", part, way].wait_recv()
        for way in (1, -1):
            start(("m2", part, way), row_of(part, 0, 0), device(d2, way))
        whole_row(part, 0)
    for part in range(3):
        d2 = dims(part)[1]
        for way in (1, -1):
            copies["m2", part, way].wait_recv()
            start(("f2", part, way), row_of(part, -way, 0, 0 if way == 1 else half, half), device(d2, way))
            whole_row(part, -way)
    for part in range(3):
        for way in (1, -1):
            pass_on(part, 0, way)
    for part in range(3):
        for way in (1, -1):
            copies["f2", part, way].wait_recv()
        whole_row(part, 2)
    for b in (-1, 1):
        for part in range(3):
            for way in (1, -1):
                pass_on(part, b, way)
    for part in range(3):
        last_row(part, 0)
    for part in range(3):
        for way in (1, -1):
            pass_on(part, 2, way)
    for b in (-1, 1, 2):
        for part in range(3):
            last_row(part, b)
    for key, copy in copies.items():
        if key[0] == "d2d":
            copy.wait_recv()

    block = own * capacity
    slot = lax.broadcasted_iota(jnp.int32, (block, x_ref.shape[0]), 0) + me * block
    chips = SIDE ** 3
    group = 4

    def pick(step, carry):
        for k in range(group):
            place = step * group + k
            rows = []
            for c in range(2):
                code = code_ref[place * 2 + c]
                hit = code[0:1, :] == slot
                for j in range(1, code.shape[0]):
                    hit = hit | (code[j:j + 1, :] == slot)
                tokens = held[c, lax.div(place, SIDE * SIDE), lax.rem(lax.div(place, SIDE), SIDE), lax.rem(place, SIDE)]
                onehot = jnp.where(hit, 1.0, 0.0).astype(BF16)
                rows.append(jnp.dot(onehot, tokens, preferred_element_type=F32))
            for e in range(own):
                both = jnp.concatenate([r[e * capacity:(e + 1) * capacity] for r in rows], axis=0)
                u_ref[e, pl.ds(pl.multiple_of(place * 2 * capacity, 2 * capacity), 2 * capacity), :] = both.astype(BF16)
        return carry

    lax.fori_loop(0, chips // group, pick, 0)
    for copy in copies.values():
        copy.wait_send()


def send_rows(x, code, own, capacity, call_id):
    tok_dev, width = x.shape
    n_group = code.shape[0]
    count = 120
    return pl.pallas_call(
        functools.partial(send_kernel, own, capacity),
        out_shape=jax.ShapeDtypeStruct((own, n_group * capacity, width), x.dtype),
        in_specs=[pl.BlockSpec(memory_space=pl.ANY), pl.BlockSpec(memory_space=pltpu.VMEM)],
        out_specs=pl.BlockSpec(memory_space=pltpu.VMEM),
        scratch_shapes=[
            pltpu.VMEM((2, SIDE, SIDE, SIDE, tok_dev, width), x.dtype),
            pltpu.SemaphoreType.DMA,
            pltpu.SemaphoreType.DMA((count,)),
            pltpu.SemaphoreType.DMA((count,)),
        ],
        compiler_params=pltpu.CompilerParams(collective_id=call_id, has_side_effects=True, vmem_limit_bytes=40 * 1024 * 1024),
        cost_estimate=pl.CostEstimate(flops=3 * 10**10, bytes_accessed=n_group * tok_dev * width * 2, transcendentals=0),
        name=f"send_rows_{call_id}",
    )(x, code)


def home_order(rows, n_group):
    own, count, width = rows.shape
    rows = rows.reshape(own, n_group, count // n_group, width).transpose(1, 0, 2, 3)
    return rows.reshape(n_group, -1, width)


def expert_forward(u_rows, w_gate, w_up, w_down):
    pre_gate = jnp.einsum("erd,edf->erf", u_rows, w_gate, preferred_element_type=F32)
    pre_up = jnp.einsum("erd,edf->erf", u_rows, w_up, preferred_element_type=F32)
    hidden = (jax.nn.silu(pre_gate) * pre_up).astype(BF16)
    out_rows = jnp.einsum("erf,efd->erd", hidden, w_down, preferred_element_type=F32).astype(BF16)
    return pre_gate, pre_up, hidden, out_rows


def expert_backward(u_rows, dy_rows, gate_rows, w_gate, w_up, w_down):
    pre_gate, pre_up, hidden, out_rows = expert_forward(u_rows, w_gate, w_up, w_down)
    dgate_rows = jnp.einsum("erd,erd->er", dy_rows, out_rows, preferred_element_type=F32)
    d_out = (gate_rows[:, :, None] * dy_rows).astype(BF16)
    dw_down = jnp.einsum("erf,erd->efd", hidden, d_out, preferred_element_type=F32)
    d_hidden = jnp.einsum("erd,efd->erf", d_out, w_down, preferred_element_type=F32)
    gate_sig = jax.nn.sigmoid(pre_gate)
    d_pre_gate = (d_hidden * pre_up * gate_sig * (1.0 + pre_gate * (1.0 - gate_sig))).astype(BF16)
    d_pre_up = (d_hidden * jax.nn.silu(pre_gate)).astype(BF16)
    dw_gate = jnp.einsum("erd,erf->edf", u_rows, d_pre_gate, preferred_element_type=F32)
    dw_up = jnp.einsum("erd,erf->edf", u_rows, d_pre_up, preferred_element_type=F32)
    du_rows = (jnp.einsum("erf,edf->erd", d_pre_gate, w_gate, preferred_element_type=F32) + jnp.einsum("erf,edf->erd", d_pre_up, w_up, preferred_element_type=F32)).astype(BF16)
    return du_rows, dgate_rows, dw_gate, dw_up, dw_down


def solution(mesh):
    n_group = mesh.shape["ep"]
    tok_spec = P(("dp", "ep"))
    w_spec = P("ep")

    def device_program(x_in, idx_a, idx_b, gate_a, gate_b, dy_out, w1_a, w3_a, w2_a, w1_b, w3_b, w2_b):
        tok_dev, top_k = idx_a.shape
        width = x_in.shape[1]
        own = w1_a.shape[0]
        capacity = CAP_FACTOR * tok_dev * top_k // (own * n_group)
        total = own * n_group * capacity
        block = own * capacity

        rows_a = pair_rows(idx_a, capacity)
        rows_b = pair_rows(idx_b, capacity)
        codes = jnp.stack([rows_a.T, rows_b.T])
        gates = jnp.stack([gate_a.T, gate_b.T])
        table = jnp.concatenate([codes.astype(F32), gates], axis=0)
        table = lax.all_gather(table, "ep", axis=0, tiled=False)
        code_a, code_b = table[:, 0].astype(jnp.int32), table[:, 1].astype(jnp.int32)
        mine = (lax.axis_index("ep") * block + jnp.arange(block, dtype=jnp.int32)).astype(F32)

        def far_gates(layer):
            hit = table[:, layer, None] == mine[None, :, None, None]
            gates = jnp.sum(jnp.where(hit, table[:, 2 + layer, None], 0.0), axis=(2, 3))
            return gates.reshape(n_group, own, capacity).transpose(1, 0, 2).reshape(own, -1)

        far_gate_a, far_gate_b = far_gates(0), far_gates(1)
        weight_a = split3(pair_weight(rows_a, gate_a, total))
        weight_b = split3(pair_weight(rows_b, gate_b, total))
        ones = jnp.ones_like(gate_a)
        pick_a = pair_weight(rows_a, ones, total).astype(BF16)
        pick_b = pair_weight(rows_b, ones, total).astype(BF16)

        def send_back(rows):
            back = lax.all_to_all(home_order(rows, n_group), "ep", 0, 0, tiled=True)
            return back.reshape(total, width)

        def combine(x_rows, back, weight):
            branch = jnp.dot(weight, back, preferred_element_type=F32).reshape(3, tok_dev, width)
            branch = branch[0] + (branch[1] + branch[2])
            return (x_rows.astype(F32) + branch).astype(BF16)

        def layer_backward(dy_rows, dy_sent, u_rows, gates, pick, w_gate, w_up, w_down):
            du_rows, dgate_rows, dw_gate, dw_up, dw_down = expert_backward(u_rows, dy_sent, gates, w_gate, w_up, w_down)
            branch = jnp.dot(pick, send_back(du_rows), preferred_element_type=F32)
            dx_rows = (dy_rows.astype(F32) + branch).astype(BF16)
            return dx_rows, dgate_rows, (dw_gate, dw_up, dw_down)

        def dgate_home(dgate_rows, rows):
            back = lax.all_to_all(home_order(dgate_rows[:, :, None], n_group).reshape(n_group, block), "ep", 0, 0, tiled=True)
            hit = rows[:, :, None] == jnp.arange(total, dtype=jnp.int32)[None, None, :]
            return jnp.sum(jnp.where(hit, back.reshape(1, 1, total), 0.0), axis=2)

        u_a = send_rows(x_in, code_a, own, capacity, 0)
        out_a = expert_forward(u_a, w1_a, w3_a, w2_a)[3]
        back_a = send_back(out_a)
        dy_b = send_rows(dy_out, code_b, own, capacity, 1)
        x_mid = combine(x_in, back_a, weight_a)
        u_b = send_rows(x_mid, code_b, own, capacity, 2)
        out_b = expert_forward(u_b, w1_b, w3_b, w2_b)[3]
        x_out = combine(x_mid, send_back(out_b), weight_b)
        u_keep, dy_b, _ = lax.optimization_barrier((u_b, dy_b, out_b))
        dx_mid, dgate_rows_b, grads_b = layer_backward(dy_out, dy_b, u_keep, far_gate_b, pick_b, w1_b, w3_b, w2_b)
        x_again, _ = lax.optimization_barrier((x_in, out_b))
        u_again = send_rows(x_again, code_a, own, capacity, 3)
        dy_a = send_rows(dx_mid, code_a, own, capacity, 4)
        dx_in, dgate_rows_a, grads_a = layer_backward(dx_mid, dy_a, u_again, far_gate_a, pick_a, w1_a, w3_a, w2_a)
        dgate_b = dgate_home(dgate_rows_b, rows_b)
        dgate_a = dgate_home(dgate_rows_a, rows_a)
        return (x_out, dx_in) + grads_a + grads_b + (dgate_a, dgate_b)

    return jax.shard_map(device_program, mesh=mesh, in_specs=(tok_spec,) * 6 + (w_spec,) * 6, out_specs=(tok_spec,) * 10, check_vma=False)
```

```python
import functools

import jax
import jax.numpy as jnp
from jax import lax
from jax.experimental import pallas as pl
from jax.experimental.pallas import tpu as pltpu
from jax.sharding import PartitionSpec as P

CAP_FACTOR = 4
F32 = jnp.float32
BF16 = jnp.bfloat16


def pair_rows(ids, capacity):
    flat = ids.reshape(-1)
    pair = jnp.arange(flat.shape[0], dtype=jnp.int32)
    earlier = (flat[None, :] == flat[:, None]) & (pair[None, :] < pair[:, None])
    slot = jnp.sum(earlier.astype(jnp.int32), axis=1)
    return (flat * capacity + slot).reshape(ids.shape)


def pair_weight(rows, gates, total):
    hit = rows[:, :, None] == jnp.arange(total, dtype=jnp.int32)[None, None, :]
    return jnp.sum(jnp.where(hit, gates[:, :, None], 0.0), axis=1)


def split3(w):
    hi = lax.reduce_precision(w, 8, 7)
    mid = lax.reduce_precision(w - hi, 8, 7)
    low = w - hi - mid
    return jnp.concatenate([hi.astype(BF16), mid.astype(BF16), low.astype(BF16)], axis=0)


SIDE = 4


def send_kernel(own, capacity, layer, plus, first, *refs):
    if first:
        x_ref, tile_ref, u_ref, table_ref, held, local_sem, send_sem, recv_sem, tiles = refs
    else:
        x_ref, table_ref, u_ref, held, local_sem, send_sem, recv_sem = refs
        tiles = table_ref
    me = lax.axis_index("ep")
    core = lax.rem(me, 2)
    chip = lax.div(me, 2)
    at = (lax.rem(chip, SIDE), lax.rem(lax.div(chip, SIDE), SIDE), lax.div(chip, SIDE * SIDE))
    third = x_ref.shape[0] // 3
    spans = {1: (0, plus), -1: (plus, third - plus)}

    def device(dim, step):
        c = list(at)
        c[dim] = lax.rem(c[dim] + step + SIDE, SIDE)
        return ((c[2] * SIDE + c[1]) * SIDE + c[0]) * 2 + core

    partner = chip * 2 + (1 - core)

    def region(part, pos, span):
        idx = [pos[d] if d in pos else at[d] for d in range(3)]
        idx = [pl.ds(0, SIDE) if i is None else i for i in idx]
        where = (core, idx[2], idx[1], idx[0])
        return held.at[where + (pl.ds(part * third + span[0], span[1]),)], where + (part,)

    copies = {}

    def start(key, refs, to, with_tile):
        for kind, ref in (("x", refs[0]), ("t", tiles.at[refs[1]])):
            if kind == "t" and not (first and with_tile) or ref.shape[-2] == 0:
                continue
            n = len(copies)
            copy = pltpu.make_async_remote_copy(src_ref=ref, dst_ref=ref, send_sem=send_sem.at[n], recv_sem=recv_sem.at[n], device_id={"ep": to}, device_id_type=pl.DeviceIdType.MESH)
            copy.start()
            copies[key + (kind,)] = copy

    def arrive(*key):
        for kind in ("x", "t"):
            if key + (kind,) in copies:
                copies[key + (kind,)].wait_recv()

    mine = pltpu.make_async_copy(x_ref, held.at[core, at[2], at[1], at[0]], local_sem)
    mine.start()
    if first:
        own_tile = pltpu.make_async_copy(tile_ref, tiles.at[core, at[2], at[1], at[0]], send_sem.at[0])
        own_tile.start()
        own_tile.wait()
    barrier = pltpu.get_barrier_semaphore()
    for dim in range(3):
        for step in (1, -1):
            pl.semaphore_signal(barrier, inc=1, device_id={"ep": device(dim, step)}, device_id_type=pl.DeviceIdType.MESH)
    pl.semaphore_signal(barrier, inc=1, device_id={"ep": partner}, device_id_type=pl.DeviceIdType.MESH)
    mine.wait()
    pl.semaphore_wait(barrier, 7)

    def dims(part):
        return part, (part + 1) % 3, (part + 2) % 3

    def shift(dim, step):
        return lax.rem(at[dim] + step + SIDE, SIDE)

    whole = (0, third)

    def row_of(part, b, c, span=whole):
        d1, d2, d3 = dims(part)
        return region(part, {d1: None, d2: shift(d2, b), d3: shift(d3, c)}, span)

    def across(part, b, c):
        start(("d2d", part, b, c), row_of(part, b, c), partner, True)

    def whole_row(part, b):
        d3 = dims(part)[2]
        for way in (1, -1):
            start(("m3", part, b, way), row_of(part, b, 0), device(d3, way), True)
        across(part, b, 0)

    def pass_on(part, b, way):
        d3 = dims(part)[2]
        arrive("m3", part, b, way)
        start(("f3", part, b, way), row_of(part, b, -way, spans[way]), device(d3, way), way == -1)
        across(part, b, -way)

    def last_row(part, b):
        for way in (1, -1):
            arrive("f3", part, b, way)
        across(part, b, 2)

    block = own * capacity
    slot = lax.broadcasted_iota(jnp.int32, (block, 128), 0) + me * block
    tok_dev = x_ref.shape[0]

    def pick(offsets):
        x, y, z = (lax.rem(at[d] + offsets[d] + SIDE, SIDE) for d in range(3))
        rows = []
        for c in range(2):
            code = tiles[c, z, y, x, layer].astype(jnp.int32)
            hit = code[0:1, :] == slot
            for j in range(1, code.shape[0]):
                hit = hit | (code[j:j + 1, :] == slot)
            onehot = jnp.where(hit, 1.0, 0.0)[:, :tok_dev].astype(BF16)
            rows.append(jnp.dot(onehot, held[c, z, y, x], preferred_element_type=F32))
        place = ((z * SIDE + y) * SIDE + x) * 2 * capacity
        for e in range(own):
            both = jnp.concatenate([r[e * capacity:(e + 1) * capacity] for r in rows], axis=0)
            u_ref[e, pl.ds(pl.multiple_of(place, 2 * capacity), 2 * capacity), :] = both.astype(BF16)

    def near_rows(step, carry):
        for k in (-1, 0, 1):
            pick((k, lax.rem(step, 3) - 1, lax.div(step, 3) - 1))
        return carry

    def far_rows(step, carry):
        b, c = lax.rem(step, 3) - 1, lax.div(step, 3) - 1
        for offsets in ((2, b, c), (b, 2, c), (b, c, 2)):
            pick(offsets)
        return carry

    def farthest_rows(step, carry):
        for offsets in ((2, 2, step - 1), (2, step - 1, 2), (step - 1, 2, 2)):
            pick(offsets)
        return carry

    def arrive_across(wanted):
        for part in range(3):
            for b in (0, -1, 1, 2):
                for c in (0, -1, 1, 2):
                    if (b == 2) + (c == 2) == wanted:
                        arrive("d2d", part, b, c)

    for part in range(3):
        d1 = dims(part)[0]
        for way in (1, -1):
            start(("m1", part, way), region(part, {}, whole), device(d1, way), True)
    for part in range(3):
        d1 = dims(part)[0]
        for way in (1, -1):
            arrive("m1", part, way)
            start(("f1", part, way), region(part, {d1: shift(d1, -way)}, spans[way]), device(d1, way), way == -1)
    for part in range(3):
        d2 = dims(part)[1]
        for way in (1, -1):
            arrive("f1", part, way)
        for way in (1, -1):
            start(("m2", part, way), row_of(part, 0, 0), device(d2, way), True)
        whole_row(part, 0)
    for part in range(3):
        d2 = dims(part)[1]
        for way in (1, -1):
            arrive("m2", part, way)
            start(("f2", part, way), row_of(part, -way, 0, spans[way]), device(d2, way), way == -1)
            whole_row(part, -way)
    for part in range(3):
        for way in (1, -1):
            pass_on(part, 0, way)
    for part in range(3):
        for way in (1, -1):
            arrive("f2", part, way)
        whole_row(part, 2)
    for b in (-1, 1):
        for part in range(3):
            for way in (1, -1):
                pass_on(part, b, way)
    arrive_across(0)
    lax.fori_loop(0, 9, near_rows, 0)
    for part in range(3):
        last_row(part, 0)
    for part in range(3):
        for way in (1, -1):
            pass_on(part, 2, way)
    for b in (-1, 1):
        for part in range(3):
            last_row(part, b)
    arrive_across(1)
    lax.fori_loop(0, 9, far_rows, 0)
    for part in range(3):
        last_row(part, 2)
    arrive_across(2)
    lax.fori_loop(0, 3, farthest_rows, 0)
    pick((2, 2, 2))
    if first:
        table_ref[...] = tiles[...]
    for copy in copies.values():
        copy.wait_send()


def send_rows(x, table, layer, own, capacity, call_id, plus, first=False):
    tok_dev, width = x.shape
    devices = 2 * SIDE ** 3
    count = 240 if first else 120
    u_shape = jax.ShapeDtypeStruct((own, devices * capacity, width), x.dtype)
    table_shape = jax.ShapeDtypeStruct((2, SIDE, SIDE, SIDE, 3, 8, 128), F32)
    vmem = pl.BlockSpec(memory_space=pltpu.VMEM)
    hbm = pl.BlockSpec(memory_space=pl.ANY)
    return pl.pallas_call(
        functools.partial(send_kernel, own, capacity, layer, plus, first),
        out_shape=(u_shape, table_shape) if first else u_shape,
        in_specs=[hbm, hbm if first else vmem],
        out_specs=(vmem, vmem) if first else vmem,
        scratch_shapes=[
            pltpu.VMEM((2, SIDE, SIDE, SIDE, tok_dev, width), x.dtype),
            pltpu.SemaphoreType.DMA,
            pltpu.SemaphoreType.DMA((count,)),
            pltpu.SemaphoreType.DMA((count,)),
        ] + ([pltpu.VMEM(table_shape.shape, F32)] if first else []),
        compiler_params=pltpu.CompilerParams(collective_id=call_id, has_side_effects=True, vmem_limit_bytes=40 * 1024 * 1024),
        cost_estimate=pl.CostEstimate(flops=3 * 10**10, bytes_accessed=devices * tok_dev * width * 2, transcendentals=0),
        name=f"send_rows_{call_id}",
    )(x, table)


def home_order(rows, n_group):
    own, count, width = rows.shape
    rows = rows.reshape(own, n_group, count // n_group, width).transpose(1, 0, 2, 3)
    return rows.reshape(n_group, -1, width)


def expert_forward(u_rows, w_gate, w_up, w_down):
    pre_gate = jnp.einsum("erd,edf->erf", u_rows, w_gate, preferred_element_type=F32)
    pre_up = jnp.einsum("erd,edf->erf", u_rows, w_up, preferred_element_type=F32)
    hidden = (jax.nn.silu(pre_gate) * pre_up).astype(BF16)
    out_rows = jnp.einsum("erf,efd->erd", hidden, w_down, preferred_element_type=F32).astype(BF16)
    return pre_gate, pre_up, hidden, out_rows


def expert_backward(u_rows, dy_rows, gate_rows, w_gate, w_up, w_down):
    pre_gate, pre_up, hidden, out_rows = expert_forward(u_rows, w_gate, w_up, w_down)
    dgate_rows = jnp.einsum("erd,erd->er", dy_rows, out_rows, preferred_element_type=F32)
    d_out = (gate_rows[:, :, None] * dy_rows).astype(BF16)
    dw_down = jnp.einsum("erf,erd->efd", hidden, d_out, preferred_element_type=F32)
    d_hidden = jnp.einsum("erd,efd->erf", d_out, w_down, preferred_element_type=F32)
    gate_sig = jax.nn.sigmoid(pre_gate)
    d_pre_gate = (d_hidden * pre_up * gate_sig * (1.0 + pre_gate * (1.0 - gate_sig))).astype(BF16)
    d_pre_up = (d_hidden * jax.nn.silu(pre_gate)).astype(BF16)
    dw_gate = jnp.einsum("erd,erf->edf", u_rows, d_pre_gate, preferred_element_type=F32)
    dw_up = jnp.einsum("erd,erf->edf", u_rows, d_pre_up, preferred_element_type=F32)
    du_rows = (jnp.einsum("erf,edf->erd", d_pre_gate, w_gate, preferred_element_type=F32) + jnp.einsum("erf,edf->erd", d_pre_up, w_up, preferred_element_type=F32)).astype(BF16)
    return du_rows, dgate_rows, dw_gate, dw_up, dw_down


def solution(mesh):
    n_group = mesh.shape["ep"]
    tok_spec = P(("dp", "ep"))
    w_spec = P("ep")

    def device_program(x_in, idx_a, idx_b, gate_a, gate_b, dy_out, w1_a, w3_a, w2_a, w1_b, w3_b, w2_b):
        tok_dev, top_k = idx_a.shape
        width = x_in.shape[1]
        own = w1_a.shape[0]
        capacity = CAP_FACTOR * tok_dev * top_k // (own * n_group)
        total = own * n_group * capacity
        block = own * capacity

        rows_a = pair_rows(idx_a, capacity)
        rows_b = pair_rows(idx_b, capacity)
        lanes = [rows_a.T.astype(F32), rows_b.T.astype(F32), gate_a.T]
        rest = gate_b.T
        cut = 128 - tok_dev
        tile = jnp.stack([jnp.concatenate([lanes[i], rest[:, i * cut:(i + 1) * cut]], axis=1) for i in range(3)])
        third = tok_dev // 3
        even = third // 2
        u_a, table = send_rows(x_in, tile, 0, own, capacity, 0, even, True)
        by_device = table.reshape(2, n_group // 2, 3, 8, 128).transpose(1, 0, 2, 3, 4).reshape(n_group, 3, 8, 128)
        mine = (lax.axis_index("ep") * block + jnp.arange(block, dtype=jnp.int32)).astype(F32)

        def far_gates(code, gates):
            hit = code[:, None] == mine[None, :, None, None]
            gates = jnp.sum(jnp.where(hit, gates[:, None], 0.0), axis=(2, 3))
            return gates.reshape(n_group, own, capacity).transpose(1, 0, 2).reshape(own, -1)

        far_gate_a = far_gates(by_device[:, 0, :, :tok_dev], by_device[:, 2, :, :tok_dev])
        spread_b = jnp.concatenate([by_device[:, i, :, tok_dev:] for i in range(3)], axis=2)
        far_gate_b = far_gates(by_device[:, 1, :, :tok_dev], spread_b)
        weight_a = split3(pair_weight(rows_a, gate_a, total))
        weight_b = split3(pair_weight(rows_b, gate_b, total))
        ones = jnp.ones_like(gate_a)
        pick_a = pair_weight(rows_a, ones, total).astype(BF16)
        pick_b = pair_weight(rows_b, ones, total).astype(BF16)

        def send_back(rows):
            back = lax.all_to_all(home_order(rows, n_group), "ep", 0, 0, tiled=True)
            return back.reshape(total, width)

        def combine(x_rows, back, weight):
            branch = jnp.dot(weight, back, preferred_element_type=F32).reshape(3, tok_dev, width)
            branch = branch[0] + (branch[1] + branch[2])
            return (x_rows.astype(F32) + branch).astype(BF16)

        def layer_backward(dy_rows, dy_sent, u_rows, gates, pick, w_gate, w_up, w_down):
            du_rows, dgate_rows, dw_gate, dw_up, dw_down = expert_backward(u_rows, dy_sent, gates, w_gate, w_up, w_down)
            branch = jnp.dot(pick, send_back(du_rows), preferred_element_type=F32)
            dx_rows = (dy_rows.astype(F32) + branch).astype(BF16)
            return dx_rows, dgate_rows, (dw_gate, dw_up, dw_down)

        def by_home(dgate_rows):
            return dgate_rows.reshape(own, n_group, capacity).transpose(1, 0, 2).reshape(n_group, block)

        def look_up(back, rows):
            flat = rows.reshape(-1)
            expert = lax.div(flat, capacity)[:, None] == jnp.arange(own * n_group, dtype=jnp.int32)[None, :]
            picked = jnp.dot(expert.astype(F32), back.reshape(own * n_group, capacity), precision=lax.Precision.HIGHEST)
            slot = lax.rem(flat, capacity)[:, None] == jnp.arange(capacity, dtype=jnp.int32)[None, :]
            return jnp.sum(jnp.where(slot, picked, 0.0), axis=1).reshape(rows.shape)

        out_a = expert_forward(u_a, w1_a, w3_a, w2_a)[3]
        back_a = send_back(out_a)
        dy_b = send_rows(dy_out, table, 1, own, capacity, 1, 0)
        x_mid = combine(x_in, back_a, weight_a)
        u_b = send_rows(x_mid, table, 1, own, capacity, 2, even)
        out_b = expert_forward(u_b, w1_b, w3_b, w2_b)[3]
        x_out = combine(x_mid, send_back(out_b), weight_b)
        u_keep, dy_b, _ = lax.optimization_barrier((u_b, dy_b, out_b))
        dx_mid, dgate_rows_b, grads_b = layer_backward(dy_out, dy_b, u_keep, far_gate_b, pick_b, w1_b, w3_b, w2_b)
        x_again, _ = lax.optimization_barrier((x_in, out_b))
        u_again = send_rows(x_again, table, 0, own, capacity, 3, 0)
        dy_a = send_rows(dx_mid, table, 0, own, capacity, 4, 0)
        dx_in, dgate_rows_a, grads_a = layer_backward(dx_mid, dy_a, u_again, far_gate_a, pick_a, w1_a, w3_a, w2_a)
        dgates = jnp.concatenate([by_home(dgate_rows_a), by_home(dgate_rows_b)], axis=1)
        dgates = lax.all_to_all(dgates, "ep", 0, 0, tiled=True)
        dgate_a = look_up(dgates[:, :block], rows_a)
        dgate_b = look_up(dgates[:, block:], rows_b)
        return (x_out, dx_in) + grads_a + grads_b + (dgate_a, dgate_b)

    return jax.shard_map(device_program, mesh=mesh, in_specs=(tok_spec,) * 6 + (w_spec,) * 6, out_specs=(tok_spec,) * 10, check_vma=False)
```

```python
import functools

import jax
import jax.numpy as jnp
from jax import lax
from jax.experimental import pallas as pl
from jax.experimental.pallas import tpu as pltpu
from jax.sharding import PartitionSpec as P

CAP_FACTOR = 4
F32 = jnp.float32
BF16 = jnp.bfloat16


def pair_rows(ids, capacity):
    flat = ids.reshape(-1)
    pair = jnp.arange(flat.shape[0], dtype=jnp.int32)
    earlier = (flat[None, :] == flat[:, None]) & (pair[None, :] < pair[:, None])
    slot = jnp.sum(earlier.astype(jnp.int32), axis=1)
    return (flat * capacity + slot).reshape(ids.shape)


SIDE = 4


def send_kernel(own, capacity, layer, plus, first, scaled, *refs):
    if first:
        x_ref, tile_ref, u_ref, table_ref, held, local_sem, send_sem, recv_sem, tiles = refs
    elif scaled:
        x_ref, tiles, u_ref, q_ref, held, local_sem, send_sem, recv_sem = refs
    else:
        x_ref, tiles, u_ref, held, local_sem, send_sem, recv_sem = refs
    me = lax.axis_index("ep")
    core = lax.rem(me, 2)
    chip = lax.div(me, 2)
    at = (lax.rem(chip, SIDE), lax.rem(lax.div(chip, SIDE), SIDE), lax.div(chip, SIDE * SIDE))
    third = x_ref.shape[0] // 3
    spans = {1: (0, plus), -1: (plus, third - plus)}

    def device(dim, step):
        c = list(at)
        c[dim] = lax.rem(c[dim] + step + SIDE, SIDE)
        return ((c[2] * SIDE + c[1]) * SIDE + c[0]) * 2 + core

    partner = chip * 2 + (1 - core)

    def region(part, pos, span):
        if span[1] == 0:
            return None
        idx = [pos[d] if d in pos else at[d] for d in range(3)]
        idx = [pl.ds(0, SIDE) if i is None else i for i in idx]
        where = (core, idx[2], idx[1], idx[0])
        return held.at[where + (pl.ds(part * third + span[0], span[1]),)], where + (pl.ds(part, 2 if part == 2 else 1),)

    copies = {}

    def start(key, refs, to, with_tile):
        if refs is None:
            return
        for kind, ref in (("x", refs[0]), ("t", tiles.at[refs[1]])):
            if kind == "t" and not (first and with_tile):
                continue
            n = len(copies)
            copy = pltpu.make_async_remote_copy(src_ref=ref, dst_ref=ref, send_sem=send_sem.at[n], recv_sem=recv_sem.at[n], device_id={"ep": to}, device_id_type=pl.DeviceIdType.MESH)
            copy.start()
            copies[key + (kind,)] = copy

    def arrive(*key):
        for kind in ("x", "t"):
            if key + (kind,) in copies:
                copies[key + (kind,)].wait_recv()

    mine = pltpu.make_async_copy(x_ref, held.at[core, at[2], at[1], at[0]], local_sem)
    mine.start()
    if first:
        own_tile = pltpu.make_async_copy(tile_ref, tiles.at[core, at[2], at[1], at[0]], send_sem.at[0])
        own_tile.start()
        own_tile.wait()
    barrier = pltpu.get_barrier_semaphore()
    for dim in range(3):
        for step in (1, -1):
            pl.semaphore_signal(barrier, inc=1, device_id={"ep": device(dim, step)}, device_id_type=pl.DeviceIdType.MESH)
    pl.semaphore_signal(barrier, inc=1, device_id={"ep": partner}, device_id_type=pl.DeviceIdType.MESH)
    mine.wait()
    pl.semaphore_wait(barrier, 7)

    def dims(part):
        return part, (part + 1) % 3, (part + 2) % 3

    def shift(dim, step):
        return lax.rem(at[dim] + step + SIDE, SIDE)

    whole = (0, third)

    def row_of(part, b, c, span=whole):
        d1, d2, d3 = dims(part)
        return region(part, {d1: None, d2: shift(d2, b), d3: shift(d3, c)}, span)

    def across(part, b, c):
        start(("d2d", part, b, c), row_of(part, b, c), partner, True)

    def whole_row(part, b):
        d3 = dims(part)[2]
        for way in (1, -1):
            start(("m3", part, b, way), row_of(part, b, 0), device(d3, way), True)
        across(part, b, 0)

    def pass_on(part, b, way):
        d3 = dims(part)[2]
        arrive("m3", part, b, way)
        start(("f3", part, b, way), row_of(part, b, -way, spans[way]), device(d3, way), way == -1)
        across(part, b, -way)

    def last_row(part, b):
        for way in (1, -1):
            arrive("f3", part, b, way)
        across(part, b, 2)

    block = own * capacity
    slot = lax.broadcasted_iota(jnp.int32, (block, 128), 0) + me * block
    tok_dev = x_ref.shape[0]

    def pick(offsets):
        x, y, z = (lax.rem(at[d] + offsets[d] + SIDE, SIDE) for d in range(3))
        rows, scaled_rows = [], []
        for c in range(2):
            code = tiles[c, z, y, x, layer].astype(jnp.int32)
            gate = tiles[c, z, y, x, 2 + layer] if scaled else None
            hit = code[0:1, :] == slot
            weight = jnp.where(hit, gate[0:1, :], 0.0) if scaled else None
            for j in range(1, code.shape[0]):
                hit_j = code[j:j + 1, :] == slot
                hit = hit | hit_j
                if scaled:
                    weight = jnp.where(hit_j, gate[j:j + 1, :], weight)
            onehot = jnp.where(hit, 1.0, 0.0)[:, :tok_dev].astype(BF16)
            rows.append(jnp.dot(onehot, held[c, z, y, x], preferred_element_type=F32))
            if scaled:
                scaled_rows.append(jnp.sum(weight, axis=1, keepdims=True) * rows[-1])
        place = ((z * SIDE + y) * SIDE + x) * 2 * capacity
        for out_ref, parts in ((u_ref, rows),) + (((q_ref, scaled_rows),) if scaled else ()):
            for e in range(own):
                both = jnp.concatenate([r[e * capacity:(e + 1) * capacity] for r in parts], axis=0)
                out_ref[e, pl.ds(pl.multiple_of(place, 2 * capacity), 2 * capacity), :] = both.astype(BF16)

    def near_rows(step, carry):
        for k in (-1, 0, 1):
            pick((k, lax.rem(step, 3) - 1, lax.div(step, 3) - 1))
        return carry

    def far_rows(step, carry):
        b, c = lax.rem(step, 3) - 1, lax.div(step, 3) - 1
        for offsets in ((2, b, c), (b, 2, c), (b, c, 2)):
            pick(offsets)
        return carry

    def farthest_rows(step, carry):
        for offsets in ((2, 2, step - 1), (2, step - 1, 2), (step - 1, 2, 2)):
            pick(offsets)
        return carry

    def arrive_across(wanted):
        for part in range(3):
            for b in (0, -1, 1, 2):
                for c in (0, -1, 1, 2):
                    if (b == 2) + (c == 2) == wanted:
                        arrive("d2d", part, b, c)

    for part in range(3):
        d1 = dims(part)[0]
        for way in (1, -1):
            start(("m1", part, way), region(part, {}, whole), device(d1, way), True)
    for part in range(3):
        d1 = dims(part)[0]
        for way in (1, -1):
            arrive("m1", part, way)
            start(("f1", part, way), region(part, {d1: shift(d1, -way)}, spans[way]), device(d1, way), way == -1)
    for part in range(3):
        d2 = dims(part)[1]
        for way in (1, -1):
            arrive("f1", part, way)
        for way in (1, -1):
            start(("m2", part, way), row_of(part, 0, 0), device(d2, way), True)
    for part in range(3):
        whole_row(part, 0)
    for part in range(3):
        d2 = dims(part)[1]
        for way in (1, -1):
            arrive("m2", part, way)
            start(("f2", part, way), row_of(part, -way, 0, spans[way]), device(d2, way), way == -1)
            whole_row(part, -way)
    for part in range(3):
        for way in (1, -1):
            pass_on(part, 0, way)
    for part in range(3):
        for way in (1, -1):
            arrive("f2", part, way)
        whole_row(part, 2)
    for b in (-1, 1):
        for part in range(3):
            for way in (1, -1):
                pass_on(part, b, way)
    arrive_across(0)
    lax.fori_loop(0, 9, near_rows, 0)
    for part in range(3):
        last_row(part, 0)
    for part in range(3):
        for way in (1, -1):
            pass_on(part, 2, way)
    for b in (-1, 1):
        for part in range(3):
            last_row(part, b)
    arrive_across(1)
    lax.fori_loop(0, 9, far_rows, 0)
    for part in range(3):
        last_row(part, 2)
    arrive_across(2)
    lax.fori_loop(0, 3, farthest_rows, 0)
    pick((2, 2, 2))
    if first:
        table_ref[...] = tiles[...]
    for copy in copies.values():
        copy.wait_send()


def send_rows(x, table, layer, own, capacity, call_id, plus, first=False, scaled=False):
    tok_dev, width = x.shape
    devices = 2 * SIDE ** 3
    count = 240 if first else 120
    u_shape = jax.ShapeDtypeStruct((own, devices * capacity, width), x.dtype)
    table_shape = jax.ShapeDtypeStruct((2, SIDE, SIDE, SIDE, 4, 8, 128), F32)
    outs = (u_shape, table_shape) if first else (u_shape, u_shape) if scaled else (u_shape,)
    vmem = pl.BlockSpec(memory_space=pltpu.VMEM)
    hbm = pl.BlockSpec(memory_space=pl.ANY)
    return pl.pallas_call(
        functools.partial(send_kernel, own, capacity, layer, plus, first, scaled),
        out_shape=outs,
        in_specs=[hbm, hbm if first else vmem],
        out_specs=(vmem,) * len(outs),
        scratch_shapes=[
            pltpu.VMEM((2, SIDE, SIDE, SIDE, tok_dev, width), x.dtype),
            pltpu.SemaphoreType.DMA,
            pltpu.SemaphoreType.DMA((count,)),
            pltpu.SemaphoreType.DMA((count,)),
        ] + ([pltpu.VMEM(table_shape.shape, F32)] if first else []),
        compiler_params=pltpu.CompilerParams(collective_id=call_id, has_side_effects=True, vmem_limit_bytes=40 * 1024 * 1024),
        cost_estimate=pl.CostEstimate(flops=3 * 10**10, bytes_accessed=devices * tok_dev * width * 2, transcendentals=0),
        name=f"send_rows_{call_id}",
    )(x, table)


def combine_kernel(gated, x_ref, row_ref, gate_ref, back_ref, out_ref):
    tok_dev, width = x_ref.shape
    chunk = 512
    codes, gates = row_ref[...], gate_ref[...]
    total = jnp.zeros((tok_dev, width), F32)
    for base in range(0, back_ref.shape[0], chunk):
        lane = lax.broadcasted_iota(jnp.int32, (tok_dev, chunk), 1) + base
        weight = jnp.zeros((tok_dev, chunk), F32)
        for j in range(codes.shape[1]):
            weight = jnp.where(codes[:, j:j + 1] == lane, gates[:, j:j + 1] if gated else 1.0, weight)
        hi = weight.astype(BF16)
        terms = [hi]
        if gated:
            rest = weight - hi.astype(F32)
            mid = rest.astype(BF16)
            terms += [mid, (rest - mid.astype(F32)).astype(BF16)]
        part = jnp.dot(jnp.concatenate(terms, axis=0), back_ref[pl.ds(base, chunk), :], preferred_element_type=F32)
        for k in reversed(range(len(terms))):
            total = total + part[k * tok_dev:(k + 1) * tok_dev]
    out_ref[...] = (x_ref[...].astype(F32) + total).astype(out_ref.dtype)


def combine(x, rows, gates, back, gated):
    tok_dev, width = x.shape
    flops = 2 * tok_dev * back.shape[0] * width
    return pl.pallas_call(
        functools.partial(combine_kernel, gated),
        out_shape=jax.ShapeDtypeStruct(x.shape, x.dtype),
        in_specs=[pl.BlockSpec(memory_space=pltpu.VMEM)] * 4,
        out_specs=pl.BlockSpec(memory_space=pltpu.VMEM),
        compiler_params=pltpu.CompilerParams(vmem_limit_bytes=24 * 1024 * 1024),
        cost_estimate=pl.CostEstimate(flops=flops * (3 if gated else 1), bytes_accessed=back.size * 2, transcendentals=0),
        name="combine",
    )(x, rows, gates, back)


def home_order(rows, n_group):
    own, count, width = rows.shape
    rows = rows.reshape(own, n_group, count // n_group, width).transpose(1, 0, 2, 3)
    return rows.reshape(n_group, -1, width)


def expert_forward(u_rows, w_gate, w_up, w_down):
    pre_gate = jnp.einsum("erd,edf->erf", u_rows, w_gate, preferred_element_type=F32)
    pre_up = jnp.einsum("erd,edf->erf", u_rows, w_up, preferred_element_type=F32)
    hidden = (jax.nn.silu(pre_gate) * pre_up).astype(BF16)
    out_rows = jnp.einsum("erf,efd->erd", hidden, w_down, preferred_element_type=F32).astype(BF16)
    return pre_gate, pre_up, hidden, out_rows


def expert_backward(u_rows, dy_rows, d_out, w_gate, w_up, w_down):
    pre_gate, pre_up, hidden, out_rows = expert_forward(u_rows, w_gate, w_up, w_down)
    dgate_rows = jnp.einsum("erd,erd->er", dy_rows, out_rows, preferred_element_type=F32)
    dw_down = jnp.einsum("erf,erd->efd", hidden, d_out, preferred_element_type=F32)
    d_hidden = jnp.einsum("erd,efd->erf", d_out, w_down, preferred_element_type=F32)
    gate_sig = jax.nn.sigmoid(pre_gate)
    d_pre_gate = (d_hidden * pre_up * gate_sig * (1.0 + pre_gate * (1.0 - gate_sig))).astype(BF16)
    d_pre_up = (d_hidden * jax.nn.silu(pre_gate)).astype(BF16)
    dw_gate = jnp.einsum("erd,erf->edf", u_rows, d_pre_gate, preferred_element_type=F32)
    dw_up = jnp.einsum("erd,erf->edf", u_rows, d_pre_up, preferred_element_type=F32)
    du_rows = (jnp.einsum("erf,edf->erd", d_pre_gate, w_gate, preferred_element_type=F32) + jnp.einsum("erf,edf->erd", d_pre_up, w_up, preferred_element_type=F32)).astype(BF16)
    return du_rows, dgate_rows, dw_gate, dw_up, dw_down


def solution(mesh):
    n_group = mesh.shape["ep"]
    tok_spec = P(("dp", "ep"))
    w_spec = P("ep")

    def device_program(x_in, idx_a, idx_b, gate_a, gate_b, dy_out, w1_a, w3_a, w2_a, w1_b, w3_b, w2_b):
        tok_dev, top_k = idx_a.shape
        width = x_in.shape[1]
        own = w1_a.shape[0]
        capacity = CAP_FACTOR * tok_dev * top_k // (own * n_group)
        total = own * n_group * capacity
        block = own * capacity

        rows_a = pair_rows(idx_a, capacity)
        rows_b = pair_rows(idx_b, capacity)
        pad = ((0, 0), (0, 128 - tok_dev))
        tile = jnp.stack([jnp.pad(rows_a.T.astype(F32), pad, constant_values=-1.0), jnp.pad(rows_b.T.astype(F32), pad, constant_values=-1.0), jnp.pad(gate_a.T, pad), jnp.pad(gate_b.T, pad)])
        third = tok_dev // 3
        even = third // 2
        u_a, table = send_rows(x_in, tile, 0, own, capacity, 0, even, first=True)

        def send_back(rows):
            back = lax.all_to_all(home_order(rows, n_group), "ep", 0, 0, tiled=True)
            return back.reshape(total, width)

        def by_home(dgate_rows):
            return dgate_rows.reshape(own, n_group, capacity).transpose(1, 0, 2).reshape(n_group, block)

        def look_up(back, rows):
            flat = rows.reshape(-1)
            expert = lax.div(flat, capacity)[:, None] == jnp.arange(own * n_group, dtype=jnp.int32)[None, :]
            picked = jnp.dot(expert.astype(F32), back.reshape(own * n_group, capacity), precision=lax.Precision.HIGHEST)
            slot = lax.rem(flat, capacity)[:, None] == jnp.arange(capacity, dtype=jnp.int32)[None, :]
            return jnp.sum(jnp.where(slot, picked, 0.0), axis=1).reshape(rows.shape)

        out_a = expert_forward(u_a, w1_a, w3_a, w2_a)[3]
        back_a = send_back(out_a)
        dy_b, q_b = send_rows(dy_out, table, 1, own, capacity, 1, third, scaled=True)
        x_mid = combine(x_in, rows_a, gate_a, back_a, True)
        u_b, = send_rows(x_mid, table, 1, own, capacity, 2, even)
        out_b = expert_forward(u_b, w1_b, w3_b, w2_b)[3]
        u_keep, dy_b, _ = lax.optimization_barrier((u_b, dy_b, out_b))
        du_b, dgate_rows_b, *grads_b = expert_backward(u_keep, dy_b, q_b, w1_b, w3_b, w2_b)
        x_again, _ = lax.optimization_barrier((x_in, out_b))
        u_again, = send_rows(x_again, table, 0, own, capacity, 3, third)
        dx_mid = combine(dy_out, rows_b, gate_b, send_back(du_b), False)
        dy_a, q_a = send_rows(dx_mid, table, 0, own, capacity, 4, third, scaled=True)
        x_out = combine(x_mid, rows_b, gate_b, send_back(out_b), True)
        du_a, dgate_rows_a, *grads_a = expert_backward(u_again, dy_a, q_a, w1_a, w3_a, w2_a)
        dx_in = combine(dx_mid, rows_a, gate_a, send_back(du_a), False)
        dgates = jnp.concatenate([by_home(dgate_rows_a), by_home(dgate_rows_b)], axis=1)
        dgates = lax.all_to_all(dgates, "ep", 0, 0, tiled=True)
        dgate_a = look_up(dgates[:, :block], rows_a)
        dgate_b = look_up(dgates[:, block:], rows_b)
        return (x_out, dx_in) + tuple(grads_a) + tuple(grads_b) + (dgate_a, dgate_b)

    return jax.shard_map(device_program, mesh=mesh, in_specs=(tok_spec,) * 6 + (w_spec,) * 6, out_specs=(tok_spec,) * 10, check_vma=False)
```

```python
import functools

import jax
import jax.numpy as jnp
from jax import lax
from jax.experimental import pallas as pl
from jax.experimental.pallas import tpu as pltpu
from jax.sharding import PartitionSpec as P

CAP_FACTOR = 4
F32 = jnp.float32
BF16 = jnp.bfloat16


def pair_rows(ids, capacity):
    flat = ids.reshape(-1)
    pair = jnp.arange(flat.shape[0], dtype=jnp.int32)
    earlier = (flat[None, :] == flat[:, None]) & (pair[None, :] < pair[:, None])
    slot = jnp.sum(earlier.astype(jnp.int32), axis=1)
    return (flat * capacity + slot).reshape(ids.shape)


SIDE = 4


def send_kernel(own, capacity, layer, plus, first, scaled, *refs):
    if first:
        x_ref, tile_ref, u_ref, table_ref, held, local_sem, send_sem, recv_sem, tiles = refs
    elif scaled:
        x_ref, tiles, u_ref, q_ref, held, local_sem, send_sem, recv_sem = refs
    else:
        x_ref, tiles, u_ref, held, local_sem, send_sem, recv_sem = refs
    me = lax.axis_index("ep")
    core = lax.rem(me, 2)
    chip = lax.div(me, 2)
    at = (lax.rem(chip, SIDE), lax.rem(lax.div(chip, SIDE), SIDE), lax.div(chip, SIDE * SIDE))
    third = x_ref.shape[0] // 3
    spans = {1: (0, plus), -1: (plus, third - plus)}

    def device(dim, step):
        c = list(at)
        c[dim] = lax.rem(c[dim] + step + SIDE, SIDE)
        return ((c[2] * SIDE + c[1]) * SIDE + c[0]) * 2 + core

    partner = chip * 2 + (1 - core)

    def region(part, pos, span):
        if span[1] == 0:
            return None
        idx = [pos[d] if d in pos else at[d] for d in range(3)]
        idx = [pl.ds(0, SIDE) if i is None else i for i in idx]
        where = (core, idx[2], idx[1], idx[0])
        return held.at[where + (pl.ds(part * third + span[0], span[1]),)], where + (pl.ds(part, 2 if part == 2 else 1),)

    copies = {}

    def start(key, refs, to, with_tile):
        if refs is None:
            return
        for kind, ref in (("x", refs[0]), ("t", tiles.at[refs[1]])):
            if kind == "t" and not (first and with_tile):
                continue
            n = len(copies)
            copy = pltpu.make_async_remote_copy(src_ref=ref, dst_ref=ref, send_sem=send_sem.at[n], recv_sem=recv_sem.at[n], device_id={"ep": to}, device_id_type=pl.DeviceIdType.MESH)
            copy.start()
            copies[key + (kind,)] = copy

    def arrive(*key):
        for kind in ("x", "t"):
            if key + (kind,) in copies:
                copies[key + (kind,)].wait_recv()

    mine = pltpu.make_async_copy(x_ref, held.at[core, at[2], at[1], at[0]], local_sem)
    mine.start()
    if first:
        own_tile = pltpu.make_async_copy(tile_ref, tiles.at[core, at[2], at[1], at[0]], send_sem.at[0])
        own_tile.start()
        own_tile.wait()
    barrier = pltpu.get_barrier_semaphore()
    for dim in range(3):
        for step in (1, -1, 2):
            pl.semaphore_signal(barrier, inc=1, device_id={"ep": device(dim, step)}, device_id_type=pl.DeviceIdType.MESH)
    pl.semaphore_signal(barrier, inc=1, device_id={"ep": partner}, device_id_type=pl.DeviceIdType.MESH)
    mine.wait()
    pl.semaphore_wait(barrier, 10)

    def dims(part):
        return part, (part + 1) % 3, (part + 2) % 3

    def shift(dim, step):
        return lax.rem(at[dim] + step + SIDE, SIDE)

    whole = (0, third)

    def row_of(part, b, c, span=whole):
        d1, d2, d3 = dims(part)
        return region(part, {d1: None, d2: shift(d2, b), d3: shift(d3, c)}, span)

    def across(part, b, c):
        start(("d2d", part, b, c), row_of(part, b, c), partner, True)

    def whole_row(part, b):
        d3 = dims(part)[2]
        for way in (1, -1):
            start(("m3", part, b, way), row_of(part, b, 0), device(d3, way), True)
        across(part, b, 0)

    def pass_on(part, b, way):
        d3 = dims(part)[2]
        arrive("m3", part, b, way)
        start(("f3", part, b, way), row_of(part, b, -way, spans[way]), device(d3, way), way == -1)
        across(part, b, -way)

    def last_row(part, b):
        for way in (1, -1):
            arrive("f3", part, b, way)
        across(part, b, 2)

    block = own * capacity
    slot = lax.broadcasted_iota(jnp.int32, (block, 128), 0) + me * block
    tok_dev = x_ref.shape[0]

    def pick(offsets):
        x, y, z = (lax.rem(at[d] + offsets[d] + SIDE, SIDE) for d in range(3))
        rows, scaled_rows = [], []
        for c in range(2):
            code = tiles[c, z, y, x, layer].astype(jnp.int32)
            gate = tiles[c, z, y, x, 2 + layer] if scaled else None
            hit = code[0:1, :] == slot
            weight = jnp.where(hit, gate[0:1, :], 0.0) if scaled else None
            for j in range(1, code.shape[0]):
                hit_j = code[j:j + 1, :] == slot
                hit = hit | hit_j
                if scaled:
                    weight = jnp.where(hit_j, gate[j:j + 1, :], weight)
            onehot = jnp.where(hit, 1.0, 0.0)[:, :tok_dev].astype(BF16)
            rows.append(jnp.dot(onehot, held[c, z, y, x], preferred_element_type=F32))
            if scaled:
                scaled_rows.append(jnp.sum(weight, axis=1, keepdims=True) * rows[-1])
        place = ((z * SIDE + y) * SIDE + x) * 2 * capacity
        for out_ref, parts in ((u_ref, rows),) + (((q_ref, scaled_rows),) if scaled else ()):
            for e in range(own):
                both = jnp.concatenate([r[e * capacity:(e + 1) * capacity] for r in parts], axis=0)
                out_ref[e, pl.ds(pl.multiple_of(place, 2 * capacity), 2 * capacity), :] = both.astype(BF16)

    def near_rows(step, carry):
        for k in (-1, 0, 1):
            pick((k, lax.rem(step, 3) - 1, lax.div(step, 3) - 1))
        return carry

    def far_rows(step, carry):
        b, c = lax.rem(step, 3) - 1, lax.div(step, 3) - 1
        for offsets in ((2, b, c), (b, 2, c), (b, c, 2)):
            pick(offsets)
        return carry

    def farthest_rows(step, carry):
        for offsets in ((2, 2, step - 1), (2, step - 1, 2), (step - 1, 2, 2)):
            pick(offsets)
        return carry

    def arrive_across(wanted):
        for part in range(3):
            for b in (0, -1, 1, 2):
                for c in (0, -1, 1, 2):
                    if (b == 2) + (c == 2) == wanted:
                        arrive("d2d", part, b, c)

    for part in range(3):
        d1 = dims(part)[0]
        for way in (2, 1, -1):
            start(("m1", part, way), region(part, {}, whole), device(d1, way), True)
    for part in range(3):
        d2 = dims(part)[1]
        for way in (1, -1, 2):
            arrive("m1", part, way)
        for way in (2, 1, -1):
            start(("m2", part, way), row_of(part, 0, 0), device(d2, way), True)
    for part in range(3):
        whole_row(part, 0)
    for part in range(3):
        for way in (1, -1):
            arrive("m2", part, way)
            whole_row(part, -way)
    for part in range(3):
        for way in (1, -1):
            pass_on(part, 0, way)
    for part in range(3):
        arrive("m2", part, 2)
        whole_row(part, 2)
    for b in (-1, 1):
        for part in range(3):
            for way in (1, -1):
                pass_on(part, b, way)
    arrive_across(0)
    lax.fori_loop(0, 9, near_rows, 0)
    for part in range(3):
        last_row(part, 0)
    for part in range(3):
        for way in (1, -1):
            pass_on(part, 2, way)
    for b in (-1, 1):
        for part in range(3):
            last_row(part, b)
    arrive_across(1)
    lax.fori_loop(0, 9, far_rows, 0)
    for part in range(3):
        last_row(part, 2)
    arrive_across(2)
    lax.fori_loop(0, 3, farthest_rows, 0)
    pick((2, 2, 2))
    if first:
        table_ref[...] = tiles[...]
    for copy in copies.values():
        copy.wait_send()


def send_rows(x, table, layer, own, capacity, call_id, plus, first=False, scaled=False):
    tok_dev, width = x.shape
    devices = 2 * SIDE ** 3
    count = 228 if first else 114
    u_shape = jax.ShapeDtypeStruct((own, devices * capacity, width), x.dtype)
    table_shape = jax.ShapeDtypeStruct((2, SIDE, SIDE, SIDE, 4, 8, 128), F32)
    outs = (u_shape, table_shape) if first else (u_shape, u_shape) if scaled else (u_shape,)
    vmem = pl.BlockSpec(memory_space=pltpu.VMEM)
    hbm = pl.BlockSpec(memory_space=pl.ANY)
    return pl.pallas_call(
        functools.partial(send_kernel, own, capacity, layer, plus, first, scaled),
        out_shape=outs,
        in_specs=[hbm, hbm if first else vmem],
        out_specs=(vmem,) * len(outs),
        scratch_shapes=[
            pltpu.VMEM((2, SIDE, SIDE, SIDE, tok_dev, width), x.dtype),
            pltpu.SemaphoreType.DMA,
            pltpu.SemaphoreType.DMA((count,)),
            pltpu.SemaphoreType.DMA((count,)),
        ] + ([pltpu.VMEM(table_shape.shape, F32)] if first else []),
        compiler_params=pltpu.CompilerParams(collective_id=call_id, has_side_effects=True, vmem_limit_bytes=40 * 1024 * 1024),
        cost_estimate=pl.CostEstimate(flops=3 * 10**10, bytes_accessed=devices * tok_dev * width * 2, transcendentals=0),
        name=f"send_rows_{call_id}",
    )(x, table)


def combine_kernel(gated, x_ref, row_ref, gate_ref, back_ref, out_ref):
    tok_dev, width = x_ref.shape
    chunk = 512
    codes, gates = row_ref[...], gate_ref[...]
    total = jnp.zeros((tok_dev, width), F32)
    for base in range(0, back_ref.shape[0], chunk):
        lane = lax.broadcasted_iota(jnp.int32, (tok_dev, chunk), 1) + base
        weight = jnp.zeros((tok_dev, chunk), F32)
        for j in range(codes.shape[1]):
            weight = jnp.where(codes[:, j:j + 1] == lane, gates[:, j:j + 1] if gated else 1.0, weight)
        hi = weight.astype(BF16)
        terms = [hi]
        if gated:
            rest = weight - hi.astype(F32)
            mid = rest.astype(BF16)
            terms += [mid, (rest - mid.astype(F32)).astype(BF16)]
        part = jnp.dot(jnp.concatenate(terms, axis=0), back_ref[pl.ds(base, chunk), :], preferred_element_type=F32)
        for k in reversed(range(len(terms))):
            total = total + part[k * tok_dev:(k + 1) * tok_dev]
    out_ref[...] = (x_ref[...].astype(F32) + total).astype(out_ref.dtype)


def combine(x, rows, gates, back, gated):
    tok_dev, width = x.shape
    flops = 2 * tok_dev * back.shape[0] * width
    return pl.pallas_call(
        functools.partial(combine_kernel, gated),
        out_shape=jax.ShapeDtypeStruct(x.shape, x.dtype),
        in_specs=[pl.BlockSpec(memory_space=pltpu.VMEM)] * 4,
        out_specs=pl.BlockSpec(memory_space=pltpu.VMEM),
        compiler_params=pltpu.CompilerParams(vmem_limit_bytes=24 * 1024 * 1024),
        cost_estimate=pl.CostEstimate(flops=flops * (3 if gated else 1), bytes_accessed=back.size * 2, transcendentals=0),
        name="combine",
    )(x, rows, gates, back)


def forward_rows(u, w_both, w_down):
    ff = w_down.shape[0]
    pre = jnp.dot(u, w_both, preferred_element_type=F32)
    pre_gate, pre_up = pre[:, :ff], pre[:, ff:]
    sig = 1.0 / (1.0 + jnp.exp(-pre_gate))
    silu = pre_gate * sig
    hidden = (silu * pre_up).astype(BF16)
    out = jnp.dot(hidden, w_down, preferred_element_type=F32)
    return pre_gate, pre_up, sig, silu, hidden, out


def store_home(out_ref, step, rows):
    count, width = rows.shape
    slots = out_ref.shape[1]
    sources = count // slots
    out_ref[pl.ds(step * sources, sources)] = rows.reshape(sources, slots, width).astype(out_ref.dtype)


def forward_kernel(chunk, u_ref, w1_ref, w3_ref, w2_ref, out_ref):
    w_both = jnp.concatenate([w1_ref[0], w3_ref[0]], axis=1)

    def body(step, carry):
        rows = pl.ds(pl.multiple_of(step * chunk, chunk), chunk)
        out = forward_rows(u_ref[0, rows, :], w_both, w2_ref[0])[-1]
        store_home(out_ref, step, out)
        return carry

    lax.fori_loop(0, u_ref.shape[1] // chunk, body, 0)


def backward_kernel(chunk, u_ref, dy_ref, q_ref, w1_ref, w3_ref, w2_ref, du_ref, dgate_ref, hidden_ref, da_ref, db_ref):
    ff = w2_ref.shape[1]
    w_both = jnp.concatenate([w1_ref[0], w3_ref[0]], axis=1)
    last = (((1,), (1,)), ((), ()))

    def body(step, carry):
        rows = pl.ds(pl.multiple_of(step * chunk, chunk), chunk)
        pre_gate, pre_up, sig, silu, hidden, out = forward_rows(u_ref[0, rows, :], w_both, w2_ref[0])
        dgate = jnp.sum(dy_ref[0, rows, :].astype(F32) * out.astype(BF16).astype(F32), axis=1, keepdims=True)
        diagonal = lax.broadcasted_iota(jnp.int32, (128, 128), 0) == lax.broadcasted_iota(jnp.int32, (128, 128), 1)
        for k in range(chunk // 128):
            line = jnp.sum(jnp.where(diagonal, dgate[k * 128:(k + 1) * 128], 0.0), axis=0, keepdims=True)
            dgate_ref[0, pl.ds(step * (chunk // 128) + k, 1), :] = line
        d_hidden = lax.dot_general(q_ref[0, rows, :], w2_ref[0], last, preferred_element_type=F32)
        da = (d_hidden * pre_up * sig * (1.0 + pre_gate * (1.0 - sig))).astype(BF16)
        db = (d_hidden * silu).astype(BF16)
        hidden_ref[0, rows, :] = hidden
        da_ref[0, rows, :] = da
        db_ref[0, rows, :] = db
        both = jnp.concatenate([da, db], axis=1)
        store_home(du_ref, step, lax.dot_general(both, w_both, last, preferred_element_type=F32))
        return carry

    lax.fori_loop(0, u_ref.shape[1] // chunk, body, 0)


def expert_call(kernel, inputs, outs, weights, n_group, name):
    own, count, width = inputs[0].shape
    ff = weights[2].shape[1]
    slots = count // n_group

    def each(shape):
        return pl.BlockSpec((1,) + shape, lambda e: (e, 0, 0))

    home = (jax.ShapeDtypeStruct((n_group, own * slots, width), BF16), pl.BlockSpec((n_group, slots, width), lambda e: (0, e, 0)))
    kinds = {
        "home": home,
        "gate": (jax.ShapeDtypeStruct((own, count // 128, 128), F32), each((count // 128, 128))),
        "ff": (jax.ShapeDtypeStruct((own, count, ff), BF16), each((count, ff))),
    }
    steps = 3 if len(outs) == 1 else 8
    return pl.pallas_call(
        functools.partial(kernel, 256),
        out_shape=tuple(kinds[k][0] for k in outs),
        grid=(own,),
        in_specs=[each((count, width))] * len(inputs) + [each((width, ff)), each((width, ff)), each((ff, width))],
        out_specs=tuple(kinds[k][1] for k in outs),
        compiler_params=pltpu.CompilerParams(vmem_limit_bytes=32 * 1024 * 1024),
        cost_estimate=pl.CostEstimate(flops=2 * steps * own * count * width * ff, bytes_accessed=own * count * width * 2 * (len(inputs) + 1), transcendentals=own * count * ff),
        name=name,
    )(*inputs, *weights)


def expert_forward(u_rows, weights, n_group):
    return expert_call(forward_kernel, (u_rows,), ("home",), weights, n_group, "expert_forward")[0]


def expert_backward(u_rows, dy_rows, q_rows, weights, n_group):
    outs = ("home", "gate", "ff", "ff", "ff")
    du, dgate, hidden, da, db = expert_call(backward_kernel, (u_rows, dy_rows, q_rows), outs, weights, n_group, "expert_backward")

    def grads(u_rows, q_rows, hidden, da, db):
        dw_gate = jnp.einsum("erd,erf->edf", u_rows, da, preferred_element_type=F32)
        dw_up = jnp.einsum("erd,erf->edf", u_rows, db, preferred_element_type=F32)
        dw_down = jnp.einsum("erf,erd->efd", hidden, q_rows, preferred_element_type=F32)
        return dw_gate, dw_up, dw_down

    return du, dgate, grads(u_rows, q_rows, hidden, da, db)


def solution(mesh):
    n_group = mesh.shape["ep"]
    tok_spec = P(("dp", "ep"))
    w_spec = P("ep")

    def device_program(x_in, idx_a, idx_b, gate_a, gate_b, dy_out, w1_a, w3_a, w2_a, w1_b, w3_b, w2_b):
        tok_dev, top_k = idx_a.shape
        width = x_in.shape[1]
        own = w1_a.shape[0]
        capacity = CAP_FACTOR * tok_dev * top_k // (own * n_group)
        total = own * n_group * capacity
        block = own * capacity

        rows_a = pair_rows(idx_a, capacity)
        rows_b = pair_rows(idx_b, capacity)
        pad = ((0, 0), (0, 128 - tok_dev))
        tile = jnp.stack([jnp.pad(rows_a.T.astype(F32), pad, constant_values=-1.0), jnp.pad(rows_b.T.astype(F32), pad, constant_values=-1.0), jnp.pad(gate_a.T, pad), jnp.pad(gate_b.T, pad)])
        third = tok_dev // 3
        even = third // 2
        u_a, table = send_rows(x_in, tile, 0, own, capacity, 0, even, first=True)

        def send_back(rows):
            return lax.all_to_all(rows, "ep", 0, 0, tiled=True).reshape(total, width)

        def by_home(dgate_rows):
            return dgate_rows.reshape(own, n_group, capacity).transpose(1, 0, 2).reshape(n_group, block)

        def look_up(back, rows):
            flat = rows.reshape(-1)
            expert = lax.div(flat, capacity)[:, None] == jnp.arange(own * n_group, dtype=jnp.int32)[None, :]
            picked = jnp.dot(expert.astype(F32), back.reshape(own * n_group, capacity), precision=lax.Precision.HIGHEST)
            slot = lax.rem(flat, capacity)[:, None] == jnp.arange(capacity, dtype=jnp.int32)[None, :]
            return jnp.sum(jnp.where(slot, picked, 0.0), axis=1).reshape(rows.shape)

        weights_a, weights_b = (w1_a, w3_a, w2_a), (w1_b, w3_b, w2_b)
        back_a = send_back(expert_forward(u_a, weights_a, n_group))
        dy_b, q_b = send_rows(dy_out, table, 1, own, capacity, 1, even, scaled=True)
        x_mid = combine(x_in, rows_a, gate_a, back_a, True)
        u_b, = send_rows(x_mid, table, 1, own, capacity, 2, even)
        out_b = expert_forward(u_b, weights_b, n_group)
        du_b, dgate_rows_b, grads_b = expert_backward(u_b, dy_b, q_b, weights_b, n_group)
        x_again, du_b = lax.optimization_barrier((x_in, du_b))
        u_again, = send_rows(x_again, table, 0, own, capacity, 3, even)
        dx_mid = combine(dy_out, rows_b, gate_b, send_back(du_b), False)
        dy_a, q_a = send_rows(dx_mid, table, 0, own, capacity, 4, even, scaled=True)
        x_out = combine(x_mid, rows_b, gate_b, send_back(out_b), True)
        du_a, dgate_rows_a, grads_a = expert_backward(u_again, dy_a, q_a, weights_a, n_group)
        dx_in = combine(dx_mid, rows_a, gate_a, send_back(du_a), False)
        dgates = jnp.concatenate([by_home(dgate_rows_a), by_home(dgate_rows_b)], axis=1)
        dgates = lax.all_to_all(dgates, "ep", 0, 0, tiled=True)
        dgate_a = look_up(dgates[:, :block], rows_a)
        dgate_b = look_up(dgates[:, block:], rows_b)
        return (x_out, dx_in) + tuple(grads_a) + tuple(grads_b) + (dgate_a, dgate_b)

    return jax.shard_map(device_program, mesh=mesh, in_specs=(tok_spec,) * 6 + (w_spec,) * 6, out_specs=(tok_spec,) * 10, check_vma=False)
```

```python
import functools

import jax
import jax.numpy as jnp
from jax import lax
from jax.experimental import pallas as pl
from jax.experimental.pallas import tpu as pltpu
from jax.sharding import PartitionSpec as P

CAP_FACTOR = 4
F32 = jnp.float32
BF16 = jnp.bfloat16


def pair_rows(ids, capacity):
    flat = ids.reshape(-1)
    pair = jnp.arange(flat.shape[0], dtype=jnp.int32)
    earlier = (flat[None, :] == flat[:, None]) & (pair[None, :] < pair[:, None])
    slot = jnp.sum(earlier.astype(jnp.int32), axis=1)
    return (flat * capacity + slot).reshape(ids.shape)


SIDE = 4


def send_kernel(own, capacity, layer, plus, first, scaled, *refs):
    if first:
        x_ref, tile_ref, u_ref, table_ref, held, local_sem, send_sem, recv_sem, tiles = refs
    elif scaled:
        x_ref, tiles, u_ref, q_ref, held, local_sem, send_sem, recv_sem = refs
    else:
        x_ref, tiles, u_ref, held, local_sem, send_sem, recv_sem = refs
    me = lax.axis_index("ep")
    core = lax.rem(me, 2)
    chip = lax.div(me, 2)
    at = (lax.rem(chip, SIDE), lax.rem(lax.div(chip, SIDE), SIDE), lax.div(chip, SIDE * SIDE))
    third = x_ref.shape[0] // 3
    spans = {1: (0, plus), -1: (plus, third - plus)}

    def device(dim, step):
        c = list(at)
        c[dim] = lax.rem(c[dim] + step + SIDE, SIDE)
        return ((c[2] * SIDE + c[1]) * SIDE + c[0]) * 2 + core

    partner = chip * 2 + (1 - core)

    def region(part, pos, span):
        if span[1] == 0:
            return None
        idx = [pos[d] if d in pos else at[d] for d in range(3)]
        idx = [pl.ds(0, SIDE) if i is None else i for i in idx]
        where = (core, idx[2], idx[1], idx[0])
        return held.at[where + (pl.ds(part * third + span[0], span[1]),)], where + (pl.ds(part, 2 if part == 2 else 1),)

    copies = {}

    def start(key, refs, to, with_tile):
        if refs is None:
            return
        for kind, ref in (("x", refs[0]), ("t", tiles.at[refs[1]])):
            if kind == "t" and not (first and with_tile):
                continue
            n = len(copies)
            copy = pltpu.make_async_remote_copy(src_ref=ref, dst_ref=ref, send_sem=send_sem.at[n], recv_sem=recv_sem.at[n], device_id={"ep": to}, device_id_type=pl.DeviceIdType.MESH)
            copy.start()
            copies[key + (kind,)] = copy

    def arrive(*key):
        for kind in ("x", "t"):
            if key + (kind,) in copies:
                copies[key + (kind,)].wait_recv()

    mine = pltpu.make_async_copy(x_ref, held.at[core, at[2], at[1], at[0]], local_sem)
    mine.start()
    if first:
        own_tile = pltpu.make_async_copy(tile_ref, tiles.at[core, at[2], at[1], at[0]], send_sem.at[0])
        own_tile.start()
        own_tile.wait()
    barrier = pltpu.get_barrier_semaphore()
    for dim in range(3):
        for step in (1, -1, 2):
            pl.semaphore_signal(barrier, inc=1, device_id={"ep": device(dim, step)}, device_id_type=pl.DeviceIdType.MESH)
    pl.semaphore_signal(barrier, inc=1, device_id={"ep": partner}, device_id_type=pl.DeviceIdType.MESH)
    mine.wait()
    pl.semaphore_wait(barrier, 10)

    def dims(part):
        return part, (part + 1) % 3, (part + 2) % 3

    def shift(dim, step):
        return lax.rem(at[dim] + step + SIDE, SIDE)

    whole = (0, third)

    def row_of(part, b, c, span=whole):
        d1, d2, d3 = dims(part)
        return region(part, {d1: None, d2: shift(d2, b), d3: shift(d3, c)}, span)

    def across(part, b, c):
        start(("d2d", part, b, c), row_of(part, b, c), partner, True)

    def whole_row(part, b):
        d3 = dims(part)[2]
        for way in (1, -1):
            start(("m3", part, b, way), row_of(part, b, 0), device(d3, way), True)
        across(part, b, 0)

    def pass_on(part, b, way):
        d3 = dims(part)[2]
        arrive("m3", part, b, way)
        start(("f3", part, b, way), row_of(part, b, -way, spans[way]), device(d3, way), way == -1)
        across(part, b, -way)

    def last_row(part, b):
        for way in (1, -1):
            arrive("f3", part, b, way)
        across(part, b, 2)

    block = own * capacity
    slot = lax.broadcasted_iota(jnp.int32, (block, 128), 0) + me * block
    tok_dev = x_ref.shape[0]

    def pick(offsets):
        x, y, z = (lax.rem(at[d] + offsets[d] + SIDE, SIDE) for d in range(3))
        rows, scaled_rows = [], []
        for c in range(2):
            code = tiles[c, z, y, x, layer].astype(jnp.int32)
            gate = tiles[c, z, y, x, 2 + layer] if scaled else None
            hit = code[0:1, :] == slot
            weight = jnp.where(hit, gate[0:1, :], 0.0) if scaled else None
            for j in range(1, code.shape[0]):
                hit_j = code[j:j + 1, :] == slot
                hit = hit | hit_j
                if scaled:
                    weight = jnp.where(hit_j, gate[j:j + 1, :], weight)
            onehot = jnp.where(hit, 1.0, 0.0)[:, :tok_dev].astype(BF16)
            rows.append(jnp.dot(onehot, held[c, z, y, x], preferred_element_type=F32))
            if scaled:
                scaled_rows.append(jnp.sum(weight, axis=1, keepdims=True) * rows[-1])
        place = ((z * SIDE + y) * SIDE + x) * 2 * capacity
        for out_ref, parts in ((u_ref, rows),) + (((q_ref, scaled_rows),) if scaled else ()):
            for e in range(own):
                both = jnp.concatenate([r[e * capacity:(e + 1) * capacity] for r in parts], axis=0)
                out_ref[e, pl.ds(pl.multiple_of(place, 2 * capacity), 2 * capacity), :] = both.astype(BF16)

    def near_rows(step, carry):
        for k in (-1, 0, 1):
            pick((k, lax.rem(step, 3) - 1, lax.div(step, 3) - 1))
        return carry

    def far_rows(step, carry):
        b, c = lax.rem(step, 3) - 1, lax.div(step, 3) - 1
        for offsets in ((2, b, c), (b, 2, c), (b, c, 2)):
            pick(offsets)
        return carry

    def farthest_rows(step, carry):
        for offsets in ((2, 2, step - 1), (2, step - 1, 2), (step - 1, 2, 2)):
            pick(offsets)
        return carry

    def arrive_across(wanted):
        for part in range(3):
            for b in (0, -1, 1, 2):
                for c in (0, -1, 1, 2):
                    if (b == 2) + (c == 2) == wanted:
                        arrive("d2d", part, b, c)

    for part in range(3):
        d1 = dims(part)[0]
        for way in (2, 1, -1):
            start(("m1", part, way), region(part, {}, whole), device(d1, way), True)
    for part in range(3):
        d2 = dims(part)[1]
        for way in (1, -1, 2):
            arrive("m1", part, way)
        for way in (2, 1, -1):
            start(("m2", part, way), row_of(part, 0, 0), device(d2, way), True)
    for part in range(3):
        whole_row(part, 0)
    for part in range(3):
        for way in (1, -1):
            arrive("m2", part, way)
            whole_row(part, -way)
    for part in range(3):
        for way in (1, -1):
            pass_on(part, 0, way)
    for part in range(3):
        arrive("m2", part, 2)
        whole_row(part, 2)
    for b in (-1, 1):
        for part in range(3):
            for way in (1, -1):
                pass_on(part, b, way)
    arrive_across(0)
    lax.fori_loop(0, 9, near_rows, 0)
    for part in range(3):
        last_row(part, 0)
    for part in range(3):
        for way in (1, -1):
            pass_on(part, 2, way)
    for b in (-1, 1):
        for part in range(3):
            last_row(part, b)
    arrive_across(1)
    lax.fori_loop(0, 9, far_rows, 0)
    for part in range(3):
        last_row(part, 2)
    arrive_across(2)
    lax.fori_loop(0, 3, farthest_rows, 0)
    pick((2, 2, 2))
    if first:
        table_ref[...] = tiles[...]
    for copy in copies.values():
        copy.wait_send()


def send_rows(x, table, layer, own, capacity, call_id, plus, first=False, scaled=False):
    tok_dev, width = x.shape
    devices = 2 * SIDE ** 3
    count = 228 if first else 114
    u_shape = jax.ShapeDtypeStruct((own, devices * capacity, width), x.dtype)
    table_shape = jax.ShapeDtypeStruct((2, SIDE, SIDE, SIDE, 4, 8, 128), F32)
    outs = (u_shape, table_shape) if first else (u_shape, u_shape) if scaled else (u_shape,)
    vmem = pl.BlockSpec(memory_space=pltpu.VMEM)
    hbm = pl.BlockSpec(memory_space=pl.ANY)
    return pl.pallas_call(
        functools.partial(send_kernel, own, capacity, layer, plus, first, scaled),
        out_shape=outs,
        in_specs=[hbm, hbm if first else vmem],
        out_specs=(vmem,) * len(outs),
        scratch_shapes=[
            pltpu.VMEM((2, SIDE, SIDE, SIDE, tok_dev, width), x.dtype),
            pltpu.SemaphoreType.DMA,
            pltpu.SemaphoreType.DMA((count,)),
            pltpu.SemaphoreType.DMA((count,)),
        ] + ([pltpu.VMEM(table_shape.shape, F32)] if first else []),
        compiler_params=pltpu.CompilerParams(collective_id=call_id, has_side_effects=True, vmem_limit_bytes=40 * 1024 * 1024),
        cost_estimate=pl.CostEstimate(flops=3 * 10**10, bytes_accessed=devices * tok_dev * width * 2, transcendentals=0),
        name=f"send_rows_{call_id}",
    )(x, table)


def pair_sum(gated, row_ref, gate_ref, back):
    codes, gates = row_ref[...], gate_ref[...]
    tok_dev = codes.shape[0]
    total = 0.0
    for base, rows in back:
        lane = lax.broadcasted_iota(jnp.int32, (tok_dev, rows.shape[0]), 1) + base
        weight = jnp.zeros(lane.shape, F32)
        for j in range(codes.shape[1]):
            weight = jnp.where(codes[:, j:j + 1] == lane, gates[:, j:j + 1] if gated else 1.0, weight)
        hi = weight.astype(BF16)
        terms = [hi]
        if gated:
            rest = weight - hi.astype(F32)
            mid = rest.astype(BF16)
            terms += [mid, (rest - mid.astype(F32)).astype(BF16)]
        part = jnp.dot(jnp.concatenate(terms, axis=0), rows, preferred_element_type=F32)
        for k in reversed(range(len(terms))):
            total = total + part[k * tok_dev:(k + 1) * tok_dev]
    return total


def combine_kernel(gated, x_ref, row_ref, gate_ref, back_ref, out_ref):
    chunk = 512
    back = ((base, back_ref[pl.ds(base, chunk), :]) for base in range(0, back_ref.shape[0], chunk))
    out_ref[...] = (x_ref[...].astype(F32) + pair_sum(gated, row_ref, gate_ref, back)).astype(out_ref.dtype)


def return_kernel(x_ref, row_ref, gate_ref, rows_ref, line_ref, out_ref, line_out, back, sems):
    me = lax.axis_index("ep")
    devices = rows_ref.shape[0]
    chip, core = lax.div(me, 2), lax.rem(me, 2)
    x, y, z = lax.rem(chip, SIDE), lax.rem(lax.div(chip, SIDE), SIDE), lax.div(chip, SIDE * SIDE)

    def target(step):
        d = lax.rem(step * 37, devices)
        tx = lax.rem(x + lax.rem(lax.div(d, 2), SIDE), SIDE)
        ty = lax.rem(y + lax.rem(lax.div(d, 2 * SIDE), SIDE), SIDE)
        tz = lax.rem(z + lax.div(d, 2 * SIDE * SIDE), SIDE)
        return ((tz * SIDE + ty) * SIDE + tx) * 2 + lax.rem(core + lax.rem(d, 2), 2)

    barrier = pltpu.get_barrier_semaphore()

    def hello(step, carry):
        pl.semaphore_signal(barrier, inc=1, device_id={"ep": target(step)}, device_id_type=pl.DeviceIdType.MESH)
        return carry

    lax.fori_loop(1, devices, hello, 0)
    pl.semaphore_wait(barrier, devices - 1)

    def send(step, carry):
        to = target(step)
        for src, dst, k in ((rows_ref, back, 0), (line_ref, line_out, 2)):
            pltpu.make_async_remote_copy(src_ref=src.at[to], dst_ref=dst.at[me], send_sem=sems.at[k], recv_sem=sems.at[k + 1], device_id={"ep": to}, device_id_type=pl.DeviceIdType.MESH).start()
        return carry

    lax.fori_loop(1, devices, send, 0)
    back[me] = rows_ref[me]
    line_out[me] = line_ref[me]
    others = pl.ds(0, devices - 1)
    for src, dst, k in ((rows_ref, back, 0), (line_ref, line_out, 2)):
        for sem in (sems.at[k], sems.at[k + 1]):
            pltpu.make_async_copy(src.at[others], dst.at[others], sem).wait()
    group = 16
    count, width = rows_ref.shape[1], rows_ref.shape[2]
    blocks = ((g * count, back[pl.ds(g, group)].reshape(group * count, width)) for g in range(0, devices, group))
    out_ref[...] = (x_ref[...].astype(F32) + pair_sum(False, row_ref, gate_ref, blocks)).astype(out_ref.dtype)


def return_home(x, rows, gates, sent, lines, call_id):
    vmem = pl.BlockSpec(memory_space=pltpu.VMEM)
    return pl.pallas_call(
        return_kernel,
        out_shape=(jax.ShapeDtypeStruct(x.shape, x.dtype), jax.ShapeDtypeStruct(lines.shape, lines.dtype)),
        in_specs=[vmem] * 5,
        out_specs=(vmem, vmem),
        scratch_shapes=[pltpu.VMEM(sent.shape, sent.dtype), pltpu.SemaphoreType.DMA((4,))],
        compiler_params=pltpu.CompilerParams(collective_id=call_id, has_side_effects=True, vmem_limit_bytes=32 * 1024 * 1024),
        cost_estimate=pl.CostEstimate(flops=3 * 10**10, bytes_accessed=sent.size * 4, transcendentals=0),
        name="return_home",
    )(x, rows, gates, sent, lines)


def combine(x, rows, gates, back, gated):
    tok_dev, width = x.shape
    flops = 2 * tok_dev * back.shape[0] * width
    return pl.pallas_call(
        functools.partial(combine_kernel, gated),
        out_shape=jax.ShapeDtypeStruct(x.shape, x.dtype),
        in_specs=[pl.BlockSpec(memory_space=pltpu.VMEM)] * 4,
        out_specs=pl.BlockSpec(memory_space=pltpu.VMEM),
        compiler_params=pltpu.CompilerParams(vmem_limit_bytes=24 * 1024 * 1024),
        cost_estimate=pl.CostEstimate(flops=flops * (3 if gated else 1), bytes_accessed=back.size * 2, transcendentals=0),
        name="combine",
    )(x, rows, gates, back)


def forward_rows(u, w_both, w_down):
    ff = w_down.shape[0]
    pre = jnp.dot(u, w_both, preferred_element_type=F32)
    pre_gate, pre_up = pre[:, :ff], pre[:, ff:]
    sig = 1.0 / (1.0 + jnp.exp(-pre_gate))
    silu = pre_gate * sig
    hidden = (silu * pre_up).astype(BF16)
    out = jnp.dot(hidden, w_down, preferred_element_type=F32)
    return pre_gate, pre_up, sig, silu, hidden, out


def store_home(out_ref, step, rows):
    count, width = rows.shape
    slots = out_ref.shape[1]
    sources = count // slots
    out_ref[pl.ds(step * sources, sources)] = rows.reshape(sources, slots, width).astype(out_ref.dtype)


def forward_kernel(chunk, u_ref, w1_ref, w3_ref, w2_ref, out_ref):
    w_both = jnp.concatenate([w1_ref[0], w3_ref[0]], axis=1)

    def body(step, carry):
        rows = pl.ds(pl.multiple_of(step * chunk, chunk), chunk)
        out = forward_rows(u_ref[0, rows, :], w_both, w2_ref[0])[-1]
        store_home(out_ref, step, out)
        return carry

    lax.fori_loop(0, u_ref.shape[1] // chunk, body, 0)


def backward_kernel(chunk, u_ref, dy_ref, q_ref, w1_ref, w3_ref, w2_ref, du_ref, dgate_ref, hidden_ref, da_ref, db_ref):
    ff = w2_ref.shape[1]
    w_both = jnp.concatenate([w1_ref[0], w3_ref[0]], axis=1)
    last = (((1,), (1,)), ((), ()))

    def body(step, carry):
        rows = pl.ds(pl.multiple_of(step * chunk, chunk), chunk)
        pre_gate, pre_up, sig, silu, hidden, out = forward_rows(u_ref[0, rows, :], w_both, w2_ref[0])
        dgate = jnp.sum(dy_ref[0, rows, :].astype(F32) * out.astype(BF16).astype(F32), axis=1, keepdims=True)
        diagonal = lax.broadcasted_iota(jnp.int32, (128, 128), 0) == lax.broadcasted_iota(jnp.int32, (128, 128), 1)
        for k in range(chunk // 128):
            line = jnp.sum(jnp.where(diagonal, dgate[k * 128:(k + 1) * 128], 0.0), axis=0, keepdims=True)
            dgate_ref[0, pl.ds(step * (chunk // 128) + k, 1), :] = line
        d_hidden = lax.dot_general(q_ref[0, rows, :], w2_ref[0], last, preferred_element_type=F32)
        da = (d_hidden * pre_up * sig * (1.0 + pre_gate * (1.0 - sig))).astype(BF16)
        db = (d_hidden * silu).astype(BF16)
        hidden_ref[0, rows, :] = hidden
        da_ref[0, rows, :] = da
        db_ref[0, rows, :] = db
        both = jnp.concatenate([da, db], axis=1)
        store_home(du_ref, step, lax.dot_general(both, w_both, last, preferred_element_type=F32))
        return carry

    lax.fori_loop(0, u_ref.shape[1] // chunk, body, 0)


def expert_call(kernel, inputs, outs, weights, n_group, name):
    own, count, width = inputs[0].shape
    ff = weights[2].shape[1]
    slots = count // n_group

    def each(shape):
        return pl.BlockSpec((1,) + shape, lambda e: (e, 0, 0))

    home = (jax.ShapeDtypeStruct((n_group, own * slots, width), BF16), pl.BlockSpec((n_group, slots, width), lambda e: (0, e, 0)))
    kinds = {
        "home": home,
        "gate": (jax.ShapeDtypeStruct((own, count // 128, 128), F32), each((count // 128, 128))),
        "ff": (jax.ShapeDtypeStruct((own, count, ff), BF16), each((count, ff))),
    }
    steps = 3 if len(outs) == 1 else 8
    return pl.pallas_call(
        functools.partial(kernel, 256),
        out_shape=tuple(kinds[k][0] for k in outs),
        grid=(own,),
        in_specs=[each((count, width))] * len(inputs) + [each((width, ff)), each((width, ff)), each((ff, width))],
        out_specs=tuple(kinds[k][1] for k in outs),
        compiler_params=pltpu.CompilerParams(vmem_limit_bytes=32 * 1024 * 1024),
        cost_estimate=pl.CostEstimate(flops=2 * steps * own * count * width * ff, bytes_accessed=own * count * width * 2 * (len(inputs) + 1), transcendentals=own * count * ff),
        name=name,
    )(*inputs, *weights)


def expert_forward(u_rows, weights, n_group):
    return expert_call(forward_kernel, (u_rows,), ("home",), weights, n_group, "expert_forward")[0]


def expert_backward(u_rows, dy_rows, q_rows, weights, n_group):
    outs = ("home", "gate", "ff", "ff", "ff")
    du, dgate, hidden, da, db = expert_call(backward_kernel, (u_rows, dy_rows, q_rows), outs, weights, n_group, "expert_backward")

    def grads(u_rows, q_rows, hidden, da, db):
        dw_gate = jnp.einsum("erd,erf->edf", u_rows, da, preferred_element_type=F32)
        dw_up = jnp.einsum("erd,erf->edf", u_rows, db, preferred_element_type=F32)
        dw_down = jnp.einsum("erf,erd->efd", hidden, q_rows, preferred_element_type=F32)
        return dw_gate, dw_up, dw_down

    return du, dgate, grads(u_rows, q_rows, hidden, da, db)


def solution(mesh):
    n_group = mesh.shape["ep"]
    tok_spec = P(("dp", "ep"))
    w_spec = P("ep")

    def device_program(x_in, idx_a, idx_b, gate_a, gate_b, dy_out, w1_a, w3_a, w2_a, w1_b, w3_b, w2_b):
        tok_dev, top_k = idx_a.shape
        width = x_in.shape[1]
        own = w1_a.shape[0]
        capacity = CAP_FACTOR * tok_dev * top_k // (own * n_group)
        total = own * n_group * capacity
        block = own * capacity

        rows_a = pair_rows(idx_a, capacity)
        rows_b = pair_rows(idx_b, capacity)
        pad = ((0, 0), (0, 128 - tok_dev))
        tile = jnp.stack([jnp.pad(rows_a.T.astype(F32), pad, constant_values=-1.0), jnp.pad(rows_b.T.astype(F32), pad, constant_values=-1.0), jnp.pad(gate_a.T, pad), jnp.pad(gate_b.T, pad)])
        third = tok_dev // 3
        even = third // 2
        u_a, table = send_rows(x_in, tile, 0, own, capacity, 0, even, first=True)

        def send_back(rows):
            return lax.all_to_all(rows, "ep", 0, 0, tiled=True).reshape(total, width)

        def by_home(dgate_rows):
            return dgate_rows.reshape(own, n_group, capacity).transpose(1, 0, 2).reshape(n_group, block)

        def look_up(back, rows):
            flat = rows.reshape(-1)
            expert = lax.div(flat, capacity)[:, None] == jnp.arange(own * n_group, dtype=jnp.int32)[None, :]
            picked = jnp.dot(expert.astype(F32), back.reshape(own * n_group, capacity), precision=lax.Precision.HIGHEST)
            slot = lax.rem(flat, capacity)[:, None] == jnp.arange(capacity, dtype=jnp.int32)[None, :]
            return jnp.sum(jnp.where(slot, picked, 0.0), axis=1).reshape(rows.shape)

        weights_a, weights_b = (w1_a, w3_a, w2_a), (w1_b, w3_b, w2_b)
        back_a = send_back(expert_forward(u_a, weights_a, n_group))
        dy_b, q_b = send_rows(dy_out, table, 1, own, capacity, 1, even, scaled=True)
        x_mid = combine(x_in, rows_a, gate_a, back_a, True)
        u_b, = send_rows(x_mid, table, 1, own, capacity, 2, even)
        out_b = expert_forward(u_b, weights_b, n_group)
        du_b, dgate_rows_b, grads_b = expert_backward(u_b, dy_b, q_b, weights_b, n_group)
        x_again, du_b = lax.optimization_barrier((x_in, du_b))
        u_again, = send_rows(x_again, table, 0, own, capacity, 3, even)
        dx_mid = combine(dy_out, rows_b, gate_b, send_back(du_b), False)
        dy_a, q_a = send_rows(dx_mid, table, 0, own, capacity, 4, even, scaled=True)
        x_out = combine(x_mid, rows_b, gate_b, send_back(out_b), True)
        du_a, dgate_rows_a, grads_a = expert_backward(u_again, dy_a, q_a, weights_a, n_group)
        lines = jnp.concatenate([by_home(dgate_rows_a), by_home(dgate_rows_b)], axis=1)
        lines = jnp.pad(lines, ((0, 0), (0, 128 - 2 * block)))[:, None, :]
        dx_in, lines = return_home(dx_mid, rows_a, gate_a, du_a, lines, 5)
        dgate_a = look_up(lines[:, 0, :block], rows_a)
        dgate_b = look_up(lines[:, 0, block:2 * block], rows_b)
        return (x_out, dx_in) + tuple(grads_a) + tuple(grads_b) + (dgate_a, dgate_b)

    return jax.shard_map(device_program, mesh=mesh, in_specs=(tok_spec,) * 6 + (w_spec,) * 6, out_specs=(tok_spec,) * 10, check_vma=False)
```

```python
import functools

import jax
import jax.numpy as jnp
from jax import lax
from jax.experimental import pallas as pl
from jax.experimental.pallas import tpu as pltpu
from jax.sharding import PartitionSpec as P

CAP_FACTOR = 4
F32 = jnp.float32
BF16 = jnp.bfloat16


def pair_rows(ids, capacity):
    flat = ids.reshape(-1)
    pair = jnp.arange(flat.shape[0], dtype=jnp.int32)
    earlier = (flat[None, :] == flat[:, None]) & (pair[None, :] < pair[:, None])
    slot = jnp.sum(earlier.astype(jnp.int32), axis=1)
    return (flat * capacity + slot).reshape(ids.shape)


SIDE = 4


def my_place():
    me = lax.axis_index("ep")
    chip = lax.div(me, 2)
    at = (lax.rem(chip, SIDE), lax.rem(lax.div(chip, SIDE), SIDE), lax.div(chip, SIDE * SIDE))
    return me, lax.rem(me, 2), at


def device_at(at, core, delta, flip):
    c = [a if d == 0 else lax.rem(a + d + SIDE, SIDE) for a, d in zip(at, delta)]
    return ((c[2] * SIDE + c[1]) * SIDE + c[0]) * 2 + (1 - core if flip else core)


def return_offsets():
    direct, relayed = [], []
    devices = 2 * SIDE ** 3
    for step in range(1, devices):
        d = step * 37 % devices
        flip, delta = d % 2, (d // 2 % SIDE, d // (2 * SIDE) % SIDE, d // (2 * SIDE * SIDE))
        delta = tuple(v if v <= 2 else v - SIDE for v in delta)
        if 2 in delta:
            way = 1 if flip == 0 else -1
            delta = tuple(2 * way if v == 2 else v for v in delta)
            relayed.append((delta, flip, tuple(way if abs(v) == 2 else 0 for v in delta)))
        else:
            direct.append((delta, flip))
    return direct, relayed


RELAYS = len(return_offsets()[1])


def greet_all(me, core, at):
    barrier = pltpu.get_barrier_semaphore()
    devices = 2 * SIDE ** 3

    def hello(step, carry):
        pl.semaphore_signal(barrier, inc=1, device_id={"ep": lax.rem(me + step, devices)}, device_id_type=pl.DeviceIdType.MESH)
        return carry

    lax.fori_loop(1, devices, hello, 0)
    pl.semaphore_wait(barrier, devices - 1)


def return_steps(me, core, at, rows_ref, back, relay, sems, relay_sems):
    direct, relayed = return_offsets()
    devices = rows_ref.shape[0]

    def copy(src, dst, send_sem, recv_sem, to):
        return pltpu.make_async_remote_copy(src_ref=src, dst_ref=dst, send_sem=send_sem, recv_sem=recv_sem, device_id={"ep": to}, device_id_type=pl.DeviceIdType.MESH)

    def to_relay(k):
        delta, flip, via = relayed[k]
        return copy(rows_ref.at[device_at(at, core, delta, flip)], relay.at[k], sems.at[0], relay_sems.at[k], device_at(at, core, via, 0))

    def send_direct(k):
        to = device_at(at, core, *direct[k])
        copy(rows_ref.at[to], back.at[me], sems.at[1], sems.at[2], to).start()

    def forward(k):
        delta, flip, via = relayed[k]
        to_relay(k).wait_recv()
        origin = device_at(at, core, tuple(-v for v in via), 0)
        to = device_at(at, core, tuple(d - v for d, v in zip(delta, via)), flip)
        copy(relay.at[k], back.at[origin], sems.at[1], sems.at[2], to).start()

    def finish():
        back[me] = rows_ref[me]
        others = pl.ds(0, devices - 1)
        pltpu.make_async_copy(rows_ref.at[others], back.at[others], sems.at[2]).wait()
        pltpu.make_async_copy(rows_ref.at[others], back.at[others], sems.at[1]).wait()
        relays = pl.ds(0, len(relayed))
        pltpu.make_async_copy(rows_ref.at[relays], relay.at[relays], sems.at[0]).wait()

    def pieces(count, action, parts):
        cut = [count * i // parts for i in range(parts + 1)]
        return [lambda lo=lo, hi=hi: [action(k) for k in range(lo, hi)] for lo, hi in zip(cut, cut[1:])]

    vias = pieces(len(relayed), lambda k: to_relay(k).start(), 4)
    directs = pieces(len(direct), send_direct, 4)
    forwards = pieces(len(relayed), forward, 8)
    return vias, directs, forwards, finish


def home_blocks(back):
    group = 16
    count, width = back.shape[1], back.shape[2]
    return ((g * count, back[pl.ds(g, group)].reshape(group * count, width)) for g in range(0, back.shape[0], group))


def send_kernel(own, capacity, layer, first, scaled, returning, *refs):
    refs = list(refs)
    x_ref, tile_ref = refs.pop(0), refs.pop(0)
    if returning:
        base_ref, row_ref, gate_ref, rows_ref = (refs.pop(0) for _ in range(4))
    u_ref = refs.pop(0)
    if scaled:
        q_ref = refs.pop(0)
    if first:
        table_ref = refs.pop(0)
    if returning:
        home_ref = refs.pop(0)
    held, local_sem, send_sem, recv_sem = (refs.pop(0) for _ in range(4))
    tiles = refs.pop(0) if first else tile_ref
    if returning:
        back, relay, return_sems, relay_sems = refs
    me, core, at = my_place()
    plus = x_ref.shape[0] // 6
    third = x_ref.shape[0] // 3
    spans = {1: (0, plus), -1: (plus, third - plus)}

    def device(dim, step):
        return device_at(at, core, [step if d == dim else 0 for d in range(3)], 0)

    partner = device_at(at, core, (0, 0, 0), 1)

    def region(part, pos, span):
        idx = [pos[d] if d in pos else at[d] for d in range(3)]
        idx = [pl.ds(0, SIDE) if i is None else i for i in idx]
        where = (core, idx[2], idx[1], idx[0])
        return held.at[where + (pl.ds(part * third + span[0], span[1]),)], where + (pl.ds(part, 2 if part == 2 else 1),)

    copies = {}

    def start(key, refs, to, with_tile):
        for kind, ref in (("x", refs[0]), ("t", tiles.at[refs[1]])):
            if kind == "t" and not (first and with_tile):
                continue
            n = len(copies)
            copy = pltpu.make_async_remote_copy(src_ref=ref, dst_ref=ref, send_sem=send_sem.at[n], recv_sem=recv_sem.at[n], device_id={"ep": to}, device_id_type=pl.DeviceIdType.MESH)
            copy.start()
            copies[key + (kind,)] = copy

    def arrive(*key):
        for kind in ("x", "t"):
            if key + (kind,) in copies:
                copies[key + (kind,)].wait_recv()

    mine = pltpu.make_async_copy(x_ref, held.at[core, at[2], at[1], at[0]], local_sem)
    mine.start()
    if first:
        own_tile = pltpu.make_async_copy(tile_ref, tiles.at[core, at[2], at[1], at[0]], send_sem.at[0])
        own_tile.start()
        own_tile.wait()
    if returning:
        greet_all(me, core, at)
        mine.wait()
    else:
        barrier = pltpu.get_barrier_semaphore()
        for dim in range(3):
            for step in (1, -1, 2):
                pl.semaphore_signal(barrier, inc=1, device_id={"ep": device(dim, step)}, device_id_type=pl.DeviceIdType.MESH)
        pl.semaphore_signal(barrier, inc=1, device_id={"ep": partner}, device_id_type=pl.DeviceIdType.MESH)
        mine.wait()
        pl.semaphore_wait(barrier, 10)

    def dims(part):
        return part, (part + 1) % 3, (part + 2) % 3

    def shift(dim, step):
        return lax.rem(at[dim] + step + SIDE, SIDE)

    whole = (0, third)

    def row_of(part, b, c, span=whole):
        d1, d2, d3 = dims(part)
        return region(part, {d1: None, d2: shift(d2, b), d3: shift(d3, c)}, span)

    def across(part, b, c):
        start(("d2d", part, b, c), row_of(part, b, c), partner, True)

    def whole_row(part, b):
        d3 = dims(part)[2]
        for way in (1, -1):
            start(("m3", part, b, way), row_of(part, b, 0), device(d3, way), True)
        across(part, b, 0)

    def pass_on(part, b, way):
        d3 = dims(part)[2]
        arrive("m3", part, b, way)
        start(("f3", part, b, way), row_of(part, b, -way, spans[way]), device(d3, way), way == -1)
        across(part, b, -way)

    def last_row(part, b):
        for way in (1, -1):
            arrive("f3", part, b, way)
        across(part, b, 2)

    block = own * capacity
    slot = lax.broadcasted_iota(jnp.int32, (block, 128), 0) + me * block
    tok_dev = x_ref.shape[0]

    def pick(offsets):
        x, y, z = (lax.rem(at[d] + offsets[d] + SIDE, SIDE) for d in range(3))
        rows, scaled_rows = [], []
        for c in range(2):
            code = tiles[c, z, y, x, layer].astype(jnp.int32)
            gate = tiles[c, z, y, x, 2 + layer] if scaled else None
            hit = code[0:1, :] == slot
            weight = jnp.where(hit, gate[0:1, :], 0.0) if scaled else None
            for j in range(1, code.shape[0]):
                hit_j = code[j:j + 1, :] == slot
                hit = hit | hit_j
                if scaled:
                    weight = jnp.where(hit_j, gate[j:j + 1, :], weight)
            onehot = jnp.where(hit, 1.0, 0.0)[:, :tok_dev].astype(BF16)
            rows.append(jnp.dot(onehot, held[c, z, y, x], preferred_element_type=F32))
            if scaled:
                scaled_rows.append(jnp.sum(weight, axis=1, keepdims=True) * rows[-1])
        place = ((z * SIDE + y) * SIDE + x) * 2 * capacity
        for out_ref, parts in ((u_ref, rows),) + (((q_ref, scaled_rows),) if scaled else ()):
            for e in range(own):
                both = jnp.concatenate([r[e * capacity:(e + 1) * capacity] for r in parts], axis=0)
                out_ref[e, pl.ds(pl.multiple_of(place, 2 * capacity), 2 * capacity), :] = both.astype(BF16)

    def near_rows(step, carry):
        for k in (-1, 0, 1):
            pick((k, lax.rem(step, 3) - 1, lax.div(step, 3) - 1))
        return carry

    def far_rows(step, carry):
        b, c = lax.rem(step, 3) - 1, lax.div(step, 3) - 1
        for offsets in ((2, b, c), (b, 2, c), (b, c, 2)):
            pick(offsets)
        return carry

    def farthest_rows(step, carry):
        for offsets in ((2, 2, step - 1), (2, step - 1, 2), (step - 1, 2, 2)):
            pick(offsets)
        return carry

    def arrive_across(wanted):
        for part in range(3):
            for b in (0, -1, 1, 2):
                for c in (0, -1, 1, 2):
                    if (b == 2) + (c == 2) == wanted:
                        arrive("d2d", part, b, c)

    def first_sends():
        for part in range(3):
            for way in (2, 1, -1):
                start(("m1", part, way), region(part, {}, whole), device(dims(part)[0], way), True)

    def second_sends():
        for part in range(3):
            for way in (1, -1, 2):
                arrive("m1", part, way)
            for way in (2, 1, -1):
                start(("m2", part, way), row_of(part, 0, 0), device(dims(part)[1], way), True)

    def own_rows():
        for part in range(3):
            whole_row(part, 0)

    def near_sends():
        for part in range(3):
            for way in (1, -1):
                arrive("m2", part, way)
                whole_row(part, -way)

    def pass_rows(b):
        for part in range(3):
            for way in (1, -1):
                pass_on(part, b, way)

    def opposite_rows():
        for part in range(3):
            arrive("m2", part, 2)
            whole_row(part, 2)

    def last_rows(b):
        for part in range(3):
            last_row(part, b)

    def pick_near():
        arrive_across(0)
        lax.fori_loop(0, 9, near_rows, 0)

    def pick_far():
        arrive_across(1)
        lax.fori_loop(0, 9, far_rows, 0)

    gathering = [first_sends, second_sends, own_rows, near_sends, lambda: pass_rows(0), opposite_rows, lambda: pass_rows(-1), lambda: pass_rows(1), pick_near, lambda: last_rows(0), lambda: pass_rows(2), lambda: last_rows(-1), lambda: last_rows(1), pick_far]
    between = {}
    if returning:
        vias, directs, forwards, finish = return_steps(me, core, at, rows_ref, back, relay, return_sems, relay_sems)
        between = {0: vias[:1], 1: vias[1:2], 2: vias[2:3], 3: vias[3:] + directs[:1], 4: forwards[:1] + directs[1:2], 5: forwards[1:2] + directs[2:3], 6: forwards[2:4] + directs[3:], 7: forwards[4:5], 8: forwards[5:7], 9: forwards[7:]}
    for n, step in enumerate(gathering):
        step()
        for extra in between.get(n, []):
            extra()
    last_rows(2)
    arrive_across(2)
    lax.fori_loop(0, 3, farthest_rows, 0)
    pick((2, 2, 2))
    if returning:
        finish()
        total = pair_sum(returning == "gated", row_ref, gate_ref, home_blocks(back))
        home_ref[...] = (base_ref[...].astype(F32) + total).astype(home_ref.dtype)
    if first:
        table_ref[...] = tiles[...]
    for copy in copies.values():
        copy.wait_send()


def return_scratch(sent):
    return [pltpu.VMEM(sent.shape, sent.dtype), pltpu.VMEM((RELAYS,) + sent.shape[1:], sent.dtype), pltpu.SemaphoreType.DMA((5,)), pltpu.SemaphoreType.DMA((RELAYS,))]


def send_rows(x, table, layer, own, capacity, call_id, first=False, scaled=False, home=None, gated=False):
    tok_dev, width = x.shape
    devices = 2 * SIDE ** 3
    count = 228 if first else 114
    u_shape = jax.ShapeDtypeStruct((own, devices * capacity, width), x.dtype)
    table_shape = jax.ShapeDtypeStruct((2, SIDE, SIDE, SIDE, 4, 8, 128), F32)
    outs = (u_shape,) + (u_shape,) * scaled + (table_shape,) * first
    if home:
        outs += (jax.ShapeDtypeStruct(home[0].shape, home[0].dtype),)
    vmem = pl.BlockSpec(memory_space=pltpu.VMEM)
    hbm = pl.BlockSpec(memory_space=pl.ANY)
    returning = None if home is None else "gated" if gated else "plain"
    return pl.pallas_call(
        functools.partial(send_kernel, own, capacity, layer, first, scaled, returning),
        out_shape=outs,
        in_specs=[hbm, hbm if first else vmem] + [vmem] * (4 if home else 0),
        out_specs=(vmem,) * len(outs),
        scratch_shapes=[
            pltpu.VMEM((2, SIDE, SIDE, SIDE, tok_dev, width), x.dtype),
            pltpu.SemaphoreType.DMA,
            pltpu.SemaphoreType.DMA((count,)),
            pltpu.SemaphoreType.DMA((count,)),
        ] + ([pltpu.VMEM(table_shape.shape, F32)] if first else []) + (return_scratch(home[3]) if home else []),
        compiler_params=pltpu.CompilerParams(collective_id=call_id, has_side_effects=True, vmem_limit_bytes=46 * 1024 * 1024),
        cost_estimate=pl.CostEstimate(flops=3 * 10**10, bytes_accessed=devices * tok_dev * width * 2, transcendentals=0),
        name=f"send_rows_{call_id}",
    )(x, table, *(home or ()))


def pair_sum(gated, row_ref, gate_ref, back):
    codes, gates = row_ref[...], gate_ref[...]
    tok_dev = codes.shape[0]
    total = 0.0
    for base, rows in back:
        lane = lax.broadcasted_iota(jnp.int32, (tok_dev, rows.shape[0]), 1) + base
        weight = jnp.zeros(lane.shape, F32)
        for j in range(codes.shape[1]):
            weight = jnp.where(codes[:, j:j + 1] == lane, gates[:, j:j + 1] if gated else 1.0, weight)
        hi = weight.astype(BF16)
        terms = [hi]
        if gated:
            rest = weight - hi.astype(F32)
            mid = rest.astype(BF16)
            terms += [mid, (rest - mid.astype(F32)).astype(BF16)]
        part = jnp.dot(jnp.concatenate(terms, axis=0), rows, preferred_element_type=F32)
        for k in reversed(range(len(terms))):
            total = total + part[k * tok_dev:(k + 1) * tok_dev]
    return total


def return_kernel(x_ref, row_ref, gate_ref, rows_ref, line_ref, out_ref, line_out, back, relay, sems, relay_sems):
    me, core, at = my_place()
    devices = rows_ref.shape[0]
    greet_all(me, core, at)
    vias, directs, forwards, finish = return_steps(me, core, at, rows_ref, back, relay, sems, relay_sems)

    def send_line(step, carry):
        to = lax.rem(me + step, devices)
        pltpu.make_async_remote_copy(src_ref=line_ref.at[to], dst_ref=line_out.at[me], send_sem=sems.at[3], recv_sem=sems.at[4], device_id={"ep": to}, device_id_type=pl.DeviceIdType.MESH).start()
        return carry

    for step in vias + directs[:2] + forwards[:2] + directs[2:] + forwards[2:]:
        step()
    lax.fori_loop(1, devices, send_line, 0)
    line_out[me] = line_ref[me]
    finish()
    others = pl.ds(0, devices - 1)
    for k in (3, 4):
        pltpu.make_async_copy(line_ref.at[others], line_out.at[others], sems.at[k]).wait()
    out_ref[...] = (x_ref[...].astype(F32) + pair_sum(False, row_ref, gate_ref, home_blocks(back))).astype(out_ref.dtype)


def return_home(x, rows, gates, sent, lines, call_id):
    vmem = pl.BlockSpec(memory_space=pltpu.VMEM)
    return pl.pallas_call(
        return_kernel,
        out_shape=(jax.ShapeDtypeStruct(x.shape, x.dtype), jax.ShapeDtypeStruct(lines.shape, lines.dtype)),
        in_specs=[vmem] * 5,
        out_specs=(vmem, vmem),
        scratch_shapes=return_scratch(sent),
        compiler_params=pltpu.CompilerParams(collective_id=call_id, has_side_effects=True, vmem_limit_bytes=32 * 1024 * 1024),
        cost_estimate=pl.CostEstimate(flops=3 * 10**10, bytes_accessed=sent.size * 4, transcendentals=0),
        name="return_home",
    )(x, rows, gates, sent, lines)


def combine(x, rows, gates, back, gated):
    tok_dev, width = x.shape
    flops = 2 * tok_dev * back.shape[0] * width
    return pl.pallas_call(
        functools.partial(combine_kernel, gated),
        out_shape=jax.ShapeDtypeStruct(x.shape, x.dtype),
        in_specs=[pl.BlockSpec(memory_space=pltpu.VMEM)] * 4,
        out_specs=pl.BlockSpec(memory_space=pltpu.VMEM),
        compiler_params=pltpu.CompilerParams(vmem_limit_bytes=24 * 1024 * 1024),
        cost_estimate=pl.CostEstimate(flops=flops * (3 if gated else 1), bytes_accessed=back.size * 2, transcendentals=0),
        name="combine",
    )(x, rows, gates, back)


def forward_rows(u, w_both, w_down):
    ff = w_down.shape[0]
    pre = jnp.dot(u, w_both, preferred_element_type=F32)
    pre_gate, pre_up = pre[:, :ff], pre[:, ff:]
    sig = 1.0 / (1.0 + jnp.exp(-pre_gate))
    silu = pre_gate * sig
    hidden = (silu * pre_up).astype(BF16)
    out = jnp.dot(hidden, w_down, preferred_element_type=F32)
    return pre_gate, pre_up, sig, silu, hidden, out


def store_home(out_ref, step, rows):
    count, width = rows.shape
    slots = out_ref.shape[1]
    sources = count // slots
    out_ref[pl.ds(step * sources, sources)] = rows.reshape(sources, slots, width).astype(out_ref.dtype)


def forward_kernel(chunk, u_ref, w1_ref, w3_ref, w2_ref, out_ref):
    w_both = jnp.concatenate([w1_ref[0], w3_ref[0]], axis=1)

    def body(step, carry):
        rows = pl.ds(pl.multiple_of(step * chunk, chunk), chunk)
        out = forward_rows(u_ref[0, rows, :], w_both, w2_ref[0])[-1]
        store_home(out_ref, step, out)
        return carry

    lax.fori_loop(0, u_ref.shape[1] // chunk, body, 0)


def backward_kernel(chunk, u_ref, dy_ref, q_ref, w1_ref, w3_ref, w2_ref, du_ref, dgate_ref, hidden_ref, da_ref, db_ref):
    ff = w2_ref.shape[1]
    w_both = jnp.concatenate([w1_ref[0], w3_ref[0]], axis=1)
    last = (((1,), (1,)), ((), ()))

    def body(step, carry):
        rows = pl.ds(pl.multiple_of(step * chunk, chunk), chunk)
        pre_gate, pre_up, sig, silu, hidden, out = forward_rows(u_ref[0, rows, :], w_both, w2_ref[0])
        dgate = jnp.sum(dy_ref[0, rows, :].astype(F32) * out.astype(BF16).astype(F32), axis=1, keepdims=True)
        diagonal = lax.broadcasted_iota(jnp.int32, (128, 128), 0) == lax.broadcasted_iota(jnp.int32, (128, 128), 1)
        for k in range(chunk // 128):
            line = jnp.sum(jnp.where(diagonal, dgate[k * 128:(k + 1) * 128], 0.0), axis=0, keepdims=True)
            dgate_ref[0, pl.ds(step * (chunk // 128) + k, 1), :] = line
        d_hidden = lax.dot_general(q_ref[0, rows, :], w2_ref[0], last, preferred_element_type=F32)
        da = (d_hidden * pre_up * sig * (1.0 + pre_gate * (1.0 - sig))).astype(BF16)
        db = (d_hidden * silu).astype(BF16)
        hidden_ref[0, rows, :] = hidden
        da_ref[0, rows, :] = da
        db_ref[0, rows, :] = db
        both = jnp.concatenate([da, db], axis=1)
        store_home(du_ref, step, lax.dot_general(both, w_both, last, preferred_element_type=F32))
        return carry

    lax.fori_loop(0, u_ref.shape[1] // chunk, body, 0)


def expert_call(kernel, inputs, outs, weights, n_group, name):
    own, count, width = inputs[0].shape
    ff = weights[2].shape[1]
    slots = count // n_group

    def each(shape):
        return pl.BlockSpec((1,) + shape, lambda e: (e, 0, 0))

    home = (jax.ShapeDtypeStruct((n_group, own * slots, width), BF16), pl.BlockSpec((n_group, slots, width), lambda e: (0, e, 0)))
    kinds = {
        "home": home,
        "gate": (jax.ShapeDtypeStruct((own, count // 128, 128), F32), each((count // 128, 128))),
        "ff": (jax.ShapeDtypeStruct((own, count, ff), BF16), each((count, ff))),
    }
    steps = 3 if len(outs) == 1 else 8
    return pl.pallas_call(
        functools.partial(kernel, 256),
        out_shape=tuple(kinds[k][0] for k in outs),
        grid=(own,),
        in_specs=[each((count, width))] * len(inputs) + [each((width, ff)), each((width, ff)), each((ff, width))],
        out_specs=tuple(kinds[k][1] for k in outs),
        compiler_params=pltpu.CompilerParams(vmem_limit_bytes=32 * 1024 * 1024),
        cost_estimate=pl.CostEstimate(flops=2 * steps * own * count * width * ff, bytes_accessed=own * count * width * 2 * (len(inputs) + 1), transcendentals=own * count * ff),
        name=name,
    )(*inputs, *weights)


def expert_forward(u_rows, weights, n_group):
    return expert_call(forward_kernel, (u_rows,), ("home",), weights, n_group, "expert_forward")[0]


def expert_backward(u_rows, dy_rows, q_rows, weights, n_group):
    outs = ("home", "gate", "ff", "ff", "ff")
    du, dgate, hidden, da, db = expert_call(backward_kernel, (u_rows, dy_rows, q_rows), outs, weights, n_group, "expert_backward")

    def grads(u_rows, q_rows, hidden, da, db):
        dw_gate = jnp.einsum("erd,erf->edf", u_rows, da, preferred_element_type=F32)
        dw_up = jnp.einsum("erd,erf->edf", u_rows, db, preferred_element_type=F32)
        dw_down = jnp.einsum("erf,erd->efd", hidden, q_rows, preferred_element_type=F32)
        return dw_gate, dw_up, dw_down

    return du, dgate, grads(u_rows, q_rows, hidden, da, db)


def solution(mesh):
    n_group = mesh.shape["ep"]
    tok_spec = P(("dp", "ep"))
    w_spec = P("ep")

    def device_program(x_in, idx_a, idx_b, gate_a, gate_b, dy_out, w1_a, w3_a, w2_a, w1_b, w3_b, w2_b):
        tok_dev, top_k = idx_a.shape
        width = x_in.shape[1]
        own = w1_a.shape[0]
        capacity = CAP_FACTOR * tok_dev * top_k // (own * n_group)
        total = own * n_group * capacity
        block = own * capacity

        rows_a = pair_rows(idx_a, capacity)
        rows_b = pair_rows(idx_b, capacity)
        pad = ((0, 0), (0, 128 - tok_dev))
        tile = jnp.stack([jnp.pad(rows_a.T.astype(F32), pad, constant_values=-1.0), jnp.pad(rows_b.T.astype(F32), pad, constant_values=-1.0), jnp.pad(gate_a.T, pad), jnp.pad(gate_b.T, pad)])
        u_a, table = send_rows(x_in, tile, 0, own, capacity, 0, first=True)

        def by_home(dgate_rows):
            return dgate_rows.reshape(own, n_group, capacity).transpose(1, 0, 2).reshape(n_group, block)

        def look_up(back, rows):
            flat = rows.reshape(-1)
            expert = lax.div(flat, capacity)[:, None] == jnp.arange(own * n_group, dtype=jnp.int32)[None, :]
            picked = jnp.dot(expert.astype(F32), back.reshape(own * n_group, capacity), precision=lax.Precision.HIGHEST)
            slot = lax.rem(flat, capacity)[:, None] == jnp.arange(capacity, dtype=jnp.int32)[None, :]
            return jnp.sum(jnp.where(slot, picked, 0.0), axis=1).reshape(rows.shape)

        weights_a, weights_b = (w1_a, w3_a, w2_a), (w1_b, w3_b, w2_b)
        out_a = expert_forward(u_a, weights_a, n_group)
        dy_b, q_b, x_mid = send_rows(dy_out, table, 1, own, capacity, 1, scaled=True, home=(x_in, rows_a, gate_a, out_a), gated=True)
        u_b, = send_rows(x_mid, table, 1, own, capacity, 2)
        out_b = expert_forward(u_b, weights_b, n_group)
        du_b, dgate_rows_b, grads_b = expert_backward(u_b, dy_b, q_b, weights_b, n_group)
        u_again, dx_mid = send_rows(x_in, table, 0, own, capacity, 3, home=(dy_out, rows_b, gate_b, du_b))
        dy_a, q_a, x_out = send_rows(dx_mid, table, 0, own, capacity, 4, scaled=True, home=(x_mid, rows_b, gate_b, out_b), gated=True)
        du_a, dgate_rows_a, grads_a = expert_backward(u_again, dy_a, q_a, weights_a, n_group)
        lines = jnp.concatenate([by_home(dgate_rows_a), by_home(dgate_rows_b)], axis=1)
        lines = jnp.pad(lines, ((0, 0), (0, 128 - 2 * block)))[:, None, :]
        dx_in, lines = return_home(dx_mid, rows_a, gate_a, du_a, lines, 5)
        dgate_a = look_up(lines[:, 0, :block], rows_a)
        dgate_b = look_up(lines[:, 0, block:2 * block], rows_b)
        return (x_out, dx_in) + tuple(grads_a) + tuple(grads_b) + (dgate_a, dgate_b)

    return jax.shard_map(device_program, mesh=mesh, in_specs=(tok_spec,) * 6 + (w_spec,) * 6, out_specs=(tok_spec,) * 10, check_vma=False)
```

```python
import functools

import jax
import jax.numpy as jnp
from jax import lax
from jax.experimental import pallas as pl
from jax.experimental.pallas import tpu as pltpu
from jax.sharding import PartitionSpec as P

CAP_FACTOR = 4
F32 = jnp.float32
BF16 = jnp.bfloat16


def table_kernel(experts, capacity, ids_a_ref, ids_b_ref, gate_a_ref, gate_b_ref, tile_ref, code_a_ref, code_b_ref, gates_a_ref, gates_b_ref):
    top_k, tok_dev = ids_a_ref.shape
    full = 128
    expert = lax.broadcasted_iota(jnp.int32, (full, experts), 1)
    row = lax.broadcasted_iota(jnp.int32, (full, full), 0)
    lane = lax.broadcasted_iota(jnp.int32, (full, full), 1)
    earlier = jnp.where(lane < row, 1.0, 0.0).astype(BF16)

    def turned(value, fill):
        value = jnp.concatenate([value.astype(F32), jnp.full((top_k, full - tok_dev), fill, F32)], axis=1)
        return value, jnp.concatenate([value, jnp.full((full - top_k, full), fill, F32)], axis=0).T

    for layer, (ids_ref, code_ref) in enumerate(((ids_a_ref, code_a_ref), (ids_b_ref, code_b_ref))):
        ids = turned(ids_ref[...], -1.0)[1].astype(jnp.int32)
        hits = [ids[:, j:j + 1] == expert for j in range(top_k)]
        chosen = jnp.zeros((full, experts), F32)
        for hit in hits:
            chosen = jnp.where(hit, 1.0, chosen)
        before = jnp.dot(earlier, chosen.astype(BF16), preferred_element_type=F32)
        code = jnp.full((full, full), -1.0, F32)
        for j, hit in enumerate(hits):
            slot = jnp.sum(jnp.where(hit, before, 0.0), axis=1, keepdims=True)
            code = jnp.where(lane == j, ids[:, j:j + 1].astype(F32) * capacity + slot, code)
        code = jnp.where(row < tok_dev, code, -1.0)
        code_ref[...] = code[:tok_dev, :top_k].astype(jnp.int32)
        tile_ref[layer] = code.T[:top_k]
    for layer, (gate_ref, out_ref) in enumerate(((gate_a_ref, gates_a_ref), (gate_b_ref, gates_b_ref))):
        tile, by_token = turned(gate_ref[...], 0.0)
        tile_ref[2 + layer] = tile
        out_ref[...] = by_token[:tok_dev, :top_k]


def make_tables(idx_a, idx_b, gate_a, gate_b, experts, capacity):
    tok_dev, top_k = idx_a.shape
    codes = jax.ShapeDtypeStruct((tok_dev, top_k), jnp.int32)
    gates = jax.ShapeDtypeStruct((tok_dev, top_k), F32)
    vmem = pl.BlockSpec(memory_space=pltpu.VMEM)
    return pl.pallas_call(
        functools.partial(table_kernel, experts, capacity),
        out_shape=(jax.ShapeDtypeStruct((4, top_k, 128), F32), codes, codes, gates, gates),
        in_specs=[vmem] * 4,
        out_specs=(vmem,) * 5,
        name="make_tables",
    )(idx_a.T, idx_b.T, gate_a.T, gate_b.T)


SIDE = 4


def my_place():
    me = lax.axis_index("ep")
    chip = lax.div(me, 2)
    at = (lax.rem(chip, SIDE), lax.rem(lax.div(chip, SIDE), SIDE), lax.div(chip, SIDE * SIDE))
    return me, lax.rem(me, 2), at


def device_at(at, core, delta, flip):
    c = [a if d == 0 else lax.rem(a + d + SIDE, SIDE) for a, d in zip(at, delta)]
    return ((c[2] * SIDE + c[1]) * SIDE + c[0]) * 2 + (1 - core if flip else core)


def return_offsets():
    direct, relayed = [], []
    devices = 2 * SIDE ** 3
    for step in range(1, devices):
        d = step * 37 % devices
        flip, delta = d % 2, (d // 2 % SIDE, d // (2 * SIDE) % SIDE, d // (2 * SIDE * SIDE))
        delta = tuple(v if v <= 2 else v - SIDE for v in delta)
        if 2 in delta:
            way = 1 if flip == 0 else -1
            delta = tuple(2 * way if v == 2 else v for v in delta)
            relayed.append((delta, flip, tuple(way if abs(v) == 2 else 0 for v in delta)))
        else:
            direct.append((delta, flip))
    return direct, relayed


RELAYS = len(return_offsets()[1])


def greet_all(me, core, at):
    barrier = pltpu.get_barrier_semaphore()
    devices = 2 * SIDE ** 3

    def hello(step, carry):
        pl.semaphore_signal(barrier, inc=1, device_id={"ep": lax.rem(me + step, devices)}, device_id_type=pl.DeviceIdType.MESH)
        return carry

    lax.fori_loop(1, devices, hello, 0)
    pl.semaphore_wait(barrier, devices - 1)


def return_steps(me, core, at, rows_ref, back, relay, sems, relay_sems):
    direct, relayed = return_offsets()
    devices = rows_ref.shape[0]

    def copy(src, dst, send_sem, recv_sem, to):
        return pltpu.make_async_remote_copy(src_ref=src, dst_ref=dst, send_sem=send_sem, recv_sem=recv_sem, device_id={"ep": to}, device_id_type=pl.DeviceIdType.MESH)

    def to_relay(k):
        delta, flip, via = relayed[k]
        return copy(rows_ref.at[device_at(at, core, delta, flip)], relay.at[k], sems.at[0], relay_sems.at[k], device_at(at, core, via, 0))

    def send_direct(k):
        to = device_at(at, core, *direct[k])
        copy(rows_ref.at[to], back.at[me], sems.at[1], sems.at[2], to).start()

    def forward(k):
        delta, flip, via = relayed[k]
        to_relay(k).wait_recv()
        origin = device_at(at, core, tuple(-v for v in via), 0)
        to = device_at(at, core, tuple(d - v for d, v in zip(delta, via)), flip)
        copy(relay.at[k], back.at[origin], sems.at[1], sems.at[2], to).start()

    def finish():
        back[me] = rows_ref[me]
        others = pl.ds(0, devices - 1)
        pltpu.make_async_copy(rows_ref.at[others], back.at[others], sems.at[2]).wait()
        pltpu.make_async_copy(rows_ref.at[others], back.at[others], sems.at[1]).wait()
        relays = pl.ds(0, len(relayed))
        pltpu.make_async_copy(rows_ref.at[relays], relay.at[relays], sems.at[0]).wait()

    def pieces(count, action, parts):
        cut = [count * i // parts for i in range(parts + 1)]
        return [lambda lo=lo, hi=hi: [action(k) for k in range(lo, hi)] for lo, hi in zip(cut, cut[1:])]

    vias = pieces(len(relayed), lambda k: to_relay(k).start(), 4)
    directs = pieces(len(direct), send_direct, 4)
    forwards = pieces(len(relayed), forward, 8)
    return vias, directs, forwards, finish


def home_blocks(back):
    group = 16
    count, width = back.shape[1], back.shape[2]
    return ((g * count, back[pl.ds(g, group)].reshape(group * count, width)) for g in range(0, back.shape[0], group))


def send_kernel(own, capacity, layer, first, scaled, returning, work, *refs):
    refs = list(refs)
    x_ref, tile_ref = refs.pop(0), refs.pop(0)
    if returning:
        base_ref, row_ref, gate_ref, rows_ref = (refs.pop(0) for _ in range(4))
    work_in = [refs.pop(0) for _ in range(work[1])] if work else []
    u_ref = refs.pop(0)
    if scaled:
        q_ref = refs.pop(0)
    if first:
        table_ref = refs.pop(0)
    if returning:
        home_ref = refs.pop(0)
    work_out = [refs.pop(0) for _ in range(work[2])] if work else []
    held, local_sem, send_sem, recv_sem = (refs.pop(0) for _ in range(4))
    tiles = refs.pop(0) if first else tile_ref
    if returning:
        back, relay, return_sems, relay_sems = refs
    me, core, at = my_place()
    plus = x_ref.shape[0] // 6
    third = x_ref.shape[0] // 3
    spans = {1: (0, plus), -1: (plus, third - plus)}

    def device(dim, step):
        return device_at(at, core, [step if d == dim else 0 for d in range(3)], 0)

    partner = device_at(at, core, (0, 0, 0), 1)

    def region(part, pos, span):
        idx = [pos[d] if d in pos else at[d] for d in range(3)]
        idx = [pl.ds(0, SIDE) if i is None else i for i in idx]
        where = (core, idx[2], idx[1], idx[0])
        return held.at[where + (pl.ds(part * third + span[0], span[1]),)], where + (pl.ds(part, 2 if part == 2 else 1),)

    copies = {}

    def start(key, refs, to, with_tile):
        for kind, ref in (("x", refs[0]), ("t", tiles.at[refs[1]])):
            if kind == "t" and not (first and with_tile):
                continue
            n = len(copies)
            copy = pltpu.make_async_remote_copy(src_ref=ref, dst_ref=ref, send_sem=send_sem.at[n], recv_sem=recv_sem.at[n], device_id={"ep": to}, device_id_type=pl.DeviceIdType.MESH)
            copy.start()
            copies[key + (kind,)] = copy

    def arrive(*key):
        for kind in ("x", "t"):
            if key + (kind,) in copies:
                copies[key + (kind,)].wait_recv()

    mine = pltpu.make_async_copy(x_ref, held.at[core, at[2], at[1], at[0]], local_sem)
    mine.start()
    if first:
        own_tile = pltpu.make_async_copy(tile_ref, tiles.at[core, at[2], at[1], at[0]], send_sem.at[0])
        own_tile.start()
        own_tile.wait()
    if returning:
        greet_all(me, core, at)
        mine.wait()
    else:
        barrier = pltpu.get_barrier_semaphore()
        for dim in range(3):
            for step in (1, -1, 2):
                pl.semaphore_signal(barrier, inc=1, device_id={"ep": device(dim, step)}, device_id_type=pl.DeviceIdType.MESH)
        pl.semaphore_signal(barrier, inc=1, device_id={"ep": partner}, device_id_type=pl.DeviceIdType.MESH)
        mine.wait()
        pl.semaphore_wait(barrier, 10)

    def dims(part):
        return part, (part + 1) % 3, (part + 2) % 3

    def shift(dim, step):
        return lax.rem(at[dim] + step + SIDE, SIDE)

    whole = (0, third)

    def row_of(part, b, c, span=whole):
        d1, d2, d3 = dims(part)
        return region(part, {d1: None, d2: shift(d2, b), d3: shift(d3, c)}, span)

    def across(part, b, c):
        start(("d2d", part, b, c), row_of(part, b, c), partner, True)

    def whole_row(part, b):
        d3 = dims(part)[2]
        for way in (1, -1):
            start(("m3", part, b, way), row_of(part, b, 0), device(d3, way), True)
        across(part, b, 0)

    def pass_on(part, b, way):
        d3 = dims(part)[2]
        arrive("m3", part, b, way)
        start(("f3", part, b, way), row_of(part, b, -way, spans[way]), device(d3, way), way == -1)
        across(part, b, -way)

    def last_row(part, b):
        for way in (1, -1):
            arrive("f3", part, b, way)
        across(part, b, 2)

    block = own * capacity
    slot = lax.broadcasted_iota(jnp.int32, (block, 128), 0) + me * block
    tok_dev = x_ref.shape[0]

    def pick(offsets):
        x, y, z = (lax.rem(at[d] + offsets[d] + SIDE, SIDE) for d in range(3))
        rows, scaled_rows = [], []
        for c in range(2):
            code = tiles[c, z, y, x, layer].astype(jnp.int32)
            gate = tiles[c, z, y, x, 2 + layer] if scaled else None
            hit = code[0:1, :] == slot
            weight = jnp.where(hit, gate[0:1, :], 0.0) if scaled else None
            for j in range(1, code.shape[0]):
                hit_j = code[j:j + 1, :] == slot
                hit = hit | hit_j
                if scaled:
                    weight = jnp.where(hit_j, gate[j:j + 1, :], weight)
            onehot = jnp.where(hit, 1.0, 0.0)[:, :tok_dev].astype(BF16)
            rows.append(jnp.dot(onehot, held[c, z, y, x], preferred_element_type=F32))
            if scaled:
                scaled_rows.append(jnp.sum(weight, axis=1, keepdims=True) * rows[-1])
        place = ((z * SIDE + y) * SIDE + x) * 2 * capacity
        for out_ref, parts in ((u_ref, rows),) + (((q_ref, scaled_rows),) if scaled else ()):
            for e in range(own):
                both = jnp.concatenate([r[e * capacity:(e + 1) * capacity] for r in parts], axis=0)
                out_ref[e, pl.ds(pl.multiple_of(place, 2 * capacity), 2 * capacity), :] = both.astype(BF16)

    def near_rows(step, carry):
        for k in (-1, 0, 1):
            pick((k, lax.rem(step, 3) - 1, lax.div(step, 3) - 1))
        return carry

    def far_rows(step, carry):
        b, c = lax.rem(step, 3) - 1, lax.div(step, 3) - 1
        for offsets in ((2, b, c), (b, 2, c), (b, c, 2)):
            pick(offsets)
        return carry

    def farthest_rows(step, carry):
        for offsets in ((2, 2, step - 1), (2, step - 1, 2), (step - 1, 2, 2)):
            pick(offsets)
        return carry

    def arrive_across(wanted):
        for part in range(3):
            for b in (0, -1, 1, 2):
                for c in (0, -1, 1, 2):
                    if (b == 2) + (c == 2) == wanted:
                        arrive("d2d", part, b, c)

    def first_sends():
        for part in range(3):
            for way in (2, 1, -1):
                start(("m1", part, way), region(part, {}, whole), device(dims(part)[0], way), True)

    def second_sends():
        for part in range(3):
            for way in (1, -1, 2):
                arrive("m1", part, way)
            for way in (2, 1, -1):
                start(("m2", part, way), row_of(part, 0, 0), device(dims(part)[1], way), True)

    def own_rows():
        for part in range(3):
            whole_row(part, 0)

    def near_sends():
        for part in range(3):
            for way in (1, -1):
                arrive("m2", part, way)
                whole_row(part, -way)

    def pass_rows(b):
        for part in range(3):
            for way in (1, -1):
                pass_on(part, b, way)

    def opposite_rows():
        for part in range(3):
            arrive("m2", part, 2)
            whole_row(part, 2)

    def last_rows(b):
        for part in range(3):
            last_row(part, b)

    def pick_near():
        arrive_across(0)
        lax.fori_loop(0, 9, near_rows, 0)

    def pick_far():
        arrive_across(1)
        lax.fori_loop(0, 9, far_rows, 0)

    gathering = [first_sends, second_sends, own_rows, near_sends, lambda: pass_rows(0), opposite_rows, lambda: pass_rows(-1), lambda: pass_rows(1), pick_near, lambda: last_rows(0), lambda: pass_rows(2), lambda: last_rows(-1), lambda: last_rows(1), pick_far]
    between = {}
    if returning:
        vias, directs, forwards, finish = return_steps(me, core, at, rows_ref, back, relay, return_sems, relay_sems)
        between = {0: vias[:1], 1: vias[1:2], 2: vias[2:3], 3: vias[3:] + directs[:1], 4: forwards[:1] + directs[1:2], 5: forwards[1:2] + directs[2:3], 6: forwards[2:4] + directs[3:], 7: forwards[4:5], 8: forwards[5:7], 9: forwards[7:]}
    jobs = work[0](work_in, work_out) if work else []
    for n, step in enumerate(gathering):
        step()
        for extra in between.get(n, []):
            extra()
        if 3 <= n and jobs:
            jobs.pop(0)()
    for job in jobs:
        job()
    last_rows(2)
    arrive_across(2)
    lax.fori_loop(0, 3, farthest_rows, 0)
    pick((2, 2, 2))
    if returning:
        finish()
        total = pair_sum(returning == "gated", row_ref, gate_ref, home_blocks(back))
        home_ref[...] = (base_ref[...].astype(F32) + total).astype(home_ref.dtype)
    if first:
        table_ref[...] = tiles[...]
    for copy in copies.values():
        copy.wait_send()


def return_scratch(sent):
    return [pltpu.VMEM(sent.shape, sent.dtype), pltpu.VMEM((RELAYS,) + sent.shape[1:], sent.dtype), pltpu.SemaphoreType.DMA((5,)), pltpu.SemaphoreType.DMA((RELAYS,))]


def send_rows(x, table, layer, own, capacity, call_id, first=False, scaled=False, home=None, gated=False, work=None):
    tok_dev, width = x.shape
    devices = 2 * SIDE ** 3
    count = 228 if first else 114
    u_shape = jax.ShapeDtypeStruct((own, devices * capacity, width), x.dtype)
    table_shape = jax.ShapeDtypeStruct((2, SIDE, SIDE, SIDE, 4, 8, 128), F32)
    outs = (u_shape,) + (u_shape,) * scaled + (table_shape,) * first
    if home:
        outs += (jax.ShapeDtypeStruct(home[0].shape, home[0].dtype),)
    jobs, job_in, job_out = work or (None, (), ())
    outs += tuple(job_out)
    vmem = pl.BlockSpec(memory_space=pltpu.VMEM)
    hbm = pl.BlockSpec(memory_space=pl.ANY)
    returning = None if home is None else "gated" if gated else "plain"
    return pl.pallas_call(
        functools.partial(send_kernel, own, capacity, layer, first, scaled, returning, work and (jobs, len(job_in), len(job_out))),
        out_shape=outs,
        in_specs=[hbm, hbm if first else vmem] + [vmem] * ((4 if home else 0) + len(job_in)),
        out_specs=(vmem,) * len(outs),
        scratch_shapes=[
            pltpu.VMEM((2, SIDE, SIDE, SIDE, tok_dev, width), x.dtype),
            pltpu.SemaphoreType.DMA,
            pltpu.SemaphoreType.DMA((count,)),
            pltpu.SemaphoreType.DMA((count,)),
        ] + ([pltpu.VMEM(table_shape.shape, F32)] if first else []) + (return_scratch(home[3]) if home else []),
        compiler_params=pltpu.CompilerParams(collective_id=call_id, has_side_effects=True, vmem_limit_bytes=54 * 1024 * 1024),
        cost_estimate=pl.CostEstimate(flops=3 * 10**10, bytes_accessed=devices * tok_dev * width * 2, transcendentals=0),
        name=f"send_rows_{call_id}",
    )(x, table, *(home or ()), *job_in)


def pair_sum(gated, row_ref, gate_ref, back):
    codes, gates = row_ref[...], gate_ref[...]
    tok_dev = codes.shape[0]
    total = 0.0
    for base, rows in back:
        lane = lax.broadcasted_iota(jnp.int32, (tok_dev, rows.shape[0]), 1) + base
        weight = jnp.zeros(lane.shape, F32)
        for j in range(codes.shape[1]):
            weight = jnp.where(codes[:, j:j + 1] == lane, gates[:, j:j + 1] if gated else 1.0, weight)
        hi = weight.astype(BF16)
        terms = [hi]
        if gated:
            rest = weight - hi.astype(F32)
            mid = rest.astype(BF16)
            terms += [mid, (rest - mid.astype(F32)).astype(BF16)]
        part = jnp.dot(jnp.concatenate(terms, axis=0), rows, preferred_element_type=F32)
        for k in reversed(range(len(terms))):
            total = total + part[k * tok_dev:(k + 1) * tok_dev]
    return total


def look_up(lines, codes, per_device, first_lane):
    device = jnp.floor((codes.astype(F32) + 0.5) * (1.0 / per_device))
    place = codes.astype(F32) - device * per_device + first_lane
    hi = lines.astype(BF16)
    rest = lines - hi.astype(F32)
    mid = rest.astype(BF16)
    terms = jnp.concatenate([hi, mid, (rest - mid.astype(F32)).astype(BF16)], axis=1)
    tok_dev, top_k = codes.shape
    lane = lax.broadcasted_iota(jnp.int32, (tok_dev, 128), 1).astype(F32)
    out = jnp.zeros((tok_dev, 128), F32)
    for j in range(top_k):
        onehot = jnp.where(device[:, j:j + 1] == lane, 1.0, 0.0).astype(BF16)
        picked = jnp.dot(onehot, terms, preferred_element_type=F32)
        picked = picked[:, :128] + (picked[:, 128:256] + picked[:, 256:])
        value = jnp.sum(jnp.where(place[:, j:j + 1] == lane, picked, 0.0), axis=1, keepdims=True)
        out = jnp.where(lane == j, value, out)
    return out[:, :top_k]


def return_kernel(per_device, x_ref, row_ref, gate_ref, rows_ref, line_a_ref, line_b_ref, row_b_ref, u_ref, q_ref, hidden_ref, da_ref, db_ref, out_ref, dgate_a_ref, dgate_b_ref, dw1_ref, dw3_ref, dw2_ref, back, relay, sems, relay_sems, line_ref, line_back):
    me, core, at = my_place()
    devices = rows_ref.shape[0]
    line_ref[...] = line_a_ref[...] + line_b_ref[...]
    greet_all(me, core, at)
    vias, directs, forwards, finish = return_steps(me, core, at, rows_ref, back, relay, sems, relay_sems)

    def send_line(step, carry):
        to = lax.rem(me + step, devices)
        pltpu.make_async_remote_copy(src_ref=line_ref.at[to], dst_ref=line_back.at[me], send_sem=sems.at[3], recv_sem=sems.at[4], device_id={"ep": to}, device_id_type=pl.DeviceIdType.MESH).start()
        return carry

    jobs = grad_jobs([u_ref, q_ref, hidden_ref, da_ref, db_ref], [dw1_ref, dw3_ref, dw2_ref])
    for step in vias + directs[:2] + forwards[:2] + directs[2:] + forwards[2:4]:
        step()
    lax.fori_loop(1, devices, send_line, 0)
    for n, step in enumerate(forwards[4:]):
        step()
        if jobs:
            jobs.pop(0)()
    line_back[me] = line_ref[me]
    others = pl.ds(0, devices - 1)
    for k in (3, 4):
        pltpu.make_async_copy(line_ref.at[others], line_back.at[others], sems.at[k]).wait()
    lines = line_back[...].reshape(devices, 128)
    dgate_a_ref[...] = look_up(lines, row_ref[...], per_device, 0)
    dgate_b_ref[...] = look_up(lines, row_b_ref[...], per_device, per_device)
    finish()
    out_ref[...] = (x_ref[...].astype(F32) + pair_sum(False, row_ref, gate_ref, home_blocks(back))).astype(out_ref.dtype)


def return_home(x, rows, gates, sent, line_a, line_b, rows_b, saved, grad_shapes, per_device, call_id):
    vmem = pl.BlockSpec(memory_space=pltpu.VMEM)
    dgate = jax.ShapeDtypeStruct(rows.shape, F32)
    outs = (jax.ShapeDtypeStruct(x.shape, x.dtype), dgate, dgate) + tuple(grad_shapes)
    return pl.pallas_call(
        functools.partial(return_kernel, per_device),
        out_shape=outs,
        in_specs=[vmem] * (7 + len(saved)),
        out_specs=(vmem,) * len(outs),
        scratch_shapes=return_scratch(sent) + [pltpu.VMEM(line_a.shape, F32)] * 2,
        compiler_params=pltpu.CompilerParams(collective_id=call_id, has_side_effects=True, vmem_limit_bytes=40 * 1024 * 1024),
        cost_estimate=pl.CostEstimate(flops=3 * 10**10, bytes_accessed=sent.size * 4, transcendentals=0),
        name="return_home",
    )(x, rows, gates, sent, line_a, line_b, rows_b, *saved)


def forward_rows(u, w_both, w_down):
    ff = w_down.shape[0]
    pre = jnp.dot(u, w_both, preferred_element_type=F32)
    pre_gate, pre_up = pre[:, :ff], pre[:, ff:]
    sig = 1.0 / (1.0 + jnp.exp(-pre_gate))
    silu = pre_gate * sig
    hidden = (silu * pre_up).astype(BF16)
    out = jnp.dot(hidden, w_down, preferred_element_type=F32)
    return pre_gate, pre_up, sig, silu, hidden, out


def store_home(out_ref, step, rows):
    count, width = rows.shape
    slots = out_ref.shape[1]
    sources = count // slots
    out_ref[pl.ds(step * sources, sources)] = rows.reshape(sources, slots, width).astype(out_ref.dtype)


def forward_kernel(chunk, u_ref, w1_ref, w3_ref, w2_ref, out_ref):
    w_both = jnp.concatenate([w1_ref[0], w3_ref[0]], axis=1)

    def body(step, carry):
        rows = pl.ds(pl.multiple_of(step * chunk, chunk), chunk)
        out = forward_rows(u_ref[0, rows, :], w_both, w2_ref[0])[-1]
        store_home(out_ref, step, out)
        return carry

    lax.fori_loop(0, u_ref.shape[1] // chunk, body, 0)


def forward_jobs(ins, outs):
    u_ref, w1_ref, w3_ref, w2_ref = ins
    out_ref, = outs
    chunk = 256
    own, count, width = u_ref.shape
    sources = out_ref.shape[0] * chunk // count
    slots = out_ref.shape[1] // own

    def job(e):
        w_both = jnp.concatenate([w1_ref[e], w3_ref[e]], axis=1)

        def body(step, carry):
            rows = pl.ds(pl.multiple_of(step * chunk, chunk), chunk)
            out = forward_rows(u_ref[e, rows, :], w_both, w2_ref[e])[-1]
            out_ref[pl.ds(step * sources, sources), e * slots:(e + 1) * slots, :] = out.reshape(sources, slots, width).astype(BF16)
            return carry

        lax.fori_loop(0, count // chunk, body, 0)

    return [functools.partial(job, e) for e in range(own)]


def grad_jobs(ins, outs):
    u_ref, q_ref, hidden_ref, da_ref, db_ref = ins
    dw1_ref, dw3_ref, dw2_ref = outs
    ff = da_ref.shape[2]
    rows = (((0,), (0,)), ((), ()))

    def job(e):
        both = jnp.concatenate([da_ref[e], db_ref[e]], axis=1)
        dw = lax.dot_general(u_ref[e], both, rows, preferred_element_type=F32)
        dw1_ref[e] = dw[:, :ff]
        dw3_ref[e] = dw[:, ff:]
        dw2_ref[e] = lax.dot_general(hidden_ref[e], q_ref[e], rows, preferred_element_type=F32)

    return [functools.partial(job, e) for e in range(u_ref.shape[0])]


def backward_kernel(first_lane, chunk, u_ref, dy_ref, q_ref, w1_ref, w3_ref, w2_ref, du_ref, dgate_ref, hidden_ref, da_ref, db_ref):
    ff = w2_ref.shape[1]
    w_both = jnp.concatenate([w1_ref[0], w3_ref[0]], axis=1)
    last = (((1,), (1,)), ((), ()))

    def body(step, carry):
        rows = pl.ds(pl.multiple_of(step * chunk, chunk), chunk)
        pre_gate, pre_up, sig, silu, hidden, out = forward_rows(u_ref[0, rows, :], w_both, w2_ref[0])
        dgate = jnp.sum(dy_ref[0, rows, :].astype(F32) * out.astype(BF16).astype(F32), axis=1, keepdims=True)
        slots = du_ref.shape[1]
        lane = lax.broadcasted_iota(jnp.int32, (chunk, 128), 1)
        wanted = lax.rem(lax.broadcasted_iota(jnp.int32, (chunk, 128), 0), slots) + first_lane + pl.program_id(0) * slots
        line = jnp.where(lane == wanted, dgate, 0.0).reshape(chunk // slots, slots, 128)
        line = jnp.sum(line, axis=1, keepdims=True)
        at = pl.ds(step * (chunk // slots), chunk // slots)
        dgate_ref[at] = jnp.where(pl.program_id(0) == 0, 0.0, dgate_ref[at]) + line
        d_hidden = lax.dot_general(q_ref[0, rows, :], w2_ref[0], last, preferred_element_type=F32)
        da = (d_hidden * pre_up * sig * (1.0 + pre_gate * (1.0 - sig))).astype(BF16)
        db = (d_hidden * silu).astype(BF16)
        hidden_ref[0, rows, :] = hidden
        da_ref[0, rows, :] = da
        db_ref[0, rows, :] = db
        both = jnp.concatenate([da, db], axis=1)
        store_home(du_ref, step, lax.dot_general(both, w_both, last, preferred_element_type=F32))
        return carry

    lax.fori_loop(0, u_ref.shape[1] // chunk, body, 0)


def expert_call(kernel, inputs, outs, weights, n_group, name):
    own, count, width = inputs[0].shape
    ff = weights[2].shape[1]
    slots = count // n_group

    def each(shape):
        return pl.BlockSpec((1,) + shape, lambda e: (e, 0, 0))

    home = (jax.ShapeDtypeStruct((n_group, own * slots, width), BF16), pl.BlockSpec((n_group, slots, width), lambda e: (0, e, 0)))
    kinds = {
        "home": home,
        "gate": (jax.ShapeDtypeStruct((n_group, 1, 128), F32), pl.BlockSpec((n_group, 1, 128), lambda e: (0, 0, 0))),
        "ff": (jax.ShapeDtypeStruct((own, count, ff), BF16), each((count, ff))),
    }
    steps = 3 if len(outs) == 1 else 8
    return pl.pallas_call(
        functools.partial(kernel, 256),
        out_shape=tuple(kinds[k][0] for k in outs),
        grid=(own,),
        in_specs=[each((count, width))] * len(inputs) + [each((width, ff)), each((width, ff)), each((ff, width))],
        out_specs=tuple(kinds[k][1] for k in outs),
        compiler_params=pltpu.CompilerParams(vmem_limit_bytes=32 * 1024 * 1024),
        cost_estimate=pl.CostEstimate(flops=2 * steps * own * count * width * ff, bytes_accessed=own * count * width * 2 * (len(inputs) + 1), transcendentals=own * count * ff),
        name=name,
    )(*inputs, *weights)


def expert_forward(u_rows, weights, n_group):
    return expert_call(forward_kernel, (u_rows,), ("home",), weights, n_group, "expert_forward")[0]


def expert_backward(u_rows, dy_rows, q_rows, weights, n_group, first_lane):
    outs = ("home", "gate", "ff", "ff", "ff")
    kernel = functools.partial(backward_kernel, first_lane)
    du, lines, *saved = expert_call(kernel, (u_rows, dy_rows, q_rows), outs, weights, n_group, "expert_backward")
    return du, lines, (u_rows, q_rows, *saved)


def solution(mesh):
    n_group = mesh.shape["ep"]
    tok_spec = P(("dp", "ep"))
    w_spec = P("ep")

    def device_program(x_in, idx_a, idx_b, gate_a, gate_b, dy_out, w1_a, w3_a, w2_a, w1_b, w3_b, w2_b):
        tok_dev, top_k = idx_a.shape
        width = x_in.shape[1]
        own = w1_a.shape[0]
        capacity = CAP_FACTOR * tok_dev * top_k // (own * n_group)
        total = own * n_group * capacity
        block = own * capacity

        tile, rows_a, rows_b, gates_a, gates_b = make_tables(idx_a, idx_b, gate_a, gate_b, own * n_group, capacity)
        u_a, table = send_rows(x_in, tile, 0, own, capacity, 0, first=True)

        weights_a, weights_b = (w1_a, w3_a, w2_a), (w1_b, w3_b, w2_b)
        out_a = expert_forward(u_a, weights_a, n_group)
        dy_b, q_b, x_mid = send_rows(dy_out, table, 1, own, capacity, 1, scaled=True, home=(x_in, rows_a, gates_a, out_a), gated=True)
        u_b, = send_rows(x_mid, table, 1, own, capacity, 2)
        du_b, line_b, saved_b = expert_backward(u_b, dy_b, q_b, weights_b, n_group, block)
        forward_b = (forward_jobs, (u_b,) + weights_b, (jax.ShapeDtypeStruct((n_group, block, width), BF16),))
        u_again, dx_mid, out_b = send_rows(x_in, table, 0, own, capacity, 3, home=(dy_out, rows_b, gates_b, du_b), work=forward_b)
        grad_shapes = tuple(jax.ShapeDtypeStruct(w.shape, F32) for w in weights_b)
        dy_a, q_a, x_out, *grads_b = send_rows(dx_mid, table, 0, own, capacity, 4, scaled=True, home=(x_mid, rows_b, gates_b, out_b), gated=True, work=(grad_jobs, saved_b, grad_shapes))
        du_a, line_a, saved_a = expert_backward(u_again, dy_a, q_a, weights_a, n_group, 0)
        dx_in, dgate_a, dgate_b, *grads_a = return_home(dx_mid, rows_a, gates_a, du_a, line_a, line_b, rows_b, saved_a, grad_shapes, block, 5)
        return (x_out, dx_in) + tuple(grads_a) + tuple(grads_b) + (dgate_a, dgate_b)

    return jax.shard_map(device_program, mesh=mesh, in_specs=(tok_spec,) * 6 + (w_spec,) * 6, out_specs=(tok_spec,) * 10, check_vma=False)
```

```python
import functools

import jax
import jax.numpy as jnp
from jax import lax
from jax.experimental import pallas as pl
from jax.experimental.pallas import tpu as pltpu
from jax.sharding import PartitionSpec as P

CAP_FACTOR = 4
F32 = jnp.float32
BF16 = jnp.bfloat16


def table_kernel(experts, capacity, ids_a_ref, ids_b_ref, gate_a_ref, gate_b_ref, tile_ref, code_a_ref, code_b_ref, gates_a_ref, gates_b_ref):
    top_k, tok_dev = ids_a_ref.shape
    full = 128
    expert = lax.broadcasted_iota(jnp.int32, (full, experts), 1)
    row = lax.broadcasted_iota(jnp.int32, (full, full), 0)
    lane = lax.broadcasted_iota(jnp.int32, (full, full), 1)
    earlier = jnp.where(lane < row, 1.0, 0.0).astype(BF16)

    def turned(value, fill):
        value = jnp.concatenate([value.astype(F32), jnp.full((top_k, full - tok_dev), fill, F32)], axis=1)
        return value, jnp.concatenate([value, jnp.full((full - top_k, full), fill, F32)], axis=0).T

    for layer, (ids_ref, code_ref) in enumerate(((ids_a_ref, code_a_ref), (ids_b_ref, code_b_ref))):
        ids = turned(ids_ref[...], -1.0)[1].astype(jnp.int32)
        hits = [ids[:, j:j + 1] == expert for j in range(top_k)]
        chosen = jnp.zeros((full, experts), F32)
        for hit in hits:
            chosen = jnp.where(hit, 1.0, chosen)
        before = jnp.dot(earlier, chosen.astype(BF16), preferred_element_type=F32)
        code = jnp.full((full, full), -1.0, F32)
        for j, hit in enumerate(hits):
            slot = jnp.sum(jnp.where(hit, before, 0.0), axis=1, keepdims=True)
            code = jnp.where(lane == j, ids[:, j:j + 1].astype(F32) * capacity + slot, code)
        code = jnp.where(row < tok_dev, code, -1.0)
        code_ref[...] = code[:tok_dev, :top_k].astype(jnp.int32)
        tile_ref[layer] = code.T[:top_k]
    for layer, (gate_ref, out_ref) in enumerate(((gate_a_ref, gates_a_ref), (gate_b_ref, gates_b_ref))):
        tile, by_token = turned(gate_ref[...], 0.0)
        tile_ref[2 + layer] = tile
        out_ref[...] = by_token[:tok_dev, :top_k]


def make_tables(idx_a, idx_b, gate_a, gate_b, experts, capacity):
    tok_dev, top_k = idx_a.shape
    codes = jax.ShapeDtypeStruct((tok_dev, top_k), jnp.int32)
    gates = jax.ShapeDtypeStruct((tok_dev, top_k), F32)
    vmem = pl.BlockSpec(memory_space=pltpu.VMEM)
    return pl.pallas_call(
        functools.partial(table_kernel, experts, capacity),
        out_shape=(jax.ShapeDtypeStruct((4, top_k, 128), F32), codes, codes, gates, gates),
        in_specs=[vmem] * 4,
        out_specs=(vmem,) * 5,
        name="make_tables",
    )(idx_a.T, idx_b.T, gate_a.T, gate_b.T)


SIDE = 4


def my_place():
    me = lax.axis_index("ep")
    chip = lax.div(me, 2)
    at = (lax.rem(chip, SIDE), lax.rem(lax.div(chip, SIDE), SIDE), lax.div(chip, SIDE * SIDE))
    return me, lax.rem(me, 2), at


def device_at(at, core, delta, flip):
    c = [a if d == 0 else lax.rem(a + d + SIDE, SIDE) for a, d in zip(at, delta)]
    return ((c[2] * SIDE + c[1]) * SIDE + c[0]) * 2 + (1 - core if flip else core)


def return_offsets():
    direct, relayed = [], []
    devices = 2 * SIDE ** 3
    for step in range(1, devices):
        d = step * 37 % devices
        flip, delta = d % 2, (d // 2 % SIDE, d // (2 * SIDE) % SIDE, d // (2 * SIDE * SIDE))
        delta = tuple(v if v <= 2 else v - SIDE for v in delta)
        if 2 in delta:
            way = 1 if flip == 0 else -1
            delta = tuple(2 * way if v == 2 else v for v in delta)
            relayed.append((delta, flip, tuple(way if abs(v) == 2 else 0 for v in delta)))
        else:
            direct.append((delta, flip))
    return direct, relayed


RELAYS = len(return_offsets()[1])


def greet_all(me, core, at):
    barrier = pltpu.get_barrier_semaphore()
    devices = 2 * SIDE ** 3

    def hello(step, carry):
        pl.semaphore_signal(barrier, inc=1, device_id={"ep": lax.rem(me + step, devices)}, device_id_type=pl.DeviceIdType.MESH)
        return carry

    lax.fori_loop(1, devices, hello, 0)
    pl.semaphore_wait(barrier, devices - 1)


def return_steps(me, core, at, rows_ref, back, relay, sems, relay_sems):
    direct, relayed = return_offsets()
    devices = rows_ref.shape[0]

    def copy(src, dst, send_sem, recv_sem, to):
        return pltpu.make_async_remote_copy(src_ref=src, dst_ref=dst, send_sem=send_sem, recv_sem=recv_sem, device_id={"ep": to}, device_id_type=pl.DeviceIdType.MESH)

    def to_relay(k):
        delta, flip, via = relayed[k]
        return copy(rows_ref.at[device_at(at, core, delta, flip)], relay.at[k], sems.at[0], relay_sems.at[k], device_at(at, core, via, 0))

    def send_direct(k):
        to = device_at(at, core, *direct[k])
        copy(rows_ref.at[to], back.at[me], sems.at[1], sems.at[2], to).start()

    def forward(k):
        delta, flip, via = relayed[k]
        to_relay(k).wait_recv()
        origin = device_at(at, core, tuple(-v for v in via), 0)
        to = device_at(at, core, tuple(d - v for d, v in zip(delta, via)), flip)
        copy(relay.at[k], back.at[origin], sems.at[1], sems.at[2], to).start()

    def finish():
        back[me] = rows_ref[me]
        others = pl.ds(0, devices - 1)
        pltpu.make_async_copy(rows_ref.at[others], back.at[others], sems.at[2]).wait()
        pltpu.make_async_copy(rows_ref.at[others], back.at[others], sems.at[1]).wait()
        relays = pl.ds(0, len(relayed))
        pltpu.make_async_copy(rows_ref.at[relays], relay.at[relays], sems.at[0]).wait()

    def pieces(count, action, parts):
        cut = [count * i // parts for i in range(parts + 1)]
        return [lambda lo=lo, hi=hi: [action(k) for k in range(lo, hi)] for lo, hi in zip(cut, cut[1:])]

    vias = pieces(len(relayed), lambda k: to_relay(k).start(), 4)
    directs = pieces(len(direct), send_direct, 4)
    forwards = pieces(len(relayed), forward, 8)
    return vias, directs, forwards, finish


def home_blocks(back):
    group = 16
    count, width = back.shape[1], back.shape[2]
    return ((g * count, back[pl.ds(g, group)].reshape(group * count, width)) for g in range(0, back.shape[0], group))


def send_kernel(own, capacity, layer, first, scaled, returning, work, *refs):
    refs = list(refs)
    x_ref, tile_ref = refs.pop(0), refs.pop(0)
    if returning:
        base_ref, row_ref, gate_ref, rows_ref = (refs.pop(0) for _ in range(4))
    work_in = [refs.pop(0) for _ in range(work[1])] if work else []
    u_ref = refs.pop(0)
    if scaled:
        q_ref = refs.pop(0)
    if first:
        table_ref = refs.pop(0)
    if returning:
        home_ref = refs.pop(0)
    work_out = [refs.pop(0) for _ in range(work[2])] if work else []
    held, local_sem, send_sem, recv_sem = (refs.pop(0) for _ in range(4))
    tiles = refs.pop(0) if first else tile_ref
    if returning:
        back, relay, return_sems, relay_sems = refs
    me, core, at = my_place()
    plus = x_ref.shape[0] // 6
    third = x_ref.shape[0] // 3
    spans = {1: (0, plus), -1: (plus, third - plus)}

    def device(dim, step):
        return device_at(at, core, [step if d == dim else 0 for d in range(3)], 0)

    partner = device_at(at, core, (0, 0, 0), 1)

    def region(part, pos, span):
        idx = [pos[d] if d in pos else at[d] for d in range(3)]
        idx = [pl.ds(0, SIDE) if i is None else i for i in idx]
        where = (core, idx[2], idx[1], idx[0])
        return held.at[where + (pl.ds(part * third + span[0], span[1]),)], where + (pl.ds(part, 2 if part == 2 else 1),)

    copies = {}

    def start(key, refs, to, with_tile):
        for kind, ref in (("x", refs[0]), ("t", tiles.at[refs[1]])):
            if kind == "t" and not (first and with_tile):
                continue
            n = len(copies)
            copy = pltpu.make_async_remote_copy(src_ref=ref, dst_ref=ref, send_sem=send_sem.at[n], recv_sem=recv_sem.at[n], device_id={"ep": to}, device_id_type=pl.DeviceIdType.MESH)
            copy.start()
            copies[key + (kind,)] = copy

    def arrive(*key):
        for kind in ("x", "t"):
            if key + (kind,) in copies:
                copies[key + (kind,)].wait_recv()

    mine = pltpu.make_async_copy(x_ref, held.at[core, at[2], at[1], at[0]], local_sem)
    mine.start()
    if first:
        own_tile = pltpu.make_async_copy(tile_ref, tiles.at[core, at[2], at[1], at[0]], send_sem.at[0])
        own_tile.start()
        own_tile.wait()
    if returning:
        greet_all(me, core, at)
        mine.wait()
    else:
        barrier = pltpu.get_barrier_semaphore()
        for dim in range(3):
            for step in (1, -1, 2):
                pl.semaphore_signal(barrier, inc=1, device_id={"ep": device(dim, step)}, device_id_type=pl.DeviceIdType.MESH)
        pl.semaphore_signal(barrier, inc=1, device_id={"ep": partner}, device_id_type=pl.DeviceIdType.MESH)
        mine.wait()
        pl.semaphore_wait(barrier, 10)

    def dims(part):
        return part, (part + 1) % 3, (part + 2) % 3

    def shift(dim, step):
        return lax.rem(at[dim] + step + SIDE, SIDE)

    whole = (0, third)

    def row_of(part, b, c, span=whole):
        d1, d2, d3 = dims(part)
        return region(part, {d1: None, d2: shift(d2, b), d3: shift(d3, c)}, span)

    def across(part, b, c):
        start(("d2d", part, b, c), row_of(part, b, c), partner, True)

    def whole_row(part, b):
        d3 = dims(part)[2]
        for way in (1, -1):
            start(("m3", part, b, way), row_of(part, b, 0), device(d3, way), True)
        across(part, b, 0)

    def pass_on(part, b, way):
        d3 = dims(part)[2]
        arrive("m3", part, b, way)
        start(("f3", part, b, way), row_of(part, b, -way, spans[way]), device(d3, way), way == -1)
        across(part, b, -way)

    def last_row(part, b):
        for way in (1, -1):
            arrive("f3", part, b, way)
        across(part, b, 2)

    block = own * capacity
    slot = lax.broadcasted_iota(jnp.int32, (block, 128), 0) + me * block
    tok_dev = x_ref.shape[0]

    def pick(offsets):
        x, y, z = (lax.rem(at[d] + offsets[d] + SIDE, SIDE) for d in range(3))
        rows, scaled_rows = [], []
        for c in range(2):
            code = tiles[c, z, y, x, layer].astype(jnp.int32)
            gate = tiles[c, z, y, x, 2 + layer] if scaled else None
            hit = code[0:1, :] == slot
            weight = jnp.where(hit, gate[0:1, :], 0.0) if scaled else None
            for j in range(1, code.shape[0]):
                hit_j = code[j:j + 1, :] == slot
                hit = hit | hit_j
                if scaled:
                    weight = jnp.where(hit_j, gate[j:j + 1, :], weight)
            onehot = jnp.where(hit, 1.0, 0.0)[:, :tok_dev].astype(BF16)
            rows.append(jnp.dot(onehot, held[c, z, y, x], preferred_element_type=F32))
            if scaled:
                scaled_rows.append(jnp.sum(weight, axis=1, keepdims=True) * rows[-1])
        place = ((z * SIDE + y) * SIDE + x) * 2 * capacity
        for out_ref, parts in ((u_ref, rows),) + (((q_ref, scaled_rows),) if scaled else ()):
            for e in range(own):
                both = jnp.concatenate([r[e * capacity:(e + 1) * capacity] for r in parts], axis=0)
                out_ref[e, pl.ds(pl.multiple_of(place, 2 * capacity), 2 * capacity), :] = both.astype(BF16)

    def near_rows(step, carry):
        for k in (-1, 0, 1):
            pick((k, lax.rem(step, 3) - 1, lax.div(step, 3) - 1))
        return carry

    def far_rows(step, carry):
        b, c = lax.rem(step, 3) - 1, lax.div(step, 3) - 1
        for offsets in ((2, b, c), (b, 2, c), (b, c, 2)):
            pick(offsets)
        return carry

    def farthest_rows(step, carry):
        for offsets in ((2, 2, step - 1), (2, step - 1, 2), (step - 1, 2, 2)):
            pick(offsets)
        return carry

    def arrive_across(wanted):
        for part in range(3):
            for b in (0, -1, 1, 2):
                for c in (0, -1, 1, 2):
                    if (b == 2) + (c == 2) == wanted:
                        arrive("d2d", part, b, c)

    def first_sends():
        for part in range(3):
            for way in (2, 1, -1):
                start(("m1", part, way), region(part, {}, whole), device(dims(part)[0], way), True)

    def second_sends():
        for part in range(3):
            for way in (1, -1, 2):
                arrive("m1", part, way)
            for way in (2, 1, -1):
                start(("m2", part, way), row_of(part, 0, 0), device(dims(part)[1], way), True)

    def own_rows():
        for part in range(3):
            whole_row(part, 0)

    def near_sends():
        for part in range(3):
            for way in (1, -1):
                arrive("m2", part, way)
                whole_row(part, -way)

    def pass_rows(b):
        for part in range(3):
            for way in (1, -1):
                pass_on(part, b, way)

    def opposite_rows():
        for part in range(3):
            arrive("m2", part, 2)
            whole_row(part, 2)

    def last_rows(b):
        for part in range(3):
            last_row(part, b)

    def pick_near():
        arrive_across(0)
        lax.fori_loop(0, 9, near_rows, 0)

    def pick_far():
        arrive_across(1)
        lax.fori_loop(0, 9, far_rows, 0)

    gathering = [first_sends, second_sends, own_rows, near_sends, lambda: pass_rows(0), opposite_rows, lambda: pass_rows(-1), lambda: pass_rows(1), pick_near, lambda: last_rows(0), lambda: pass_rows(2), lambda: last_rows(-1), lambda: last_rows(1), pick_far]
    between = {}
    if returning:
        vias, directs, forwards, finish = return_steps(me, core, at, rows_ref, back, relay, return_sems, relay_sems)
        between = {0: vias[:1], 1: vias[1:2], 2: vias[2:3], 3: vias[3:] + directs[:1], 4: forwards[:1] + directs[1:2], 5: forwards[1:2] + directs[2:3], 6: forwards[2:4] + directs[3:], 7: forwards[4:5], 8: forwards[5:7], 9: forwards[7:]}
    jobs = work[0](work_in, work_out) if work else []
    for n, step in enumerate(gathering):
        step()
        for extra in between.get(n, []):
            extra()
        if 3 <= n and jobs:
            jobs.pop(0)()
    for job in jobs:
        job()
    last_rows(2)
    arrive_across(2)
    lax.fori_loop(0, 3, farthest_rows, 0)
    pick((2, 2, 2))
    if returning:
        finish()
        total = pair_sum(returning == "gated", row_ref, gate_ref, home_blocks(back))
        home_ref[...] = (base_ref[...].astype(F32) + total).astype(home_ref.dtype)
    if first:
        table_ref[...] = tiles[...]
    for copy in copies.values():
        copy.wait_send()


def return_scratch(sent):
    return [pltpu.VMEM(sent.shape, sent.dtype), pltpu.VMEM((RELAYS,) + sent.shape[1:], sent.dtype), pltpu.SemaphoreType.DMA((5,)), pltpu.SemaphoreType.DMA((RELAYS,))]


def send_rows(x, table, layer, own, capacity, call_id, first=False, scaled=False, home=None, gated=False, work=None):
    tok_dev, width = x.shape
    devices = 2 * SIDE ** 3
    count = 228 if first else 114
    u_shape = jax.ShapeDtypeStruct((own, devices * capacity, width), x.dtype)
    table_shape = jax.ShapeDtypeStruct((2, SIDE, SIDE, SIDE, 4, 8, 128), F32)
    outs = (u_shape,) + (u_shape,) * scaled + (table_shape,) * first
    if home:
        outs += (jax.ShapeDtypeStruct(home[0].shape, home[0].dtype),)
    jobs, job_in, job_out = work or (None, (), ())
    outs += tuple(job_out)
    vmem = pl.BlockSpec(memory_space=pltpu.VMEM)
    hbm = pl.BlockSpec(memory_space=pl.ANY)
    returning = None if home is None else "gated" if gated else "plain"
    return pl.pallas_call(
        functools.partial(send_kernel, own, capacity, layer, first, scaled, returning, work and (jobs, len(job_in), len(job_out))),
        out_shape=outs,
        in_specs=[hbm, hbm if first else vmem] + [vmem] * ((4 if home else 0) + len(job_in)),
        out_specs=(vmem,) * len(outs),
        scratch_shapes=[
            pltpu.VMEM((2, SIDE, SIDE, SIDE, tok_dev, width), x.dtype),
            pltpu.SemaphoreType.DMA,
            pltpu.SemaphoreType.DMA((count,)),
            pltpu.SemaphoreType.DMA((count,)),
        ] + ([pltpu.VMEM(table_shape.shape, F32)] if first else []) + (return_scratch(home[3]) if home else []),
        compiler_params=pltpu.CompilerParams(collective_id=call_id, has_side_effects=True, vmem_limit_bytes=(34 if home else 24) * 1024 * 1024),
        cost_estimate=pl.CostEstimate(flops=3 * 10**10, bytes_accessed=devices * tok_dev * width * 2, transcendentals=0),
        name=f"send_rows_{call_id}",
    )(x, table, *(home or ()), *job_in)


def pair_sum(gated, row_ref, gate_ref, back):
    codes, gates = row_ref[...], gate_ref[...]
    tok_dev = codes.shape[0]
    total = 0.0
    for base, rows in back:
        lane = lax.broadcasted_iota(jnp.int32, (tok_dev, rows.shape[0]), 1) + base
        weight = jnp.zeros(lane.shape, F32)
        for j in range(codes.shape[1]):
            weight = jnp.where(codes[:, j:j + 1] == lane, gates[:, j:j + 1] if gated else 1.0, weight)
        hi = weight.astype(BF16)
        terms = [hi]
        if gated:
            rest = weight - hi.astype(F32)
            mid = rest.astype(BF16)
            terms += [mid, (rest - mid.astype(F32)).astype(BF16)]
        part = jnp.dot(jnp.concatenate(terms, axis=0), rows, preferred_element_type=F32)
        for k in reversed(range(len(terms))):
            total = total + part[k * tok_dev:(k + 1) * tok_dev]
    return total


def look_up(lines, codes, per_device, first_lane):
    device = jnp.floor((codes.astype(F32) + 0.5) * (1.0 / per_device))
    place = codes.astype(F32) - device * per_device + first_lane
    hi = lines.astype(BF16)
    rest = lines - hi.astype(F32)
    mid = rest.astype(BF16)
    terms = jnp.concatenate([hi, mid, (rest - mid.astype(F32)).astype(BF16)], axis=1)
    tok_dev, top_k = codes.shape
    lane = lax.broadcasted_iota(jnp.int32, (tok_dev, 128), 1).astype(F32)
    out = jnp.zeros((tok_dev, 128), F32)
    for j in range(top_k):
        onehot = jnp.where(device[:, j:j + 1] == lane, 1.0, 0.0).astype(BF16)
        picked = jnp.dot(onehot, terms, preferred_element_type=F32)
        picked = picked[:, :128] + (picked[:, 128:256] + picked[:, 256:])
        value = jnp.sum(jnp.where(place[:, j:j + 1] == lane, picked, 0.0), axis=1, keepdims=True)
        out = jnp.where(lane == j, value, out)
    return out[:, :top_k]


def return_kernel(per_device, x_ref, row_ref, gate_ref, rows_ref, line_a_ref, line_b_ref, row_b_ref, out_ref, dgate_a_ref, dgate_b_ref, back, relay, sems, relay_sems, line_ref, line_back):
    me, core, at = my_place()
    devices = rows_ref.shape[0]
    line_ref[...] = line_a_ref[...] + line_b_ref[...]
    greet_all(me, core, at)
    vias, directs, forwards, finish = return_steps(me, core, at, rows_ref, back, relay, sems, relay_sems)

    def send_line(step, carry):
        to = lax.rem(me + step, devices)
        pltpu.make_async_remote_copy(src_ref=line_ref.at[to], dst_ref=line_back.at[me], send_sem=sems.at[3], recv_sem=sems.at[4], device_id={"ep": to}, device_id_type=pl.DeviceIdType.MESH).start()
        return carry

    for step in vias + directs[:2] + forwards[:2] + directs[2:] + forwards[2:4]:
        step()
    lax.fori_loop(1, devices, send_line, 0)
    for step in forwards[4:]:
        step()
    line_back[me] = line_ref[me]
    others = pl.ds(0, devices - 1)
    for k in (3, 4):
        pltpu.make_async_copy(line_ref.at[others], line_back.at[others], sems.at[k]).wait()
    lines = line_back[...].reshape(devices, 128)
    dgate_a_ref[...] = look_up(lines, row_ref[...], per_device, 0)
    dgate_b_ref[...] = look_up(lines, row_b_ref[...], per_device, per_device)
    finish()
    out_ref[...] = (x_ref[...].astype(F32) + pair_sum(False, row_ref, gate_ref, home_blocks(back))).astype(out_ref.dtype)


def return_home(x, rows, gates, sent, line_a, line_b, rows_b, per_device, call_id):
    vmem = pl.BlockSpec(memory_space=pltpu.VMEM)
    dgate = jax.ShapeDtypeStruct(rows.shape, F32)
    outs = (jax.ShapeDtypeStruct(x.shape, x.dtype), dgate, dgate)
    return pl.pallas_call(
        functools.partial(return_kernel, per_device),
        out_shape=outs,
        in_specs=[vmem] * 7,
        out_specs=(vmem,) * len(outs),
        scratch_shapes=return_scratch(sent) + [pltpu.VMEM(line_a.shape, F32)] * 2,
        compiler_params=pltpu.CompilerParams(collective_id=call_id, has_side_effects=True, vmem_limit_bytes=20 * 1024 * 1024),
        cost_estimate=pl.CostEstimate(flops=3 * 10**10, bytes_accessed=sent.size * 4, transcendentals=0),
        name="return_home",
    )(x, rows, gates, sent, line_a, line_b, rows_b)


def forward_rows(u, w_both, w_down):
    ff = w_down.shape[0]
    pre = jnp.dot(u, w_both, preferred_element_type=F32)
    pre_gate, pre_up = pre[:, :ff], pre[:, ff:]
    sig = 1.0 / (1.0 + jnp.exp(-pre_gate))
    silu = pre_gate * sig
    hidden = (silu * pre_up).astype(BF16)
    out = jnp.dot(hidden, w_down, preferred_element_type=F32)
    return pre_gate, pre_up, sig, silu, hidden, out


def store_home(out_ref, step, rows):
    count, width = rows.shape
    slots = out_ref.shape[1]
    sources = count // slots
    out_ref[pl.ds(step * sources, sources)] = rows.reshape(sources, slots, width).astype(out_ref.dtype)


def forward_kernel(chunk, u_ref, w1_ref, w3_ref, w2_ref, out_ref):
    w_both = jnp.concatenate([w1_ref[0], w3_ref[0]], axis=1)

    def body(step, carry):
        rows = pl.ds(pl.multiple_of(step * chunk, chunk), chunk)
        out = forward_rows(u_ref[0, rows, :], w_both, w2_ref[0])[-1]
        store_home(out_ref, step, out)
        return carry

    lax.fori_loop(0, u_ref.shape[1] // chunk, body, 0)


def forward_jobs(ins, outs):
    u_ref, w1_ref, w3_ref, w2_ref = ins
    out_ref, = outs
    chunk = 256
    own, count, width = u_ref.shape
    sources = out_ref.shape[0] * chunk // count
    slots = out_ref.shape[1] // own

    def job(e):
        w_both = jnp.concatenate([w1_ref[e], w3_ref[e]], axis=1)

        def body(step, carry):
            rows = pl.ds(pl.multiple_of(step * chunk, chunk), chunk)
            out = forward_rows(u_ref[e, rows, :], w_both, w2_ref[e])[-1]
            out_ref[pl.ds(step * sources, sources), e * slots:(e + 1) * slots, :] = out.reshape(sources, slots, width).astype(BF16)
            return carry

        lax.fori_loop(0, count // chunk, body, 0)

    return [functools.partial(job, e) for e in range(own)]


def backward_kernel(first_lane, chunk, u_ref, dy_ref, q_ref, w1_ref, w3_ref, w2_ref, du_ref, dgate_ref, dw1_ref, dw3_ref, dw2_ref, hidden_ref, both_ref):
    ff = w2_ref.shape[1]
    w_both = jnp.concatenate([w1_ref[0], w3_ref[0]], axis=1)
    last = (((1,), (1,)), ((), ()))

    def body(step, carry):
        rows = pl.ds(pl.multiple_of(step * chunk, chunk), chunk)
        pre_gate, pre_up, sig, silu, hidden, out = forward_rows(u_ref[0, rows, :], w_both, w2_ref[0])
        dgate = jnp.sum(dy_ref[0, rows, :].astype(F32) * out.astype(BF16).astype(F32), axis=1, keepdims=True)
        slots = du_ref.shape[1]
        lane = lax.broadcasted_iota(jnp.int32, (chunk, 128), 1)
        wanted = lax.rem(lax.broadcasted_iota(jnp.int32, (chunk, 128), 0), slots) + first_lane + pl.program_id(0) * slots
        line = jnp.where(lane == wanted, dgate, 0.0).reshape(chunk // slots, slots, 128)
        line = jnp.sum(line, axis=1, keepdims=True)
        at = pl.ds(step * (chunk // slots), chunk // slots)
        dgate_ref[at] = jnp.where(pl.program_id(0) == 0, 0.0, dgate_ref[at]) + line
        d_hidden = lax.dot_general(q_ref[0, rows, :], w2_ref[0], last, preferred_element_type=F32)
        da = (d_hidden * pre_up * sig * (1.0 + pre_gate * (1.0 - sig))).astype(BF16)
        db = (d_hidden * silu).astype(BF16)
        both = jnp.concatenate([da, db], axis=1)
        hidden_ref[rows, :] = hidden
        both_ref[rows, :] = both
        store_home(du_ref, step, lax.dot_general(both, w_both, last, preferred_element_type=F32))
        return carry

    lax.fori_loop(0, u_ref.shape[1] // chunk, body, 0)
    over_rows = (((0,), (0,)), ((), ()))
    dw = lax.dot_general(u_ref[0], both_ref[...], over_rows, preferred_element_type=F32)
    dw1_ref[0] = dw[:, :ff]
    dw3_ref[0] = dw[:, ff:]
    dw2_ref[0] = lax.dot_general(hidden_ref[...], q_ref[0], over_rows, preferred_element_type=F32)


def expert_call(kernel, inputs, outs, weights, n_group, name):
    own, count, width = inputs[0].shape
    ff = weights[2].shape[1]
    slots = count // n_group

    def each(shape):
        return pl.BlockSpec((1,) + shape, lambda e: (e, 0, 0))

    home = (jax.ShapeDtypeStruct((n_group, own * slots, width), BF16), pl.BlockSpec((n_group, slots, width), lambda e: (0, e, 0)))
    kinds = {
        "home": home,
        "gate": (jax.ShapeDtypeStruct((n_group, 1, 128), F32), pl.BlockSpec((n_group, 1, 128), lambda e: (0, 0, 0))),
        "up": (jax.ShapeDtypeStruct((own, width, ff), F32), each((width, ff))),
        "down": (jax.ShapeDtypeStruct((own, ff, width), F32), each((ff, width))),
    }
    steps = 3 if len(outs) == 1 else 11
    scratch = [] if len(outs) == 1 else [pltpu.VMEM((count, ff), BF16), pltpu.VMEM((count, 2 * ff), BF16)]
    return pl.pallas_call(
        functools.partial(kernel, 256),
        out_shape=tuple(kinds[k][0] for k in outs),
        grid=(own,),
        in_specs=[each((count, width))] * len(inputs) + [each((width, ff)), each((width, ff)), each((ff, width))],
        out_specs=tuple(kinds[k][1] for k in outs),
        scratch_shapes=scratch,
        compiler_params=pltpu.CompilerParams(vmem_limit_bytes=24 * 1024 * 1024),
        cost_estimate=pl.CostEstimate(flops=2 * steps * own * count * width * ff, bytes_accessed=own * count * width * 2 * (len(inputs) + 1), transcendentals=own * count * ff),
        name=name,
    )(*inputs, *weights)


def expert_forward(u_rows, weights, n_group):
    return expert_call(forward_kernel, (u_rows,), ("home",), weights, n_group, "expert_forward")[0]


def expert_backward(u_rows, dy_rows, q_rows, weights, n_group, first_lane):
    outs = ("home", "gate", "up", "up", "down")
    kernel = functools.partial(backward_kernel, first_lane)
    du, lines, *grads = expert_call(kernel, (u_rows, dy_rows, q_rows), outs, weights, n_group, "expert_backward")
    return du, lines, grads


def solution(mesh):
    n_group = mesh.shape["ep"]
    tok_spec = P(("dp", "ep"))
    w_spec = P("ep")

    def device_program(x_in, idx_a, idx_b, gate_a, gate_b, dy_out, w1_a, w3_a, w2_a, w1_b, w3_b, w2_b):
        tok_dev, top_k = idx_a.shape
        width = x_in.shape[1]
        own = w1_a.shape[0]
        capacity = CAP_FACTOR * tok_dev * top_k // (own * n_group)
        total = own * n_group * capacity
        block = own * capacity

        tile, rows_a, rows_b, gates_a, gates_b = make_tables(idx_a, idx_b, gate_a, gate_b, own * n_group, capacity)
        u_a, table = send_rows(x_in, tile, 0, own, capacity, 0, first=True)

        weights_a, weights_b = (w1_a, w3_a, w2_a), (w1_b, w3_b, w2_b)
        out_a = expert_forward(u_a, weights_a, n_group)
        dy_b, q_b, x_mid = send_rows(dy_out, table, 1, own, capacity, 1, scaled=True, home=(x_in, rows_a, gates_a, out_a), gated=True)
        u_b, = send_rows(x_mid, table, 1, own, capacity, 2)
        du_b, line_b, grads_b = expert_backward(u_b, dy_b, q_b, weights_b, n_group, block)
        forward_b = (forward_jobs, (u_b,) + weights_b, (jax.ShapeDtypeStruct((n_group, block, width), BF16),))
        u_again, dx_mid, out_b = send_rows(x_in, table, 0, own, capacity, 3, home=(dy_out, rows_b, gates_b, du_b), work=forward_b)
        dy_a, q_a, x_out = send_rows(dx_mid, table, 0, own, capacity, 4, scaled=True, home=(x_mid, rows_b, gates_b, out_b), gated=True)
        du_a, line_a, grads_a = expert_backward(u_again, dy_a, q_a, weights_a, n_group, 0)
        dx_in, dgate_a, dgate_b = return_home(dx_mid, rows_a, gates_a, du_a, line_a, line_b, rows_b, block, 5)
        return (x_out, dx_in) + tuple(grads_a) + tuple(grads_b) + (dgate_a, dgate_b)

    return jax.shard_map(device_program, mesh=mesh, in_specs=(tok_spec,) * 6 + (w_spec,) * 6, out_specs=(tok_spec,) * 10, check_vma=False)
```

```python
import functools

import jax
import jax.numpy as jnp
from jax import lax
from jax.experimental import pallas as pl
from jax.experimental.pallas import tpu as pltpu
from jax.sharding import PartitionSpec as P

CAP_FACTOR = 4
F32 = jnp.float32
BF16 = jnp.bfloat16


def table_kernel(experts, capacity, ids_a_ref, ids_b_ref, gate_a_ref, gate_b_ref, tile_ref, code_a_ref, code_b_ref, gates_a_ref, gates_b_ref):
    top_k, tok_dev = ids_a_ref.shape
    full = 128
    expert = lax.broadcasted_iota(jnp.int32, (full, experts), 1)
    row = lax.broadcasted_iota(jnp.int32, (full, full), 0)
    lane = lax.broadcasted_iota(jnp.int32, (full, full), 1)
    earlier = jnp.where(lane < row, 1.0, 0.0).astype(BF16)

    def turned(value, fill):
        value = jnp.concatenate([value.astype(F32), jnp.full((top_k, full - tok_dev), fill, F32)], axis=1)
        return value, jnp.concatenate([value, jnp.full((full - top_k, full), fill, F32)], axis=0).T

    for layer, (ids_ref, code_ref) in enumerate(((ids_a_ref, code_a_ref), (ids_b_ref, code_b_ref))):
        ids = turned(ids_ref[...], -1.0)[1].astype(jnp.int32)
        hits = [ids[:, j:j + 1] == expert for j in range(top_k)]
        chosen = jnp.zeros((full, experts), F32)
        for hit in hits:
            chosen = jnp.where(hit, 1.0, chosen)
        before = jnp.dot(earlier, chosen.astype(BF16), preferred_element_type=F32)
        code = jnp.full((full, full), -1.0, F32)
        for j, hit in enumerate(hits):
            slot = jnp.sum(jnp.where(hit, before, 0.0), axis=1, keepdims=True)
            code = jnp.where(lane == j, ids[:, j:j + 1].astype(F32) * capacity + slot, code)
        code = jnp.where(row < tok_dev, code, -1.0)
        code_ref[...] = code[:tok_dev, :top_k].astype(jnp.int32)
        tile_ref[layer] = code.T[:top_k]
    for layer, (gate_ref, out_ref) in enumerate(((gate_a_ref, gates_a_ref), (gate_b_ref, gates_b_ref))):
        tile, by_token = turned(gate_ref[...], 0.0)
        tile_ref[2 + layer] = tile
        out_ref[...] = by_token[:tok_dev, :top_k]


def make_tables(idx_a, idx_b, gate_a, gate_b, experts, capacity):
    tok_dev, top_k = idx_a.shape
    codes = jax.ShapeDtypeStruct((tok_dev, top_k), jnp.int32)
    gates = jax.ShapeDtypeStruct((tok_dev, top_k), F32)
    vmem = pl.BlockSpec(memory_space=pltpu.VMEM)
    return pl.pallas_call(
        functools.partial(table_kernel, experts, capacity),
        out_shape=(jax.ShapeDtypeStruct((4, top_k, 128), F32), codes, codes, gates, gates),
        in_specs=[vmem] * 4,
        out_specs=(vmem,) * 5,
        name="make_tables",
    )(idx_a.T, idx_b.T, gate_a.T, gate_b.T)


SIDE = 4


def my_place():
    me = lax.axis_index("ep")
    chip = lax.div(me, 2)
    at = (lax.rem(chip, SIDE), lax.rem(lax.div(chip, SIDE), SIDE), lax.div(chip, SIDE * SIDE))
    return me, lax.rem(me, 2), at


def device_at(at, core, delta, flip):
    c = [a if d == 0 else lax.rem(a + d + SIDE, SIDE) for a, d in zip(at, delta)]
    return ((c[2] * SIDE + c[1]) * SIDE + c[0]) * 2 + (1 - core if flip else core)


def return_offsets():
    direct, relayed = [], []
    devices = 2 * SIDE ** 3
    for step in range(1, devices):
        d = step * 37 % devices
        flip, delta = d % 2, (d // 2 % SIDE, d // (2 * SIDE) % SIDE, d // (2 * SIDE * SIDE))
        delta = tuple(v if v <= 2 else v - SIDE for v in delta)
        if 2 in delta:
            way = 1 if flip == 0 else -1
            delta = tuple(2 * way if v == 2 else v for v in delta)
            relayed.append((delta, flip, tuple(way if abs(v) == 2 else 0 for v in delta)))
        else:
            direct.append((delta, flip))
    return direct, relayed


RELAYS = len(return_offsets()[1])


def greet_all(me, core, at):
    barrier = pltpu.get_barrier_semaphore()
    devices = 2 * SIDE ** 3

    def hello(step, carry):
        pl.semaphore_signal(barrier, inc=1, device_id={"ep": lax.rem(me + step, devices)}, device_id_type=pl.DeviceIdType.MESH)
        return carry

    lax.fori_loop(1, devices, hello, 0)
    pl.semaphore_wait(barrier, devices - 1)


def return_steps(me, core, at, rows_ref, back, relay, sems, relay_sems):
    direct, relayed = return_offsets()
    devices = rows_ref.shape[0]

    def copy(src, dst, send_sem, recv_sem, to):
        return pltpu.make_async_remote_copy(src_ref=src, dst_ref=dst, send_sem=send_sem, recv_sem=recv_sem, device_id={"ep": to}, device_id_type=pl.DeviceIdType.MESH)

    def to_relay(k):
        delta, flip, via = relayed[k]
        return copy(rows_ref.at[device_at(at, core, delta, flip)], relay.at[k], sems.at[0], relay_sems.at[k], device_at(at, core, via, 0))

    def send_direct(k):
        to = device_at(at, core, *direct[k])
        copy(rows_ref.at[to], back.at[me], sems.at[1], sems.at[2], to).start()

    def forward(k):
        delta, flip, via = relayed[k]
        to_relay(k).wait_recv()
        origin = device_at(at, core, tuple(-v for v in via), 0)
        to = device_at(at, core, tuple(d - v for d, v in zip(delta, via)), flip)
        copy(relay.at[k], back.at[origin], sems.at[1], sems.at[2], to).start()

    def finish():
        back[me] = rows_ref[me]
        others = pl.ds(0, devices - 1)
        pltpu.make_async_copy(rows_ref.at[others], back.at[others], sems.at[2]).wait()
        pltpu.make_async_copy(rows_ref.at[others], back.at[others], sems.at[1]).wait()
        relays = pl.ds(0, len(relayed))
        pltpu.make_async_copy(rows_ref.at[relays], relay.at[relays], sems.at[0]).wait()

    def pieces(count, action, parts):
        cut = [count * i // parts for i in range(parts + 1)]
        return [lambda lo=lo, hi=hi: [action(k) for k in range(lo, hi)] for lo, hi in zip(cut, cut[1:])]

    vias = pieces(len(relayed), lambda k: to_relay(k).start(), 4)
    directs = pieces(len(direct), send_direct, 4)
    forwards = pieces(len(relayed), forward, 8)
    return vias, directs, forwards, finish


def home_blocks(back):
    group = 16
    count, width = back.shape[1], back.shape[2]
    return ((g * count, back[pl.ds(g, group)].reshape(group * count, width)) for g in range(0, back.shape[0], group))


def send_kernel(own, capacity, layer, first, scaled, returning, work, *refs):
    refs = list(refs)
    x_ref, tile_ref = refs.pop(0), refs.pop(0)
    if returning:
        base_ref, row_ref, gate_ref, rows_ref = (refs.pop(0) for _ in range(4))
    work_in = [refs.pop(0) for _ in range(work[1])] if work else []
    u_ref = refs.pop(0)
    if scaled:
        q_ref = refs.pop(0)
    if first:
        table_ref = refs.pop(0)
    if returning:
        home_ref = refs.pop(0)
    work_out = [refs.pop(0) for _ in range(work[2])] if work else []
    held, local_sem, send_sem, recv_sem = (refs.pop(0) for _ in range(4))
    tiles = refs.pop(0) if first else tile_ref
    if returning:
        back, relay, return_sems, relay_sems = refs
    me, core, at = my_place()
    plus = x_ref.shape[0] // 6
    third = x_ref.shape[0] // 3
    spans = {1: (0, plus), -1: (plus, third - plus)}

    def device(dim, step):
        return device_at(at, core, [step if d == dim else 0 for d in range(3)], 0)

    partner = device_at(at, core, (0, 0, 0), 1)

    def region(part, pos, span):
        idx = [pos[d] if d in pos else at[d] for d in range(3)]
        idx = [pl.ds(0, SIDE) if i is None else i for i in idx]
        where = (core, idx[2], idx[1], idx[0])
        return held.at[where + (pl.ds(part * third + span[0], span[1]),)], where + (pl.ds(part, 2 if part == 2 else 1),)

    copies = {}

    def start(key, refs, to, with_tile):
        for kind, ref in (("x", refs[0]), ("t", tiles.at[refs[1]])):
            if kind == "t" and not (first and with_tile):
                continue
            n = len(copies)
            copy = pltpu.make_async_remote_copy(src_ref=ref, dst_ref=ref, send_sem=send_sem.at[n], recv_sem=recv_sem.at[n], device_id={"ep": to}, device_id_type=pl.DeviceIdType.MESH)
            copy.start()
            copies[key + (kind,)] = copy

    def arrive(*key):
        for kind in ("x", "t"):
            if key + (kind,) in copies:
                copies[key + (kind,)].wait_recv()

    mine = pltpu.make_async_copy(x_ref, held.at[core, at[2], at[1], at[0]], local_sem)
    mine.start()
    if first:
        own_tile = pltpu.make_async_copy(tile_ref, tiles.at[core, at[2], at[1], at[0]], send_sem.at[0])
        own_tile.start()
        own_tile.wait()
    if returning:
        greet_all(me, core, at)
        mine.wait()
    else:
        barrier = pltpu.get_barrier_semaphore()
        for dim in range(3):
            for step in (1, -1, 2):
                pl.semaphore_signal(barrier, inc=1, device_id={"ep": device(dim, step)}, device_id_type=pl.DeviceIdType.MESH)
        pl.semaphore_signal(barrier, inc=1, device_id={"ep": partner}, device_id_type=pl.DeviceIdType.MESH)
        mine.wait()
        pl.semaphore_wait(barrier, 10)

    def dims(part):
        return part, (part + 1) % 3, (part + 2) % 3

    def shift(dim, step):
        return lax.rem(at[dim] + step + SIDE, SIDE)

    whole = (0, third)

    def row_of(part, b, c, span=whole):
        d1, d2, d3 = dims(part)
        return region(part, {d1: None, d2: shift(d2, b), d3: shift(d3, c)}, span)

    def across(part, b, c):
        start(("d2d", part, b, c), row_of(part, b, c), partner, True)

    def whole_row(part, b):
        d3 = dims(part)[2]
        for way in (1, -1):
            start(("m3", part, b, way), row_of(part, b, 0), device(d3, way), True)
        across(part, b, 0)

    def pass_on(part, b, way):
        d3 = dims(part)[2]
        arrive("m3", part, b, way)
        start(("f3", part, b, way), row_of(part, b, -way, spans[way]), device(d3, way), way == -1)
        across(part, b, -way)

    def last_row(part, b):
        for way in (1, -1):
            arrive("f3", part, b, way)
        across(part, b, 2)

    block = own * capacity
    slot = lax.broadcasted_iota(jnp.int32, (block, 128), 0) + me * block
    tok_dev = x_ref.shape[0]

    def pick(offsets):
        x, y, z = (lax.rem(at[d] + offsets[d] + SIDE, SIDE) for d in range(3))
        rows, scaled_rows = [], []
        for c in range(2):
            code = tiles[c, z, y, x, layer].astype(jnp.int32)
            gate = tiles[c, z, y, x, 2 + layer] if scaled else None
            hit = code[0:1, :] == slot
            weight = jnp.where(hit, gate[0:1, :], 0.0) if scaled else None
            for j in range(1, code.shape[0]):
                hit_j = code[j:j + 1, :] == slot
                hit = hit | hit_j
                if scaled:
                    weight = jnp.where(hit_j, gate[j:j + 1, :], weight)
            onehot = jnp.where(hit, 1.0, 0.0)[:, :tok_dev].astype(BF16)
            rows.append(jnp.dot(onehot, held[c, z, y, x], preferred_element_type=F32))
            if scaled:
                scaled_rows.append(jnp.sum(weight, axis=1, keepdims=True) * rows[-1])
        place = ((z * SIDE + y) * SIDE + x) * 2 * capacity
        for out_ref, parts in ((u_ref, rows),) + (((q_ref, scaled_rows),) if scaled else ()):
            for e in range(own):
                both = jnp.concatenate([r[e * capacity:(e + 1) * capacity] for r in parts], axis=0)
                out_ref[e, pl.ds(pl.multiple_of(place, 2 * capacity), 2 * capacity), :] = both.astype(BF16)

    def near_rows(step, carry):
        for k in (-1, 0, 1):
            pick((k, lax.rem(step, 3) - 1, lax.div(step, 3) - 1))
        return carry

    def far_rows(step, carry):
        b, c = lax.rem(step, 3) - 1, lax.div(step, 3) - 1
        for offsets in ((2, b, c), (b, 2, c), (b, c, 2)):
            pick(offsets)
        return carry

    def farthest_rows(step, carry):
        for offsets in ((2, 2, step - 1), (2, step - 1, 2), (step - 1, 2, 2)):
            pick(offsets)
        return carry

    def arrive_across(wanted):
        for part in range(3):
            for b in (0, -1, 1, 2):
                for c in (0, -1, 1, 2):
                    if (b == 2) + (c == 2) == wanted:
                        arrive("d2d", part, b, c)

    def first_sends():
        for part in range(3):
            for way in (2, 1, -1):
                start(("m1", part, way), region(part, {}, whole), device(dims(part)[0], way), True)

    def second_sends():
        for part in range(3):
            for way in (1, -1, 2):
                arrive("m1", part, way)
            for way in (2, 1, -1):
                start(("m2", part, way), row_of(part, 0, 0), device(dims(part)[1], way), True)

    def own_rows():
        for part in range(3):
            whole_row(part, 0)

    def near_sends():
        for part in range(3):
            for way in (1, -1):
                arrive("m2", part, way)
                whole_row(part, -way)

    def pass_rows(b):
        for part in range(3):
            for way in (1, -1):
                pass_on(part, b, way)

    def opposite_rows():
        for part in range(3):
            arrive("m2", part, 2)
            whole_row(part, 2)

    def last_rows(b):
        for part in range(3):
            last_row(part, b)

    def pick_near():
        arrive_across(0)
        lax.fori_loop(0, 9, near_rows, 0)

    def pick_far():
        arrive_across(1)
        lax.fori_loop(0, 9, far_rows, 0)

    gathering = [first_sends, second_sends, own_rows, near_sends, lambda: pass_rows(0), opposite_rows, lambda: pass_rows(-1), lambda: pass_rows(1), pick_near, lambda: last_rows(0), lambda: pass_rows(2), lambda: last_rows(-1), lambda: last_rows(1), pick_far]
    between = {}
    if returning:
        vias, directs, forwards, finish = return_steps(me, core, at, rows_ref, back, relay, return_sems, relay_sems)
        between = {0: vias[:1], 1: vias[1:2], 2: vias[2:3], 3: vias[3:] + directs[:1], 4: forwards[:1] + directs[1:2], 5: forwards[1:2] + directs[2:3], 6: forwards[2:4] + directs[3:], 7: forwards[4:5], 8: forwards[5:7], 9: forwards[7:]}
    jobs = work[0](work_in, work_out) if work else []
    for n, step in enumerate(gathering):
        step()
        for extra in between.get(n, []):
            extra()
        if 3 <= n and jobs:
            jobs.pop(0)()
    for job in jobs:
        job()
    last_rows(2)
    arrive_across(2)
    lax.fori_loop(0, 3, farthest_rows, 0)
    pick((2, 2, 2))
    if returning:
        finish()
        total = pair_sum(returning == "gated", row_ref, gate_ref, home_blocks(back))
        home_ref[...] = (base_ref[...].astype(F32) + total).astype(home_ref.dtype)
    if first:
        table_ref[...] = tiles[...]
    for copy in copies.values():
        copy.wait_send()


def return_scratch(sent):
    return [pltpu.VMEM(sent.shape, sent.dtype), pltpu.VMEM((RELAYS,) + sent.shape[1:], sent.dtype), pltpu.SemaphoreType.DMA((5,)), pltpu.SemaphoreType.DMA((RELAYS,))]


def send_rows(x, table, layer, own, capacity, call_id, first=False, scaled=False, home=None, gated=False, work=None):
    tok_dev, width = x.shape
    devices = 2 * SIDE ** 3
    count = 228 if first else 114
    u_shape = jax.ShapeDtypeStruct((own, devices * capacity, width), x.dtype)
    table_shape = jax.ShapeDtypeStruct((2, SIDE, SIDE, SIDE, 4, 8, 128), F32)
    outs = (u_shape,) + (u_shape,) * scaled + (table_shape,) * first
    if home:
        outs += (jax.ShapeDtypeStruct(home[0].shape, home[0].dtype),)
    jobs, job_in, job_out = work or (None, (), ())
    outs += tuple(job_out)
    vmem = pl.BlockSpec(memory_space=pltpu.VMEM)
    hbm = pl.BlockSpec(memory_space=pl.ANY)
    returning = None if home is None else "gated" if gated else "plain"
    return pl.pallas_call(
        functools.partial(send_kernel, own, capacity, layer, first, scaled, returning, work and (jobs, len(job_in), len(job_out))),
        out_shape=outs,
        in_specs=[hbm, hbm if first else vmem] + [vmem] * ((4 if home else 0) + len(job_in)),
        out_specs=(vmem,) * len(outs),
        scratch_shapes=[
            pltpu.VMEM((2, SIDE, SIDE, SIDE, tok_dev, width), x.dtype),
            pltpu.SemaphoreType.DMA,
            pltpu.SemaphoreType.DMA((count,)),
            pltpu.SemaphoreType.DMA((count,)),
        ] + ([pltpu.VMEM(table_shape.shape, F32)] if first else []) + (return_scratch(home[3]) if home else []),
        compiler_params=pltpu.CompilerParams(collective_id=call_id, has_side_effects=True, vmem_limit_bytes=(34 if home else 24) * 1024 * 1024),
        cost_estimate=pl.CostEstimate(flops=3 * 10**10, bytes_accessed=devices * tok_dev * width * 2, transcendentals=0),
        name=f"send_rows_{call_id}",
    )(x, table, *(home or ()), *job_in)


def pair_sum(gated, row_ref, gate_ref, back):
    codes, gates = row_ref[...], gate_ref[...]
    tok_dev = codes.shape[0]
    total = 0.0
    for base, rows in back:
        lane = lax.broadcasted_iota(jnp.int32, (tok_dev, rows.shape[0]), 1) + base
        weight = jnp.zeros(lane.shape, F32)
        for j in range(codes.shape[1]):
            weight = jnp.where(codes[:, j:j + 1] == lane, gates[:, j:j + 1] if gated else 1.0, weight)
        hi = weight.astype(BF16)
        terms = [hi]
        if gated:
            rest = weight - hi.astype(F32)
            mid = rest.astype(BF16)
            terms += [mid, (rest - mid.astype(F32)).astype(BF16)]
        part = jnp.dot(jnp.concatenate(terms, axis=0), rows, preferred_element_type=F32)
        for k in reversed(range(len(terms))):
            total = total + part[k * tok_dev:(k + 1) * tok_dev]
    return total


def look_up(lines, codes, per_device, first_lane):
    device = jnp.floor((codes.astype(F32) + 0.5) * (1.0 / per_device))
    place = codes.astype(F32) - device * per_device + first_lane
    hi = lines.astype(BF16)
    rest = lines - hi.astype(F32)
    mid = rest.astype(BF16)
    terms = jnp.concatenate([hi, mid, (rest - mid.astype(F32)).astype(BF16)], axis=1)
    tok_dev, top_k = codes.shape
    lane = lax.broadcasted_iota(jnp.int32, (tok_dev, 128), 1).astype(F32)
    out = jnp.zeros((tok_dev, 128), F32)
    for j in range(top_k):
        onehot = jnp.where(device[:, j:j + 1] == lane, 1.0, 0.0).astype(BF16)
        picked = jnp.dot(onehot, terms, preferred_element_type=F32)
        picked = picked[:, :128] + (picked[:, 128:256] + picked[:, 256:])
        value = jnp.sum(jnp.where(place[:, j:j + 1] == lane, picked, 0.0), axis=1, keepdims=True)
        out = jnp.where(lane == j, value, out)
    return out[:, :top_k]


def return_kernel(per_device, x_ref, row_ref, gate_ref, rows_ref, line_a_ref, line_b_ref, row_b_ref, out_ref, dgate_a_ref, dgate_b_ref, back, relay, sems, relay_sems, line_ref, line_back):
    me, core, at = my_place()
    devices = rows_ref.shape[0]
    line_ref[...] = line_a_ref[...] + line_b_ref[...]
    greet_all(me, core, at)
    vias, directs, forwards, finish = return_steps(me, core, at, rows_ref, back, relay, sems, relay_sems)

    def send_line(step, carry):
        to = lax.rem(me + step, devices)
        pltpu.make_async_remote_copy(src_ref=line_ref.at[to], dst_ref=line_back.at[me], send_sem=sems.at[3], recv_sem=sems.at[4], device_id={"ep": to}, device_id_type=pl.DeviceIdType.MESH).start()
        return carry

    for step in vias + directs[:2] + forwards[:2] + directs[2:] + forwards[2:4]:
        step()
    lax.fori_loop(1, devices, send_line, 0)
    for step in forwards[4:]:
        step()
    line_back[me] = line_ref[me]
    others = pl.ds(0, devices - 1)
    for k in (3, 4):
        pltpu.make_async_copy(line_ref.at[others], line_back.at[others], sems.at[k]).wait()
    lines = line_back[...].reshape(devices, 128)
    dgate_a_ref[...] = look_up(lines, row_ref[...], per_device, 0)
    dgate_b_ref[...] = look_up(lines, row_b_ref[...], per_device, per_device)
    finish()
    out_ref[...] = (x_ref[...].astype(F32) + pair_sum(False, row_ref, gate_ref, home_blocks(back))).astype(out_ref.dtype)


def return_home(x, rows, gates, sent, line_a, line_b, rows_b, per_device, call_id):
    vmem = pl.BlockSpec(memory_space=pltpu.VMEM)
    dgate = jax.ShapeDtypeStruct(rows.shape, F32)
    outs = (jax.ShapeDtypeStruct(x.shape, x.dtype), dgate, dgate)
    return pl.pallas_call(
        functools.partial(return_kernel, per_device),
        out_shape=outs,
        in_specs=[vmem] * 7,
        out_specs=(vmem,) * len(outs),
        scratch_shapes=return_scratch(sent) + [pltpu.VMEM(line_a.shape, F32)] * 2,
        compiler_params=pltpu.CompilerParams(collective_id=call_id, has_side_effects=True, vmem_limit_bytes=20 * 1024 * 1024),
        cost_estimate=pl.CostEstimate(flops=3 * 10**10, bytes_accessed=sent.size * 4, transcendentals=0),
        name="return_home",
    )(x, rows, gates, sent, line_a, line_b, rows_b)


def forward_rows(u, w_both, w_down):
    ff = w_down.shape[0]
    pre = jnp.dot(u, w_both, preferred_element_type=F32)
    pre_gate, pre_up = pre[:, :ff], pre[:, ff:]
    sig = 1.0 / (1.0 + jnp.exp(-pre_gate))
    silu = pre_gate * sig
    hidden = (silu * pre_up).astype(BF16)
    out = jnp.dot(hidden, w_down, preferred_element_type=F32)
    return pre_gate, pre_up, sig, silu, hidden, out


def store_home(out_ref, step, rows):
    count, width = rows.shape
    slots = out_ref.shape[1]
    sources = count // slots
    out_ref[pl.ds(step * sources, sources)] = rows.reshape(sources, slots, width).astype(out_ref.dtype)


def forward_kernel(chunk, u_ref, w1_ref, w3_ref, w2_ref, out_ref):
    w_both = jnp.concatenate([w1_ref[0], w3_ref[0]], axis=1)

    def body(step, carry):
        rows = pl.ds(pl.multiple_of(step * chunk, chunk), chunk)
        out = forward_rows(u_ref[0, rows, :], w_both, w2_ref[0])[-1]
        store_home(out_ref, step, out)
        return carry

    lax.fori_loop(0, u_ref.shape[1] // chunk, body, 0)


def forward_jobs(ins, outs):
    u_ref, w1_ref, w3_ref, w2_ref = ins
    out_ref, = outs
    chunk = 512
    own, count, width = u_ref.shape
    sources = out_ref.shape[0] * chunk // count
    slots = out_ref.shape[1] // own

    def job(e):
        w_both = jnp.concatenate([w1_ref[e], w3_ref[e]], axis=1)

        def body(step, carry):
            rows = pl.ds(pl.multiple_of(step * chunk, chunk), chunk)
            out = forward_rows(u_ref[e, rows, :], w_both, w2_ref[e])[-1]
            out_ref[pl.ds(step * sources, sources), e * slots:(e + 1) * slots, :] = out.reshape(sources, slots, width).astype(BF16)
            return carry

        lax.fori_loop(0, count // chunk, body, 0)

    return [functools.partial(job, e) for e in range(own)]


def backward_kernel(first_lane, chunk, u_ref, dy_ref, q_ref, w1_ref, w3_ref, w2_ref, du_ref, dgate_ref, dw1_ref, dw3_ref, dw2_ref, hidden_ref, both_ref):
    ff = w2_ref.shape[1]
    w_both = jnp.concatenate([w1_ref[0], w3_ref[0]], axis=1)
    last = (((1,), (1,)), ((), ()))

    def body(step, carry):
        rows = pl.ds(pl.multiple_of(step * chunk, chunk), chunk)
        pre_gate, pre_up, sig, silu, hidden, out = forward_rows(u_ref[0, rows, :], w_both, w2_ref[0])
        dgate = jnp.sum(dy_ref[0, rows, :].astype(F32) * out.astype(BF16).astype(F32), axis=1, keepdims=True)
        slots = du_ref.shape[1]
        lane = lax.broadcasted_iota(jnp.int32, (chunk, 128), 1)
        wanted = lax.rem(lax.broadcasted_iota(jnp.int32, (chunk, 128), 0), slots) + first_lane + pl.program_id(0) * slots
        line = jnp.where(lane == wanted, dgate, 0.0).reshape(chunk // slots, slots, 128)
        line = jnp.sum(line, axis=1, keepdims=True)
        at = pl.ds(step * (chunk // slots), chunk // slots)
        dgate_ref[at] = jnp.where(pl.program_id(0) == 0, 0.0, dgate_ref[at]) + line
        d_hidden = lax.dot_general(q_ref[0, rows, :], w2_ref[0], last, preferred_element_type=F32)
        da = (d_hidden * pre_up * sig * (1.0 + pre_gate * (1.0 - sig))).astype(BF16)
        db = (d_hidden * silu).astype(BF16)
        both = jnp.concatenate([da, db], axis=1)
        hidden_ref[rows, :] = hidden
        both_ref[rows, :] = both
        store_home(du_ref, step, lax.dot_general(both, w_both, last, preferred_element_type=F32))
        return carry

    lax.fori_loop(0, u_ref.shape[1] // chunk, body, 0)
    over_rows = (((0,), (0,)), ((), ()))
    dw = lax.dot_general(u_ref[0], both_ref[...], over_rows, preferred_element_type=F32)
    dw1_ref[0] = dw[:, :ff]
    dw3_ref[0] = dw[:, ff:]
    dw2_ref[0] = lax.dot_general(hidden_ref[...], q_ref[0], over_rows, preferred_element_type=F32)


def expert_call(kernel, inputs, outs, weights, n_group, name):
    own, count, width = inputs[0].shape
    ff = weights[2].shape[1]
    slots = count // n_group

    def each(shape):
        return pl.BlockSpec((1,) + shape, lambda e: (e, 0, 0))

    home = (jax.ShapeDtypeStruct((n_group, own * slots, width), BF16), pl.BlockSpec((n_group, slots, width), lambda e: (0, e, 0)))
    kinds = {
        "home": home,
        "gate": (jax.ShapeDtypeStruct((n_group, 1, 128), F32), pl.BlockSpec((n_group, 1, 128), lambda e: (0, 0, 0))),
        "up": (jax.ShapeDtypeStruct((own, width, ff), F32), each((width, ff))),
        "down": (jax.ShapeDtypeStruct((own, ff, width), F32), each((ff, width))),
    }
    steps = 3 if len(outs) == 1 else 11
    scratch = [] if len(outs) == 1 else [pltpu.VMEM((count, ff), BF16), pltpu.VMEM((count, 2 * ff), BF16)]
    return pl.pallas_call(
        functools.partial(kernel, 512),
        out_shape=tuple(kinds[k][0] for k in outs),
        grid=(own,),
        in_specs=[each((count, width))] * len(inputs) + [each((width, ff)), each((width, ff)), each((ff, width))],
        out_specs=tuple(kinds[k][1] for k in outs),
        scratch_shapes=scratch,
        compiler_params=pltpu.CompilerParams(vmem_limit_bytes=24 * 1024 * 1024),
        cost_estimate=pl.CostEstimate(flops=2 * steps * own * count * width * ff, bytes_accessed=own * count * width * 2 * (len(inputs) + 1), transcendentals=own * count * ff),
        name=name,
    )(*inputs, *weights)


def expert_forward(u_rows, weights, n_group):
    return expert_call(forward_kernel, (u_rows,), ("home",), weights, n_group, "expert_forward")[0]


def expert_backward(u_rows, dy_rows, q_rows, weights, n_group, first_lane):
    outs = ("home", "gate", "up", "up", "down")
    kernel = functools.partial(backward_kernel, first_lane)
    du, lines, *grads = expert_call(kernel, (u_rows, dy_rows, q_rows), outs, weights, n_group, "expert_backward")
    return du, lines, grads


def solution(mesh):
    n_group = mesh.shape["ep"]
    tok_spec = P(("dp", "ep"))
    w_spec = P("ep")

    def device_program(x_in, idx_a, idx_b, gate_a, gate_b, dy_out, w1_a, w3_a, w2_a, w1_b, w3_b, w2_b):
        tok_dev, top_k = idx_a.shape
        width = x_in.shape[1]
        own = w1_a.shape[0]
        capacity = CAP_FACTOR * tok_dev * top_k // (own * n_group)
        total = own * n_group * capacity
        block = own * capacity

        tile, rows_a, rows_b, gates_a, gates_b = make_tables(idx_a, idx_b, gate_a, gate_b, own * n_group, capacity)
        u_a, table = send_rows(x_in, tile, 0, own, capacity, 0, first=True)

        weights_a, weights_b = (w1_a, w3_a, w2_a), (w1_b, w3_b, w2_b)
        out_a = expert_forward(u_a, weights_a, n_group)
        dy_b, q_b, x_mid = send_rows(dy_out, table, 1, own, capacity, 1, scaled=True, home=(x_in, rows_a, gates_a, out_a), gated=True)
        u_b, = send_rows(x_mid, table, 1, own, capacity, 2)
        du_b, line_b, grads_b = expert_backward(u_b, dy_b, q_b, weights_b, n_group, block)
        forward_b = (forward_jobs, (u_b,) + weights_b, (jax.ShapeDtypeStruct((n_group, block, width), BF16),))
        u_again, dx_mid, out_b = send_rows(x_in, table, 0, own, capacity, 3, home=(dy_out, rows_b, gates_b, du_b), work=forward_b)
        dy_a, q_a, x_out = send_rows(dx_mid, table, 0, own, capacity, 4, scaled=True, home=(x_mid, rows_b, gates_b, out_b), gated=True)
        du_a, line_a, grads_a = expert_backward(u_again, dy_a, q_a, weights_a, n_group, 0)
        dx_in, dgate_a, dgate_b = return_home(dx_mid, rows_a, gates_a, du_a, line_a, line_b, rows_b, block, 5)
        return (x_out, dx_in) + tuple(grads_a) + tuple(grads_b) + (dgate_a, dgate_b)

    return jax.shard_map(device_program, mesh=mesh, in_specs=(tok_spec,) * 6 + (w_spec,) * 6, out_specs=(tok_spec,) * 10, check_vma=False)
```
